32 devices in a mesh: rows: 4 (over y, x), heads: 8 (over z, core).
Axes of the slice: x: 2, y: 2, z: 4, core: 2. Of those that a mesh axis runs over, the one named last changes fastest.
Arguments:
- hidden_in: bfloat16 [16384, 2048], P('rows', 'heads'), may hold values from -6 to 6
- lengths: int32 [4, 4], P('rows'), may hold values from 0 to 4096, as said below
- norm_gain: float32 [2048], P('heads'), may hold values from 0.5 to 1.5
- in_gate_inner: bfloat16 [2048, 2, 4096], P(None, None, 'heads'), may hold values from -0.125 to 0.125
- in_step: bfloat16 [2048, 64], P(None, 'heads'), may hold values from -0.25 to 0.25
- in_shared: bfloat16 [128, 2048], P(None, 'heads'), may hold values from -0.125 to 0.125
- conv_inner: float32 [4, 4096], P(None, 'heads'), may hold values from -3 to 3
- conv_inner_bias: float32 [4096], P('heads'), may hold values from -3 to 3
- conv_shared: float32 [4, 128], replicated, may hold values from -3 to 3
- conv_shared_bias: float32 [128], replicated, may hold values from -3 to 3
- step_bias: float32 [64], P('heads'), may hold values from -4 to -2
- log_decay: float32 [64], P('heads'), may hold values from -6 to 1
- skip_gain: float32 [64], P('heads'), may hold values from 0.5 to 1.5
- gate_gain: float32 [4096], P('heads'), may hold values from 0.5 to 1.5
- out_weight: bfloat16 [4096, 2048], P('heads'), may hold values from -0.09375 to 0.09375
- cotangent: bfloat16 [16384, 2048], P('rows', 'heads'), may hold values from -6 to 6
Outputs:
- output: bfloat16 [16384, 2048], P('rows', 'heads')
- grad_input: float32 [16384, 2048], P('rows', 'heads')
- grad_norm_gain: float32 [2048], P('heads')
- grad_in_gate_inner: float32 [2048, 2, 4096], P(None, None, 'heads')
- grad_in_step: float32 [2048, 64], P(None, 'heads')
- grad_in_shared: float32 [128, 2048], P(None, 'heads')
- grad_conv_inner: float32 [4, 4096], P(None, 'heads')
- grad_conv_inner_bias: float32 [4096], P('heads')
- grad_conv_shared: float32 [4, 128], replicated
- grad_conv_shared_bias: float32 [128], replicated
- grad_step_bias: float32 [64], P('heads')
- grad_log_decay: float32 [64], P('heads')
- grad_skip_gain: float32 [64], P('heads')
- grad_gate_gain: float32 [4096], P('heads')
- grad_out_weight: float32 [4096, 2048], P('heads')
The draws below stay inside these ranges and needn't reach their ends.
Inputs may be any that keep to these rules, and one draw needn't show every extreme that they name: `lengths`: row g lists the sequences packed at the start of group g: its nonzero entries come first, each from 512 to 4096, then zeros; their sum is at most 4096 and the rest of the group is padding. In every draw one row holds a single sequence of exactly 4096 tokens.
All inputs are finite; a program needn't handle non-finite values.
Results may differ from the reference program's by a relative error of at most 0.00155.
The reference program's roundings to bfloat16 on the way (of `normed` and `scaled`) count: a program that leaves them out, or rounds other values in their place, can miss the bound.
Values may be sent and summed in bfloat16 or wider, within the bound.
A program may use at most 320 MiB of HBM per device.

```python
import jax
import jax.numpy as jnp
from jax import lax

D = 2048
NH = 64
N = 64
KW = 4
CH = 256
DI = 4096
TOK_DEV = 4096
SLOTS = 4
MIN_LEN = 512
GROUPS = 4
TOKENS = 16384


def draw_lengths(key, part):
    group_count = TOKENS // TOK_DEV
    first_key, second_key, third_key, fourth_key = jax.random.split(key, 4)
    used_count = jax.random.randint(first_key, (group_count, 1), 1, SLOTS + 1)
    weights_raw = jax.random.randint(second_key, (group_count, SLOTS), 1, 33)
    weights_cube = weights_raw * weights_raw * weights_raw
    slot_index = jnp.arange(SLOTS)[None, :]
    used_slot = slot_index < used_count
    weights_used = jnp.where(used_slot, weights_cube, 0)
    padding_raw = jax.random.randint(third_key, (group_count, 1), 0, 33)
    padding_weight = padding_raw * padding_raw * padding_raw
    remaining = TOK_DEV - used_count * MIN_LEN
    denominator = jnp.sum(weights_used, axis=1, keepdims=True) + padding_weight
    spread_len = MIN_LEN + remaining * weights_used // denominator
    lengths_drawn = jnp.where(used_slot, spread_len, 0)
    full_group = jax.random.randint(fourth_key, (), 0, group_count)
    group_index = jnp.arange(group_count)[:, None]
    single = jnp.where(slot_index == 0, TOK_DEV, 0)
    return jnp.where(group_index == full_group, single, lengths_drawn).astype(jnp.int32)


def steps_of(own_key, dims, shards, smallest, high):
    loudness, own = 1.0, jax.random.fold_in(own_key, 6)
    for dim, parts in shards:
        steps = jnp.exp(jax.random.uniform(jax.random.fold_in(own, dim), (parts,), jnp.float32, smallest / len(shards), high / len(shards)))
        loudness = loudness * jnp.repeat(steps, dims[dim] // parts).reshape([-1 if axis == dim else 1 for axis in range(len(dims))])
    return loudness


def gaussian(rng, shape, deviation, most, pieces=(), held_as=jnp.bfloat16):
    loudness = steps_of(rng, shape, pieces, -0.22, 0.18) if pieces else 1.0
    values = jax.random.normal(rng, shape, jnp.float32) * deviation * loudness
    return jnp.minimum(jnp.maximum(values, -most), most).astype(held_as)


def setup_inputs(seed: int = 0) -> dict:
    keys = jax.random.split(jax.random.key(seed), 17)
    hidden_in = gaussian(keys[0], (TOKENS, D), 1.0, 6.0, ((0, 4), (1, 8)))
    lengths = draw_lengths(jax.random.fold_in(keys[16], 71), 0)
    norm_gain = jnp.clip(1.0 + 0.1 * jax.random.normal(keys[2], (D,), jnp.float32), 0.5, 1.5)
    in_gate_inner = gaussian(keys[3], (D, 2, DI), D ** -0.5, 0.125, ((2, 8),))
    in_step = gaussian(keys[4], (D, NH), (D // 4) ** -0.5, 0.25, ((1, 8),))
    in_shared = gaussian(keys[5], (2 * N, D), D ** -0.5, 0.125, ((1, 8),))
    conv_inner = gaussian(keys[6], (KW, DI), KW ** -0.5, 3.0, ((1, 8),), jnp.float32)
    conv_inner_bias = gaussian(keys[7], (DI,), 0.5, 3.0, ((0, 8),), jnp.float32)
    conv_shared = gaussian(keys[8], (KW, 2 * N), KW ** -0.5, 3.0, (), jnp.float32)
    conv_shared_bias = gaussian(keys[9], (2 * N,), 0.5, 3.0, (), jnp.float32)
    step_bias = jnp.clip(-4.0 + 2.0 * jax.random.uniform(keys[10], (NH,), jnp.float32) ** steps_of(keys[10], (NH,), ((0, 8),), -0.2, 0.2), -4.0, -2.0)
    log_decay = jnp.clip(-6.0 + 7.0 * jax.random.uniform(keys[11], (NH,), jnp.float32) ** steps_of(keys[11], (NH,), ((0, 8),), -0.2, 0.2), -6.0, 1.0)
    skip_gain = jnp.clip(0.5 + 1.0 * jax.random.uniform(keys[12], (NH,), jnp.float32) ** steps_of(keys[12], (NH,), ((0, 8),), -0.2, 0.2), 0.5, 1.5)
    gate_gain = jnp.clip(1.0 + 0.1 * jax.random.normal(keys[13], (DI,), jnp.float32), 0.5, 1.5)
    out_weight = gaussian(keys[14], (DI, D), DI ** -0.5, 0.09375, ((0, 8),))
    cotangent = gaussian(keys[15], (TOKENS, D), 1.0, 6.0, ((0, 4), (1, 8)))
    return {"hidden_in": hidden_in, "lengths": lengths, "norm_gain": norm_gain, "in_gate_inner": in_gate_inner, "in_step": in_step, "in_shared": in_shared, "conv_inner": conv_inner, "conv_inner_bias": conv_inner_bias, "conv_shared": conv_shared, "conv_shared_bias": conv_shared_bias, "step_bias": step_bias, "log_decay": log_decay, "skip_gain": skip_gain, "gate_gain": gate_gain, "out_weight": out_weight, "cotangent": cotangent}


exact_mode = lax.Precision.HIGHEST
EPSILON = 1e-05

@jax.custom_vjp
def low(v):
    return lax.optimization_barrier(v.astype(jnp.bfloat16)).astype(jnp.float32)

@jax.custom_vjp
def low_back(v):
    return v

def low_keep(v):
    return (low(v), None)

def low_pass(kept, grad):
    return (grad,)

def back_keep(v):
    return (v, None)

def back_low(kept, grad):
    return (low(grad),)
low.defvjp(low_keep, low_pass)
low_back.defvjp(back_keep, back_low)

def segment_ids(length_row, count_tokens):
    bounds = jnp.cumsum(length_row.astype(jnp.int32), dtype=jnp.int32)
    places = jnp.arange(count_tokens, dtype=jnp.int32)
    return lax.optimization_barrier(jnp.sum((places[:, None] >= bounds[None, :]).astype(jnp.int32), axis=1, dtype=jnp.int32))

def conv_silu(values, kernel, biases, segment):
    kernel_width = kernel.shape[0]
    length = values.shape[0]
    padded = jnp.concatenate([jnp.zeros((kernel_width - 1, values.shape[1]), jnp.float32), values], axis=0)
    seg_padded = jnp.concatenate([jnp.full((kernel_width - 1,), -1, jnp.int32), segment], axis=0)
    summed = jnp.zeros_like(values) + biases[None, :]
    for offset in range(kernel_width):
        same_seg = (seg_padded[offset:offset + length] == segment).astype(jnp.float32)
        summed = summed + kernel[offset][None, :] * padded[offset:offset + length] * same_seg[:, None]
    return jax.nn.silu(summed)

def block_step(carried_in, block):
    carry_state, last_seg = carried_in
    inner_blk, write_blk, read_blk, step_blk, decay_blk, seg_blk = block
    block_len = seg_blk.shape[0]
    cumulative = jnp.cumsum(decay_blk, axis=0).T
    places = jnp.arange(block_len)
    causal = (places[:, None] >= places[None, :]) & (seg_blk[:, None] == seg_blk[None, :])
    spread = cumulative[:, :, None] - cumulative[:, None, :]
    factor = jnp.exp(jnp.where(causal[None], spread, -10000.0))
    scores = jnp.einsum('in,jn->ij', read_blk, write_blk, precision=exact_mode)
    mixing = factor * scores[None] * step_blk.T[:, None, :]
    within = jnp.einsum('hij,jhp->ihp', mixing, inner_blk, precision=exact_mode)
    carried = (seg_blk == last_seg).astype(jnp.float32)
    entry_gain = (jnp.exp(cumulative) * carried[None, :]).T
    from_state = jnp.einsum('in,hpn->ihp', read_blk, carry_state, precision=exact_mode) * entry_gain[:, :, None]
    tail_same = (seg_blk == seg_blk[-1]).astype(jnp.float32)
    to_end = jnp.exp(cumulative[:, -1:] - cumulative).T * tail_same[:, None] * step_blk
    weighted = inner_blk * to_end[:, :, None]
    new_state = jnp.einsum('jhp,jn->hpn', weighted, write_blk, precision=exact_mode)
    new_state = new_state + carry_state * (jnp.exp(cumulative[:, -1]) * carried[-1])[:, None, None]
    return ((new_state, seg_blk[-1]), within + from_state)

def mixer(gate_in, inner_raw, shared, step_raw, conv_inner, conv_inner_bias, conv_shared, conv_shared_bias, step_bias, log_decay, skip_gain, segment):
    tokens = inner_raw.shape[0]
    head_count = step_bias.shape[0]
    head_size = inner_raw.shape[1] // head_count
    state_size = shared.shape[1] // 2
    inner_act = conv_silu(inner_raw, conv_inner, conv_inner_bias, segment)
    shared_act = conv_silu(shared, conv_shared, conv_shared_bias, segment)
    write_all = shared_act[:, :state_size]
    read_all = shared_act[:, state_size:]
    step_size = jax.nn.softplus(step_raw + step_bias[None, :])
    decay_log = -jnp.exp(log_decay)[None, :] * step_size
    blocks = tokens // CH
    stacked = (inner_act.reshape(blocks, CH, head_count, head_size), write_all.reshape(blocks, CH, state_size), read_all.reshape(blocks, CH, state_size), step_size.reshape(blocks, CH, head_count), decay_log.reshape(blocks, CH, head_count), segment.reshape(blocks, CH))
    start_state = (jnp.zeros((head_count, head_size, state_size), jnp.float32), jnp.array(-1, jnp.int32))
    last_carry, outputs = lax.scan(jax.checkpoint(block_step), start_state, stacked)
    heads_out = outputs.reshape(tokens, head_count, head_size) + skip_gain[None, :, None] * inner_act.reshape(tokens, head_count, head_size)
    return heads_out.reshape(tokens, head_count * head_size) * jax.nn.silu(gate_in)

def layer(source, norm_gain, in_gate_inner, in_step, in_shared, conv_inner, conv_inner_bias, conv_shared, conv_shared_bias, step_bias, log_decay, skip_gain, gate_gain, out_weight, segment, live_mask):
    inv_rms = lax.rsqrt(lax.optimization_barrier(jnp.mean(source * source, axis=1)) + EPSILON)
    normed = low(source * inv_rms[:, None] * norm_gain[None, :])
    projected = jnp.einsum('td,dke->tke', normed, in_gate_inner, precision=exact_mode)
    gate_in = low_back(projected[:, 0])
    inner_raw = low_back(projected[:, 1])
    step_raw = low_back(jnp.dot(normed, in_step, precision=exact_mode))
    shared = low_back(jnp.dot(normed, in_shared.T, precision=exact_mode))
    gated_out = mixer(gate_in, inner_raw, shared, step_raw, conv_inner, conv_inner_bias, conv_shared, conv_shared_bias, step_bias, log_decay, skip_gain, segment)
    gate_rms = lax.rsqrt(lax.optimization_barrier(jnp.mean(gated_out * gated_out, axis=1)) + EPSILON)
    scaled = low(gated_out * gate_rms[:, None] * gate_gain[None, :])
    mixed_out = jnp.dot(scaled, out_weight, precision=exact_mode)
    return source + live_mask[:, None] * mixed_out

def reference(hidden_in, lengths, norm_gain, in_gate_inner, in_step, in_shared, conv_inner, conv_inner_bias, conv_shared, conv_shared_bias, step_bias, log_decay, skip_gain, gate_gain, out_weight, cotangent):
    params = (norm_gain.astype(jnp.float32), in_gate_inner.astype(jnp.float32), in_step.astype(jnp.float32), in_shared.astype(jnp.float32), conv_inner.astype(jnp.float32), conv_inner_bias.astype(jnp.float32), conv_shared.astype(jnp.float32), conv_shared_bias.astype(jnp.float32), step_bias.astype(jnp.float32), log_decay.astype(jnp.float32), skip_gain.astype(jnp.float32), gate_gain.astype(jnp.float32), out_weight.astype(jnp.float32))
    groups_in = hidden_in.astype(jnp.float32).reshape(GROUPS, TOK_DEV, D)
    groups_back = cotangent.astype(jnp.float32).reshape(GROUPS, TOK_DEV, D)
    zeros_init = tuple((jnp.zeros_like(weight) for weight in params))

    def group_step(running, inputs):
        source, grad_out, length_row = inputs
        segment = segment_ids(length_row, TOK_DEV)
        live_mask = (segment < length_row.shape[0]).astype(jnp.float32)

        def closed(source_in, *weights):
            return layer(source_in, *weights, segment, live_mask)
        result, backward = jax.vjp(closed, source, *params)
        gradients = backward(grad_out)
        running = tuple((so_far + fresh for so_far, fresh in zip(running, gradients[1:])))
        return (running, (result.astype(jnp.bfloat16), gradients[0]))
    totals, (outputs, grad_inputs) = lax.scan(group_step, zeros_init, (groups_in, groups_back, lengths))
    return (outputs.reshape(TOKENS, D), grad_inputs.reshape(TOKENS, D), totals[0], totals[1], totals[2], totals[3], totals[4], totals[5], totals[6], totals[7], totals[8], totals[9], totals[10], totals[11], totals[12])
```

```python
import functools

import jax
import jax.numpy as jnp
from jax import lax
from jax.experimental import pallas as pl
from jax.experimental.pallas import tpu as pltpu
from jax.sharding import PartitionSpec as P


EPSILON = 1e-05
L = 128
LB = 512
NSUB = LB // L
HEAD = 64
STATE = 64
f32 = jnp.float32
bf16 = jnp.bfloat16


def mm(a, b, ca=1, cb=0):
    return lax.dot_general(a, b, (((ca,), (cb,)), ((), ())), preferred_element_type=f32)


def split(x):
    hi = x.astype(bf16)
    return hi, (x - hi.astype(f32)).astype(bf16)


def mm3(a, b, ca=1, cb=0):
    ah, al = split(a)
    bh, bl = split(b)
    return mm(ah, bh, ca, cb) + mm(ah, bl, ca, cb) + mm(al, bh, ca, cb)


def mm_exact_left(mask, x):
    hi = x.astype(bf16)
    rest = x - hi.astype(f32)
    mid = rest.astype(bf16)
    low = (rest - mid.astype(f32)).astype(bf16)
    return mm(mask, hi) + mm(mask, mid) + mm(mask, low)


def block_diag(x, first):
    zero = jnp.zeros_like(x)
    return jnp.concatenate([jnp.where(first, x, zero), jnp.where(first, zero, x)], axis=0)


def bounds_of(len_ref):
    b0 = len_ref[0, 0]
    b1 = b0 + len_ref[0, 1]
    b2 = b1 + len_ref[0, 2]
    b3 = b2 + len_ref[0, 3]
    return b0, b1, b2, b3


def start_of(bounds, t):
    start = jnp.zeros_like(t)
    for b in bounds:
        start = jnp.where(t >= b, b, start)
    return start


def to_row(col):
    return jnp.transpose(jnp.broadcast_to(col, (L, L)))[0:1, :]


def to_col(row):
    return jnp.transpose(jnp.broadcast_to(row, (L, L)))


def pair_cols(a, q, first):
    return jnp.where(first, a[:, 2 * q : 2 * q + 1], a[:, 2 * q + 1 : 2 * q + 2])


def softplus(v):
    return jnp.maximum(v, 0.0) + jnp.log1p(jnp.exp(-jnp.abs(v)))


def shifted(win, m):
    if m == 0:
        return win[8:, :]
    return pltpu.roll(win, m, 0)[8:, :]


def chunk_columns(hp_ref, step, bounds, base):
    tcol = lax.broadcasted_iota(jnp.int32, (L, L), 0) + base
    trow = lax.broadcasted_iota(jnp.int32, (L, L), 1) + base
    start_col = start_of(bounds, tcol)
    start_end = start_of(bounds, base + (L - 1))
    raw = step + hp_ref[0:1, :]
    dt = softplus(raw)
    decay = hp_ref[1:2, :] * dt
    lower = jnp.where(trow <= tcol, 1.0, 0.0).astype(bf16)
    cum = mm_exact_left(lower, decay)
    cum_end = cum[L - 1 : L, :]
    ecum = jnp.where(start_col < base, jnp.exp(cum), 0.0)
    wend = jnp.where(tcol >= start_end, jnp.exp(cum_end - cum), 0.0)
    carried_end = (start_end < base).astype(f32)
    cdec = jnp.exp(cum_end) * carried_end
    return tcol, trow, start_col, start_end, raw, dt, decay, cum, ecum, wend, cdec


def fwd_kernel(
    len_ref, h_ref, gain_ref, wgi_ref, wss_ref, cp_ref, sp_ref, hp_ref,
    normed_ref, inv_ref, gate_ref, rest_ref, gated_ref, y_ref, st_ref, gsum_ref,
    vbuf, state,
):
    blk = pl.program_id(0)
    width = gate_ref.shape[1]
    full = h_ref.shape[1]
    pairs = width // L

    @pl.when(blk == 0)
    def _():
        vbuf[0:8, :] = jnp.zeros((8, vbuf.shape[1]), f32)
        state[...] = jnp.zeros(state.shape, f32)

    piece = 256

    def norm_rows(s, carry):
        rows = pl.ds(pl.multiple_of(s * L, L), L)
        acc = jnp.zeros((L, piece), f32)
        for k in range(full // piece):
            x = h_ref[rows, k * piece : (k + 1) * piece].astype(f32)
            acc = acc + x * x
        inv = lax.rsqrt(jnp.sum(acc, axis=1, keepdims=True) / full + EPSILON)
        for k in range(full // piece):
            cols = slice(k * piece, (k + 1) * piece)
            x = h_ref[rows, cols].astype(f32)
            normed_ref[rows, cols] = (x * inv * gain_ref[0:1, cols]).astype(bf16)
        inv_ref[s] = to_row(inv)
        return carry

    lax.fori_loop(0, NSUB, norm_rows, 0)
    normed = normed_ref[...]
    gate_ref[...] = mm(normed, wgi_ref[:, :width])
    inner = mm(normed, wgi_ref[:, width:])
    vbuf[8:, :width] = inner
    rest_ref[:, :width] = inner
    tail = mm(normed, wss_ref[...])
    vbuf[8:, width:] = tail[:, :L]
    rest_ref[:, width:] = tail

    bounds = bounds_of(len_ref)
    first = lax.broadcasted_iota(jnp.int32, (L, L), 1) < HEAD

    def chunk(s, carry):
        r0 = pl.multiple_of(s * L, L)
        rows = pl.ds(r0, L)
        base = blk * LB + s * L
        step = rest_ref[rows, width + L :]
        tcol, trow, start_col, _, _, dt, _, cum, ecum, wend, cdec = chunk_columns(
            hp_ref, step, bounds, base
        )
        cum_t = jnp.transpose(cum)
        mask = (trow <= tcol) & (trow >= start_col)
        valid = [tcol - m >= start_col for m in range(4)]

        def conv(cols, taps):
            win = vbuf[pl.ds(r0, L + 8), cols]
            pre = taps[4:5, :] + taps[3:4, :] * win[8:, :]
            for m in range(1, 4):
                pre = pre + taps[3 - m : 4 - m, :] * jnp.where(valid[m], shifted(win, m), 0.0)
            return pre

        pre_s = conv(slice(width, width + L), sp_ref)
        act = pre_s * lax.logistic(pre_s)
        b_map = act[:, :STATE]
        c_map = act[:, STATE:]
        scores = jnp.where(mask, mm3(c_map, b_map, 1, 1), 0.0)
        square = jnp.zeros((L, L), f32)
        for q in range(pairs):
            cols = slice(q * L, (q + 1) * L)
            pre = conv(cols, cp_ref.at[:, cols])
            xin = pre * lax.logistic(pre)
            xp = xin * pair_cols(dt, q, first)
            xh, xl = split(xp)
            bdh, bdl = block_diag(xh, first), block_diag(xl, first)
            mix = []
            for h in (2 * q, 2 * q + 1):
                spread = jnp.minimum(cum[:, h : h + 1] - cum_t[h : h + 1, :], 0.0)
                mix.append(jnp.exp(spread) * scores)
            mh, ml = split(jnp.concatenate(mix, axis=1))
            both = mm(mh, jnp.concatenate([bdh, bdl], axis=1))
            y = both[:, :L] + both[:, L:] + mm(ml, bdh)
            st = state[:, cols]
            st_ref[s, :, cols] = st
            y = y + mm3(c_map, st) * pair_cols(ecum, q, first)
            xw = xp * pair_cols(wend, q, first)
            state[:, cols] = mm3(b_map, xw, 0, 0) + st * pair_cols(cdec, q, first[0:1, :])
            y_ref[rows, cols] = y
            gate = gate_ref[rows, cols]
            gated = (y + cp_ref[5:6, cols] * xin) * (gate * lax.logistic(gate))
            gated_ref[rows, cols] = gated
            square = square + gated * gated
        gsum_ref[s] = to_row(jnp.sum(square, axis=1, keepdims=True))
        return carry

    lax.fori_loop(0, NSUB, chunk, 0)
    vbuf[0:8, :] = vbuf[LB : LB + 8, :]


def mid_kernel(len_ref, cot_ref, w_ref, gated_ref, cp_ref, gs_ref, gdot_ref):
    blk = pl.program_id(0)
    live = bounds_of(len_ref)[3]
    t = lax.broadcasted_iota(jnp.int32, gs_ref.shape, 0) + blk * LB
    gs = jnp.where(t < live, mm(cot_ref[...], w_ref[...], 1, 1), 0.0)
    gs_ref[...] = gs
    dots = jnp.sum(gs * cp_ref[6:7, :] * gated_ref[...], axis=1, keepdims=True)
    for s in range(NSUB):
        gdot_ref[s] = to_row(dots[s * L : (s + 1) * L, :])


def bwd_kernel(
    inner_total,
    len_ref, gate_ref, rest_ref, halo_ref, gs_ref, y_ref, st_ref, gsum_ref, gdot_ref,
    cp_ref, sp_ref, hp_ref,
    low_ref, gsh_ref, nd_ref, size_ref, pg_ref, sg_ref, hg_ref,
    vbuf, qnext, adj, send,
):
    step_id = pl.program_id(0)
    blk = pl.num_programs(0) - 1 - step_id
    width = gate_ref.shape[1]
    pairs = width // L

    @pl.when(step_id == 0)
    def _():
        qnext[...] = jnp.zeros(qnext.shape, f32)
        adj[...] = jnp.zeros(adj.shape, f32)
        send[...] = jnp.zeros(send.shape, f32)
        pg_ref[...] = jnp.zeros(pg_ref.shape, f32)
        sg_ref[...] = jnp.zeros(sg_ref.shape, f32)
        hg_ref[...] = jnp.zeros(hg_ref.shape, f32)

    vbuf[0:8, :] = halo_ref[:, : width + L]
    vbuf[8:, :] = rest_ref[:, : width + L]
    bounds = bounds_of(len_ref)
    first = lax.broadcasted_iota(jnp.int32, (L, L), 1) < HEAD
    lane = lax.broadcasted_iota(jnp.int32, (L, L), 1)
    half = lax.broadcasted_iota(jnp.int32, (L, L), 0) // HEAD

    def chunk(i, carry):
        s = NSUB - 1 - i
        r0 = pl.multiple_of(s * L, L)
        rows = pl.ds(r0, L)
        base = blk * LB + s * L
        step = rest_ref[rows, width + L :]
        tcol, trow, start_col, start_end, raw, dt, decay, cum, ecum, wend, cdec = chunk_columns(
            hp_ref, step, bounds, base
        )
        cum_t = jnp.transpose(cum)
        mask_t = (trow >= tcol) & (start_of(bounds, trow) <= tcol)
        valid = [tcol - m >= start_col for m in range(4)]
        valid_up = [start_of(bounds, tcol + m) <= tcol for m in range(4)]
        gate_rms_row = lax.rsqrt(gsum_ref[s] / inner_total + EPSILON)
        pull_row = gate_rms_row * gate_rms_row * gate_rms_row * gdot_ref[s] / inner_total
        gate_rms = to_col(gate_rms_row)
        pull = to_col(pull_row)

        def conv(cols, taps):
            win = vbuf[pl.ds(r0, L + 8), cols]
            seen = [win[8:, :]]
            pre = taps[4:5, :] + taps[3:4, :] * seen[0]
            for m in range(1, 4):
                seen.append(jnp.where(valid[m], shifted(win, m), 0.0))
                pre = pre + taps[3 - m : 4 - m, :] * seen[m]
            return seen, pre

        def conv_back(q, seen, cols, taps, grad_ref, grad_cols):
            win = jnp.concatenate([q, qnext[:, cols]], axis=0)
            qnext[:, cols] = q[0:8, :]
            grad = taps[3:4, :] * q
            for m in range(1, 4):
                up = pltpu.roll(win, L + 8 - m, 0)[:L, :]
                grad = grad + taps[3 - m : 4 - m, :] * jnp.where(valid_up[m], up, 0.0)
            for m in range(4):
                k = 3 - m
                grad_ref[k : k + 1, grad_cols] += jnp.sum(q * seen[m], axis=0, keepdims=True)
            grad_ref[4:5, grad_cols] += jnp.sum(q, axis=0, keepdims=True)
            return grad

        seen_s, pre_s = conv(slice(width, width + L), sp_ref)
        sig_s = lax.logistic(pre_s)
        act = pre_s * sig_s
        b_map = act[:, :STATE]
        c_map = act[:, STATE:]
        scores_t = jnp.where(mask_t, mm3(b_map, c_map, 1, 1), 0.0)
        d_scores = jnp.zeros((L, L), f32)
        d_b = jnp.zeros((L, STATE), f32)
        d_c = jnp.zeros((L, STATE), f32)
        reduced = jnp.zeros((2 * L, L), f32)
        ends = jnp.zeros((8, L), f32)
        norm_dot = jnp.zeros((L, L), f32)
        size = jnp.zeros((L, L), f32)
        for q in range(pairs):
            cols = slice(q * L, (q + 1) * L)
            taps = cp_ref.at[:, cols]
            skip = cp_ref[5:6, cols]
            seen, pre = conv(cols, taps)
            sig = lax.logistic(pre)
            xin = pre * sig
            dtx = pair_cols(dt, q, first)
            xp = xin * dtx
            y = y_ref[rows, cols]
            ho = y + skip * xin
            gate = gate_ref[rows, cols]
            gsig = lax.logistic(gate)
            sl = gate * gsig
            gated = ho * sl
            gs = gs_ref[rows, cols]
            pg_ref[6:7, cols] += jnp.sum(gs * gated * gate_rms, axis=0, keepdims=True)
            gg = gate_rms * cp_ref[6:7, cols] * gs - gated * pull
            gy = gg * sl
            low_gate = (gg * ho * (gsig * (1.0 + gate * (1.0 - gsig)))).astype(bf16)
            low_ref[rows, cols] = low_gate
            pg_ref[5:6, cols] += jnp.sum(gy * xin, axis=0, keepdims=True)

            yh, yl = split(gy)
            bdh, bdl = block_diag(yh, first), block_diag(yl, first)
            xh, xl = split(xp)
            d_mix = mm(
                jnp.concatenate([xh, xl], axis=1), jnp.concatenate([bdh, bdh], axis=1), 1, 1
            ) + mm(xh, bdl, 1, 1)
            mix = []
            for k in range(2):
                h = 2 * q + k
                spread = jnp.minimum(cum_t[h : h + 1, :] - cum[:, h : h + 1], 0.0)
                factor = jnp.exp(spread)
                d_scores = d_scores + d_mix[:, k * L : (k + 1) * L] * factor
                mix.append(factor * scores_t)
            mh, ml = split(jnp.concatenate(mix, axis=1))
            both = mm(mh, jnp.concatenate([bdh, bdl], axis=1))
            dxp = both[:, :L] + both[:, L:] + mm(ml, bdh)
            wendx = pair_cols(wend, q, first)
            a_in = adj[:, cols]
            dxp = dxp + mm3(b_map, a_in) * wendx
            xw = xp * wendx
            gyw = gy * pair_cols(ecum, q, first)
            s_in = st_ref[s, :, cols]
            d_b = d_b + mm3(xw, a_in, 1, 1)
            d_c = d_c + mm3(gyw, s_in, 1, 1)
            adj[:, cols] = mm3(c_map, gyw, 0, 0) + a_in * pair_cols(cdec, q, first[0:1, :])
            heads = jnp.where(lane == 2 * q + half, 1.0, 0.0).astype(bf16)
            zh, zl = split(jnp.concatenate([gy * y - dxp * xp, dxp * xin], axis=0))
            reduced = reduced + mm(zh, heads) + mm(zl, heads)
            end = jnp.broadcast_to(
                jnp.sum(a_in * send[:, cols], axis=0, keepdims=True), (8, L)
            )
            eh, el = split(end)
            ends = ends + mm(eh, heads) + mm(el, heads)
            send[:, cols] = s_in

            dxin = dxp * dtx + skip * gy
            qv = dxin * (sig * (1.0 + pre * (1.0 - sig)))
            grad = conv_back(qv, seen, cols, taps, pg_ref, cols)
            low_inner = grad.astype(bf16)
            low_ref[rows, width + q * L : width + (q + 1) * L] = low_inner
            wide_gate, wide_inner = low_gate.astype(f32), low_inner.astype(f32)
            norm_dot = norm_dot + wide_gate * gate + wide_inner * seen[0]
            size = size + wide_gate * wide_gate + wide_inner * wide_inner

        d_scores = jnp.where(mask_t, d_scores, 0.0)
        d_b = d_b + mm3(d_scores, c_map)
        d_c = d_c + mm3(d_scores, b_map, 0, 0)
        d_act = jnp.concatenate([d_b, d_c], axis=1)
        q_s = d_act * (sig_s * (1.0 + pre_s * (1.0 - sig_s)))
        shared_cols = slice(width, width + L)
        gsh_ref[rows, :] = conv_back(q_s, seen_s, shared_cols, sp_ref, sg_ref, slice(0, L))

        tail = jnp.where(tcol >= start_end, ends[0:1, :], 0.0)
        keep = jnp.where(mask_t, 1.0, 0.0).astype(bf16)
        d_decay = mm_exact_left(keep, reduced[:L, :]) + tail
        d_dt = reduced[L:, :] + d_decay * hp_ref[1:2, :]
        d_raw = d_dt * lax.logistic(raw)
        hg_ref[0:1, :] += jnp.sum(d_raw, axis=0, keepdims=True)
        hg_ref[1:2, :] += jnp.sum(d_decay * decay, axis=0, keepdims=True)
        low_step = d_raw.astype(bf16)
        low_ref[rows, 2 * width :] = low_step
        wide_step = low_step.astype(f32)
        norm_dot = norm_dot + wide_step * step
        size = size + wide_step * wide_step
        nd_ref[s] = to_row(jnp.sum(norm_dot, axis=1, keepdims=True))
        size_ref[s] = to_row(jnp.sum(size, axis=1, keepdims=True))
        return carry

    lax.fori_loop(0, NSUB, chunk, 0)


def unpack_kernel(x_ref, gate_inner_ref, step_ref):
    width = gate_inner_ref.shape[2]
    gate_inner_ref[:, 0, :] = x_ref[:, :width]
    gate_inner_ref[:, 1, :] = x_ref[:, width : 2 * width]
    step_ref[...] = x_ref[:, 2 * width : 2 * width + step_ref.shape[1]]


def unpack(x, width, heads):
    rows = x.shape[0]
    return pl.pallas_call(
        unpack_kernel,
        grid=(rows // 256,),
        in_specs=[pl.BlockSpec((256, x.shape[1]), lambda i: (i, 0))],
        out_specs=[
            pl.BlockSpec((256, 2, width), lambda i: (i, 0, 0)),
            pl.BlockSpec((256, heads), lambda i: (i, 0)),
        ],
        out_shape=[
            jax.ShapeDtypeStruct((rows, 2, width), f32),
            jax.ShapeDtypeStruct((rows, heads), f32),
        ],
        name="unpack",
    )(x)


def rows_spec(cols, order):
    return pl.BlockSpec((LB, cols), lambda i: (order(i), 0))


def line_spec(order):
    return pl.BlockSpec((NSUB, 1, L), lambda i: (order(i), 0, 0))


def whole_spec(shape):
    return pl.BlockSpec(shape, lambda i: (0,) * len(shape), pipeline_mode=pl.Buffered(1))


def smem_spec():
    return pl.BlockSpec(memory_space=pltpu.SMEM)


VMEM_LIMIT = 60 * 1024 * 1024


def run_fwd(lengths, hidden, gain, wgi, wss, cp, sp, hp):
    tokens, full = hidden.shape
    width = wgi.shape[1] // 2
    lines = tokens // L

    def same(i):
        return i

    return pl.pallas_call(
        fwd_kernel,
        grid=(tokens // LB,),
        in_specs=[
            smem_spec(),
            rows_spec(full, same),
            whole_spec(gain.shape),
            whole_spec(wgi.shape),
            whole_spec(wss.shape),
            whole_spec(cp.shape),
            whole_spec(sp.shape),
            whole_spec(hp.shape),
        ],
        out_specs=[
            rows_spec(full, same),
            line_spec(same),
            rows_spec(width, same),
            rows_spec(width + 2 * L, same),
            rows_spec(width, same),
            rows_spec(width, same),
            pl.BlockSpec((NSUB, STATE, width), lambda i: (i, 0, 0)),
            line_spec(same),
        ],
        out_shape=[
            jax.ShapeDtypeStruct((tokens, full), bf16),
            jax.ShapeDtypeStruct((lines, 1, L), f32),
            jax.ShapeDtypeStruct((tokens, width), f32),
            jax.ShapeDtypeStruct((tokens, width + 2 * L), f32),
            jax.ShapeDtypeStruct((tokens, width), f32),
            jax.ShapeDtypeStruct((tokens, width), f32),
            jax.ShapeDtypeStruct((lines, STATE, width), f32),
            jax.ShapeDtypeStruct((lines, 1, L), f32),
        ],
        scratch_shapes=[
            pltpu.VMEM((LB + 8, width + L), f32),
            pltpu.VMEM((STATE, width), f32),
        ],
        compiler_params=pltpu.CompilerParams(
            dimension_semantics=("arbitrary",), vmem_limit_bytes=VMEM_LIMIT
        ),
        name="mixer_fwd",
    )(lengths, hidden, gain, wgi, wss, cp, sp, hp)


def run_mid(lengths, cot, w_out, gated, cp):
    tokens, full = cot.shape
    width = gated.shape[1]
    lines = tokens // L

    def same(i):
        return i

    return pl.pallas_call(
        mid_kernel,
        grid=(tokens // LB,),
        in_specs=[
            smem_spec(),
            rows_spec(full, same),
            whole_spec(w_out.shape),
            rows_spec(width, same),
            whole_spec(cp.shape),
        ],
        out_specs=[rows_spec(width, same), line_spec(same)],
        out_shape=[
            jax.ShapeDtypeStruct((tokens, width), f32),
            jax.ShapeDtypeStruct((lines, 1, L), f32),
        ],
        compiler_params=pltpu.CompilerParams(
            dimension_semantics=("arbitrary",), vmem_limit_bytes=VMEM_LIMIT
        ),
        name="mixer_mid",
    )(lengths, cot, w_out, gated, cp)


def run_bwd(inner_total, lengths, gate, rest, gs, y, st, gsum, gdot, cp, sp, hp):
    tokens, width = gate.shape
    lines = tokens // L
    blocks = tokens // LB

    def back(i):
        return blocks - 1 - i

    def halo(i):
        return (jnp.maximum(back(i) * (LB // 8) - 1, 0), 0)

    return pl.pallas_call(
        functools.partial(bwd_kernel, float(inner_total)),
        grid=(blocks,),
        in_specs=[
            smem_spec(),
            rows_spec(width, back),
            rows_spec(width + 2 * L, back),
            pl.BlockSpec((8, width + 2 * L), halo),
            rows_spec(width, back),
            rows_spec(width, back),
            pl.BlockSpec((NSUB, STATE, width), lambda i: (back(i), 0, 0)),
            line_spec(back),
            line_spec(back),
            whole_spec(cp.shape),
            whole_spec(sp.shape),
            whole_spec(hp.shape),
        ],
        out_specs=[
            rows_spec(2 * width + L, back),
            rows_spec(L, back),
            line_spec(back),
            line_spec(back),
            pl.BlockSpec((8, width), lambda i: (0, 0)),
            pl.BlockSpec((8, L), lambda i: (0, 0)),
            pl.BlockSpec((8, L), lambda i: (0, 0)),
        ],
        out_shape=[
            jax.ShapeDtypeStruct((tokens, 2 * width + L), bf16),
            jax.ShapeDtypeStruct((tokens, L), f32),
            jax.ShapeDtypeStruct((lines, 1, L), f32),
            jax.ShapeDtypeStruct((lines, 1, L), f32),
            jax.ShapeDtypeStruct((8, width), f32),
            jax.ShapeDtypeStruct((8, L), f32),
            jax.ShapeDtypeStruct((8, L), f32),
        ],
        scratch_shapes=[
            pltpu.VMEM((LB + 8, width + L), f32),
            pltpu.VMEM((8, width + L), f32),
            pltpu.VMEM((STATE, width), f32),
            pltpu.VMEM((STATE, width), f32),
        ],
        compiler_params=pltpu.CompilerParams(
            dimension_semantics=("arbitrary",), vmem_limit_bytes=VMEM_LIMIT
        ),
        name="mixer_bwd",
    )(lengths, gate, rest, rest, gs, y, st, gsum, gdot, cp, sp, hp)


def pack_params(conv_inner, conv_inner_bias, conv_shared, conv_shared_bias, step_bias, log_decay,
                skip_gain, gate_gain):
    width = conv_inner.shape[1]
    heads = step_bias.shape[0]
    skip = jnp.repeat(skip_gain, HEAD)
    cp = jnp.concatenate(
        [conv_inner, conv_inner_bias[None], skip[None], gate_gain[None], jnp.zeros((1, width), f32)],
        axis=0,
    )
    sp = jnp.concatenate([conv_shared, conv_shared_bias[None], jnp.zeros((3, L), f32)], axis=0)
    hp = jnp.zeros((8, L), f32)
    hp = hp.at[0, :heads].set(step_bias).at[1, :heads].set(-jnp.exp(log_decay))
    return cp, sp, hp


def exchange_kernel(axis, x_ref, out_ref, slots, send_sem, recv_sem):
    me = lax.axis_index(axis)
    n = slots.shape[0]
    barrier = pltpu.get_barrier_semaphore()
    for k in range(1, n):
        peer = lax.rem(me + k, n)
        pl.semaphore_signal(barrier, inc=1, device_id={axis: peer})
    pl.semaphore_wait(barrier, n - 1)
    copies = []
    for k in range(1, n):
        peer = lax.rem(me + k, n)
        copy = pltpu.make_async_remote_copy(
            src_ref=x_ref,
            dst_ref=slots.at[k],
            send_sem=send_sem.at[k],
            recv_sem=recv_sem.at[k],
            device_id={axis: peer},
        )
        copy.start()
        copies.append(copy)
    for copy in copies:
        copy.wait()
    slots[0] = x_ref[...]
    total = slots[lax.rem(me, n)]
    for d in range(1, n):
        total = total + slots[lax.rem(me - d + n, n)]
    out_ref[...] = total


def sum_small(x, axis, collective_id):
    n = lax.axis_size(axis)
    return pl.pallas_call(
        functools.partial(exchange_kernel, axis),
        out_shape=jax.ShapeDtypeStruct(x.shape, f32),
        in_specs=[pl.BlockSpec(memory_space=pltpu.VMEM)],
        out_specs=pl.BlockSpec(memory_space=pltpu.VMEM),
        scratch_shapes=[
            pltpu.VMEM((n,) + x.shape, f32),
            pltpu.SemaphoreType.DMA((n,)),
            pltpu.SemaphoreType.DMA((n,)),
        ],
        compiler_params=pltpu.CompilerParams(collective_id=collective_id, has_side_effects=True),
        name="sum_small",
    )(x)


def after(x, *deps):
    deps = [d for d in deps if d is not None]
    return lax.optimization_barrier((x, *deps))[0]


SCALE = 16384.0


def encode(x, bound, kind):
    if bound is not None:
        x = x * (SCALE / bound)
    return x.astype(kind)


def decode(x, bound):
    x = x.astype(f32)
    return x if bound is None else x * (bound / SCALE)


class ScatterLine:

    def __init__(self, send, own, bound, kind):
        self.n = lax.axis_size("heads")
        self.chips = self.n // 2
        self.z = lax.axis_index("heads") >> 1
        self.own, self.kind, self.bound = own, kind, bound
        self.moving, self.out = [None, None], [None, None]
        self.message = encode(send, bound, kind)

    def swap(self):
        pairs = [(i, i ^ 1) for i in range(self.n)]
        self.got = lax.ppermute(self.message, "heads", pairs)

    def block(self, b):
        mine = lax.dynamic_index_in_dim(self.own, b, 0, keepdims=False)
        theirs = lax.dynamic_index_in_dim(self.got, b, 0, keepdims=False)
        return mine + decode(theirs, self.bound)

    def pack(self, r):
        last = self.chips - 1
        for way in range(2):
            b = last - r + self.z if way == 0 else r - last + self.z
            total = self.block(jnp.clip(b, 0, last))
            if r > 0:
                total = total + decode(self.moving[way], self.bound)
            self.out[way] = encode(total, self.bound, self.kind)

    def hold(self, *deps):
        self.moving = [after(m, *deps) for m in self.moving]

    def send(self, r):
        last = self.chips - 1
        out = lax.optimization_barrier(tuple(self.out))
        for way in range(2):
            chips = range(r + 1) if way == 0 else range(last - r, last + 1)
            hop = 2 if way == 0 else -2
            pairs = [(2 * k + c, 2 * k + c + hop) for k in chips for c in range(2)]
            self.moving[way] = lax.ppermute(out[way], "heads", pairs)
        self.moving = list(lax.optimization_barrier(tuple(self.moving)))

    def rest(self, r):
        for k in range(r, self.chips - 1):
            self.pack(k)
            self.send(k)

    def total(self):
        total = self.block(self.z)
        for way in range(2):
            if self.moving[way] is not None:
                total = total + decode(self.moving[way], self.bound)
        return total


class RowSum:

    def __init__(self, x, bound):
        self.n = lax.axis_size("rows")
        self.me = lax.axis_index("rows")
        self.bits = self.n.bit_length() - 1
        self.shape, self.bound = x.shape, bound
        piece = x.shape[0] // (2 * self.n)
        cut = x.reshape((2,) + (2,) * self.bits + (piece, x.shape[1]))
        self.cur = [cut[0], cut[1]]
        self.order = [[(k + part) % self.bits for k in range(self.bits)] for part in range(2)]
        self.left = [list(range(self.bits))[::-1] for _ in range(2)]

    def pairs(self, bit):
        return [(i, i ^ (1 << bit)) for i in range(self.n)]

    def reduce(self):
        for k in range(self.bits):
            for part in range(2):
                bit, left = self.order[part][k], self.left[part]
                mine = (self.me >> bit) & 1
                axis = left.index(bit)
                left.remove(bit)
                cur = self.cur[part]
                send = lax.dynamic_index_in_dim(cur, 1 - mine, axis, keepdims=False)
                keep = lax.dynamic_index_in_dim(cur, mine, axis, keepdims=False)
                got = lax.ppermute(encode(send, self.bound, jnp.float16), "rows", self.pairs(bit))
                self.cur[part] = keep + decode(got, self.bound)

    def spread(self):
        mine = jnp.stack([encode(cur, self.bound, jnp.float16) for cur in self.cur])
        every = lax.all_gather(mine, "rows", axis=1, tiled=True)
        return decode(every.reshape(self.shape), self.bound)


def per_device(
    hidden_in, lengths, norm_gain, in_gate_inner, in_step, in_shared, conv_inner, conv_inner_bias,
    conv_shared, conv_shared_bias, step_bias, log_decay, skip_gain, gate_gain, out_weight, cotangent,
):
    tokens, local = hidden_in.shape
    full = in_gate_inner.shape[0]
    width = in_gate_inner.shape[2]
    heads = step_bias.shape[0]
    chips = full // local // 2
    lines = tokens // L
    inner_total = width * (full // local)
    core = lax.axis_index("heads") & 1
    source = hidden_in.astype(f32)

    hidden_all = lax.all_gather(hidden_in, "heads", axis=1, tiled=True)
    shared_all = lax.all_gather(in_shared, "heads", axis=1, tiled=True)
    gain_all = lax.all_gather(norm_gain, "heads", axis=0, tiled=True)
    cot_all = lax.all_gather(cotangent, "heads", axis=1, tiled=True)
    wgi = in_gate_inner.reshape(full, 2 * width)
    step_pad = jnp.pad(in_step, ((0, 0), (0, L - heads)))
    wss = jnp.concatenate([shared_all.T, step_pad], axis=1)
    w_back = jnp.concatenate([wgi, step_pad], axis=1)

    def halves(w, axis):
        both = []
        for side in (1 - core, core):
            parts = [
                lax.dynamic_slice_in_dim(w, (2 * k + side) * local, local, axis) for k in range(chips)
            ]
            both.append(jnp.stack(parts))
        return both

    back_send, back_own = halves(w_back, 0)
    out_send, out_own = halves(out_weight, 1)
    w_size = jnp.sqrt(jnp.max(jnp.sum(jnp.square(w_back.astype(f32)), axis=1)))
    cp, sp, hp = pack_params(
        conv_inner, conv_inner_bias, conv_shared, conv_shared_bias, step_bias, log_decay,
        skip_gain, gate_gain,
    )

    hidden_all = after(hidden_all, back_send, back_own, out_send, out_own, w_size, cp, sp, hp)
    normed, inv_rows, gate, rest, gated, y, st, gsum_part = run_fwd(
        lengths, hidden_all, gain_all[None], wgi, wss, cp, sp, hp
    )
    inv_rms = inv_rows.reshape(tokens)
    gsum = sum_small(gsum_part.reshape(lines, L), "heads", 1)

    live = (jnp.arange(tokens, dtype=jnp.int32) < jnp.sum(lengths[0])).astype(bf16)
    gate_rms = lax.rsqrt(gsum.reshape(tokens) / inner_total + EPSILON)
    scaled = (gated * gate_rms[:, None] * gate_gain[None, :]).astype(bf16) * live[:, None]

    def project(w, v, axis):
        return lax.dot_general(w, v, (((axis,), (1,)), ((), ())), preferred_element_type=f32)

    mixed = ScatterLine(
        project(out_send, scaled, 1), project(out_own, scaled, 1), None, jnp.float16
    )
    mixed.swap()
    mixed.pack(0)
    cot_late = after(cot_all, *mixed.out)
    mixed.send(0)
    gs, gdot_part = run_mid(lengths, cot_late, out_weight, gated, cp)
    gdot = sum_small(gdot_part.reshape(lines, L), "heads", 2)
    mixed.hold(gdot)
    mixed.pack(1)
    gdot = after(gdot, *mixed.out)
    mixed.send(1)

    low, gsh_part, nd_part, size, pg, sg, hg = run_bwd(
        inner_total, lengths, gate, rest, gs, y, st, gsum.reshape(lines, 1, L),
        gdot.reshape(lines, 1, L), cp, sp, hp,
    )
    bound = jnp.sqrt(size.reshape(lines, L)) * (1.01 * w_size) + 1e-30
    mixed.hold(low)
    small = sum_small(
        jnp.concatenate([nd_part.reshape(lines, L), bound, sg], axis=0), "heads", 3
    )
    norm_dot, sg = small[:lines].reshape(tokens), small[2 * lines :]
    bound = small[lines : 2 * lines].reshape(tokens)
    low = after(low, bound)

    normal = ScatterLine(project(back_send, low, 2), project(back_own, low, 2), bound, jnp.float16)
    normal.swap()
    normal.pack(0)
    low_late = after(low, *normal.out)
    scaled_late = after(scaled, *normal.out)
    normal.send(0)
    mixed.hold(*normal.out)
    mixed.rest(2)
    output = (source + mixed.total().T).astype(bf16)

    grad_proj = lax.dot_general(
        normed, low_late, (((0,), (0,)), ((), ())), preferred_element_type=f32
    )
    top_proj = jnp.max(jnp.abs(grad_proj))
    grad_wout = lax.dot_general(
        scaled_late, cot_all, (((0,), (0,)), ((), ())), preferred_element_type=f32
    )
    top_wout = jnp.max(jnp.abs(grad_wout))
    tops = jnp.stack([top_proj, top_wout])
    tops = jnp.broadcast_to(jnp.repeat(tops * 1.01 + 1e-30, 8)[:, None], (16, L))
    wide = pg.reshape(8 * width // L, L)
    small = sum_small(jnp.concatenate([tops, sg, hg, wide], axis=0), "rows", 4)
    top_proj, top_wout, sg, hg = small[0, 0], small[8, 0], small[16:24], small[24:32]
    pg = small[32:].reshape(8, width)
    sum_proj, sum_wout = RowSum(grad_proj, top_proj), RowSum(grad_wout, top_wout)
    sum_proj.reduce()
    sum_wout.reduce()

    cut = gsh_part.T.reshape(chips, 2, L // (2 * chips), tokens)
    gsh_own = lax.dynamic_index_in_dim(cut, core, 1, keepdims=False)
    gsh_send = lax.dynamic_index_in_dim(cut, 1 - core, 1, keepdims=False)
    shared = ScatterLine(gsh_send, gsh_own, None, f32)
    shared.swap()
    shared.rest(0)
    low_shared = lax.all_gather(shared.total().astype(bf16), "heads", axis=0, tiled=True)
    shared_raw = rest[:, width : width + L]
    norm_dot = norm_dot + jnp.sum(low_shared.T.astype(f32) * shared_raw, axis=1)
    grad_proj, grad_step = unpack(sum_proj.spread(), width, heads)
    grad_wout = sum_wout.spread()
    normed_local = (source * inv_rms[:, None] * norm_gain[None, :]).astype(bf16)
    grad_shared_w = lax.dot_general(
        low_shared, normed_local, (((1,), (0,)), ((), ())), preferred_element_type=f32
    )
    grad_shared_w = lax.psum(grad_shared_w, "rows")

    normal.rest(1)
    grad_normed = normal.total() + lax.dot_general(
        in_shared, low_shared, (((0,), (0,)), ((), ())), preferred_element_type=f32
    )
    grad_normed = grad_normed.T
    grad_gain_norm = jnp.sum(grad_normed * source * inv_rms[:, None], axis=0)
    grad_source = (
        inv_rms[:, None] * norm_gain[None, :] * grad_normed
        - source * (inv_rms * inv_rms * norm_dot / full)[:, None]
    )
    grad_input = cotangent.astype(f32) + grad_source
    grad_gain_norm = sum_small(grad_gain_norm.reshape(local // L, L), "rows", 5).reshape(local)
    return (
        output,
        grad_input,
        grad_gain_norm,
        grad_proj,
        grad_step,
        grad_shared_w,
        pg[0:4],
        pg[4],
        sg[0:4],
        sg[4],
        hg[0, :heads],
        hg[1, :heads],
        pg[5].reshape(heads, HEAD).sum(axis=1),
        pg[6],
        grad_wout,
    )


def solution(mesh):
    return jax.shard_map(
        per_device,
        mesh=mesh,
        in_specs=(
            P("rows", "heads"), P("rows", None), P("heads"), P(None, None, "heads"),
            P(None, "heads"), P(None, "heads"), P(None, "heads"), P("heads"), P(), P(),
            P("heads"), P("heads"), P("heads"), P("heads"), P("heads", None), P("rows", "heads"),
        ),
        out_specs=(
            P("rows", "heads"), P("rows", "heads"), P("heads"), P(None, None, "heads"),
            P(None, "heads"), P(None, "heads"), P(None, "heads"), P("heads"), P(), P(),
            P("heads"), P("heads"), P("heads"), P("heads"), P("heads", None),
        ),
        check_vma=False,
    )
```

```python
import functools

import jax
import jax.numpy as jnp
from jax import lax
from jax.experimental import pallas as pl
from jax.experimental.pallas import tpu as pltpu
from jax.sharding import PartitionSpec as P


EPSILON = 1e-05
L = 128
LB = 512
NSUB = LB // L
HEAD = 64
STATE = 64
f32 = jnp.float32
bf16 = jnp.bfloat16


def mm(a, b, ca=1, cb=0):
    return lax.dot_general(a, b, (((ca,), (cb,)), ((), ())), preferred_element_type=f32)


def split(x):
    hi = x.astype(bf16)
    return hi, (x - hi.astype(f32)).astype(bf16)


def mm3(a, b, ca=1, cb=0):
    ah, al = split(a)
    bh, bl = split(b)
    return mm(ah, bh, ca, cb) + mm(ah, bl, ca, cb) + mm(al, bh, ca, cb)


def mm_exact_left(mask, x):
    hi = x.astype(bf16)
    rest = x - hi.astype(f32)
    mid = rest.astype(bf16)
    low = (rest - mid.astype(f32)).astype(bf16)
    return mm(mask, hi) + mm(mask, mid) + mm(mask, low)


def block_diag(x, first):
    zero = jnp.zeros_like(x)
    return jnp.concatenate([jnp.where(first, x, zero), jnp.where(first, zero, x)], axis=0)


def bounds_of(len_ref):
    b0 = len_ref[0, 0]
    b1 = b0 + len_ref[0, 1]
    b2 = b1 + len_ref[0, 2]
    b3 = b2 + len_ref[0, 3]
    return b0, b1, b2, b3


def start_of(bounds, t):
    start = jnp.zeros_like(t)
    for b in bounds:
        start = jnp.where(t >= b, b, start)
    return start


def to_row(col):
    return jnp.transpose(jnp.broadcast_to(col, (L, L)))[0:1, :]


def to_col(row):
    return jnp.transpose(jnp.broadcast_to(row, (L, L)))


def pair_cols(a, q, first):
    return jnp.where(first, a[:, 2 * q : 2 * q + 1], a[:, 2 * q + 1 : 2 * q + 2])


def softplus(v):
    return jnp.maximum(v, 0.0) + jnp.log1p(jnp.exp(-jnp.abs(v)))


def shifted(win, m):
    if m == 0:
        return win[8:, :]
    return pltpu.roll(win, m, 0)[8:, :]


def chunk_columns(hp_ref, step, bounds, base):
    tcol = lax.broadcasted_iota(jnp.int32, (L, L), 0) + base
    trow = lax.broadcasted_iota(jnp.int32, (L, L), 1) + base
    start_col = start_of(bounds, tcol)
    start_end = start_of(bounds, base + (L - 1))
    raw = step + hp_ref[0:1, :]
    dt = softplus(raw)
    decay = hp_ref[1:2, :] * dt
    lower = jnp.where(trow <= tcol, 1.0, 0.0).astype(bf16)
    cum = mm_exact_left(lower, decay)
    cum_end = cum[L - 1 : L, :]
    ecum = jnp.where(start_col < base, jnp.exp(cum), 0.0)
    wend = jnp.where(tcol >= start_end, jnp.exp(cum_end - cum), 0.0)
    carried_end = (start_end < base).astype(f32)
    cdec = jnp.exp(cum_end) * carried_end
    return tcol, trow, start_col, start_end, raw, dt, decay, cum, ecum, wend, cdec


def fwd_kernel(
    len_ref, h_ref, gain_ref, wgi_ref, wss_ref, cp_ref, sp_ref, hp_ref,
    normed_ref, inv_ref, gate_ref, rest_ref, gated_ref, y_ref, st_ref, gsum_ref,
    vbuf, state,
):
    blk = pl.program_id(0)
    width = gate_ref.shape[1]
    full = h_ref.shape[1]
    pairs = width // L

    @pl.when(blk == 0)
    def _():
        vbuf[0:8, :] = jnp.zeros((8, vbuf.shape[1]), f32)
        state[...] = jnp.zeros(state.shape, f32)

    piece = 256

    def norm_rows(s, carry):
        rows = pl.ds(pl.multiple_of(s * L, L), L)
        acc = jnp.zeros((L, piece), f32)
        for k in range(full // piece):
            x = h_ref[rows, k * piece : (k + 1) * piece].astype(f32)
            acc = acc + x * x
        inv = lax.rsqrt(jnp.sum(acc, axis=1, keepdims=True) / full + EPSILON)
        for k in range(full // piece):
            cols = slice(k * piece, (k + 1) * piece)
            x = h_ref[rows, cols].astype(f32)
            normed_ref[rows, cols] = (x * inv * gain_ref[0:1, cols]).astype(bf16)
        inv_ref[s] = to_row(inv)
        return carry

    lax.fori_loop(0, NSUB, norm_rows, 0)
    normed = normed_ref[...]
    gate_ref[...] = mm(normed, wgi_ref[:, :width])
    inner = mm(normed, wgi_ref[:, width:])
    vbuf[8:, :width] = inner
    rest_ref[:, :width] = inner
    tail = mm(normed, wss_ref[...])
    vbuf[8:, width:] = tail[:, :L]
    rest_ref[:, width:] = tail

    bounds = bounds_of(len_ref)
    first = lax.broadcasted_iota(jnp.int32, (L, L), 1) < HEAD

    def chunk(s, carry):
        r0 = pl.multiple_of(s * L, L)
        rows = pl.ds(r0, L)
        base = blk * LB + s * L
        step = rest_ref[rows, width + L :]
        tcol, trow, start_col, _, _, dt, _, cum, ecum, wend, cdec = chunk_columns(
            hp_ref, step, bounds, base
        )
        cum_t = jnp.transpose(cum)
        mask = (trow <= tcol) & (trow >= start_col)
        valid = [tcol - m >= start_col for m in range(4)]

        def conv(cols, taps):
            win = vbuf[pl.ds(r0, L + 8), cols]
            pre = taps[4:5, :] + taps[3:4, :] * win[8:, :]
            for m in range(1, 4):
                pre = pre + taps[3 - m : 4 - m, :] * jnp.where(valid[m], shifted(win, m), 0.0)
            return pre

        pre_s = conv(slice(width, width + L), sp_ref)
        act = pre_s * lax.logistic(pre_s)
        b_map = act[:, :STATE]
        c_map = act[:, STATE:]
        scores = jnp.where(mask, mm3(c_map, b_map, 1, 1), 0.0)
        square = jnp.zeros((L, L), f32)
        for q in range(pairs):
            cols = slice(q * L, (q + 1) * L)
            pre = conv(cols, cp_ref.at[:, cols])
            xin = pre * lax.logistic(pre)
            xp = xin * pair_cols(dt, q, first)
            xh, xl = split(xp)
            bdh, bdl = block_diag(xh, first), block_diag(xl, first)
            mix = []
            for h in (2 * q, 2 * q + 1):
                spread = jnp.minimum(cum[:, h : h + 1] - cum_t[h : h + 1, :], 0.0)
                mix.append(jnp.exp(spread) * scores)
            mh, ml = split(jnp.concatenate(mix, axis=1))
            both = mm(mh, jnp.concatenate([bdh, bdl], axis=1))
            y = both[:, :L] + both[:, L:] + mm(ml, bdh)
            st = state[:, cols]
            st_ref[s, :, cols] = st
            y = y + mm3(c_map, st) * pair_cols(ecum, q, first)
            xw = xp * pair_cols(wend, q, first)
            state[:, cols] = mm3(b_map, xw, 0, 0) + st * pair_cols(cdec, q, first[0:1, :])
            y_ref[rows, cols] = y
            gate = gate_ref[rows, cols]
            gated = (y + cp_ref[5:6, cols] * xin) * (gate * lax.logistic(gate))
            gated_ref[rows, cols] = gated
            square = square + gated * gated
        gsum_ref[s] = to_row(jnp.sum(square, axis=1, keepdims=True))
        return carry

    lax.fori_loop(0, NSUB, chunk, 0)
    vbuf[0:8, :] = vbuf[LB : LB + 8, :]


def mid_kernel(len_ref, cot_ref, w_ref, gated_ref, cp_ref, gs_ref, gdot_ref):
    blk = pl.program_id(0)
    live = bounds_of(len_ref)[3]
    t = lax.broadcasted_iota(jnp.int32, gs_ref.shape, 0) + blk * LB
    gs = jnp.where(t < live, mm(cot_ref[...], w_ref[...], 1, 1), 0.0)
    gs_ref[...] = gs
    dots = jnp.sum(gs * cp_ref[6:7, :] * gated_ref[...], axis=1, keepdims=True)
    for s in range(NSUB):
        gdot_ref[s] = to_row(dots[s * L : (s + 1) * L, :])


def bwd_kernel(
    inner_total,
    len_ref, gate_ref, rest_ref, halo_ref, gs_ref, y_ref, st_ref, gsum_ref, gdot_ref,
    cp_ref, sp_ref, hp_ref,
    low_ref, gsh_ref, nd_ref, size_ref, pg_ref, sg_ref, hg_ref,
    vbuf, qnext, adj, send,
):
    step_id = pl.program_id(0)
    blk = pl.num_programs(0) - 1 - step_id
    width = gate_ref.shape[1]
    pairs = width // L

    @pl.when(step_id == 0)
    def _():
        qnext[...] = jnp.zeros(qnext.shape, f32)
        adj[...] = jnp.zeros(adj.shape, f32)
        send[...] = jnp.zeros(send.shape, f32)
        pg_ref[...] = jnp.zeros(pg_ref.shape, f32)
        sg_ref[...] = jnp.zeros(sg_ref.shape, f32)
        hg_ref[...] = jnp.zeros(hg_ref.shape, f32)

    vbuf[0:8, :] = halo_ref[:, : width + L]
    vbuf[8:, :] = rest_ref[:, : width + L]
    bounds = bounds_of(len_ref)
    first = lax.broadcasted_iota(jnp.int32, (L, L), 1) < HEAD
    lane = lax.broadcasted_iota(jnp.int32, (L, L), 1)
    half = lax.broadcasted_iota(jnp.int32, (L, L), 0) // HEAD

    def chunk(i, carry):
        s = NSUB - 1 - i
        r0 = pl.multiple_of(s * L, L)
        rows = pl.ds(r0, L)
        base = blk * LB + s * L
        step = rest_ref[rows, width + L :]
        tcol, trow, start_col, start_end, raw, dt, decay, cum, ecum, wend, cdec = chunk_columns(
            hp_ref, step, bounds, base
        )
        cum_t = jnp.transpose(cum)
        mask_t = (trow >= tcol) & (start_of(bounds, trow) <= tcol)
        valid = [tcol - m >= start_col for m in range(4)]
        valid_up = [start_of(bounds, tcol + m) <= tcol for m in range(4)]
        gate_rms_row = lax.rsqrt(gsum_ref[s] / inner_total + EPSILON)
        pull_row = gate_rms_row * gate_rms_row * gate_rms_row * gdot_ref[s] / inner_total
        gate_rms = to_col(gate_rms_row)
        pull = to_col(pull_row)

        def conv(cols, taps):
            win = vbuf[pl.ds(r0, L + 8), cols]
            seen = [win[8:, :]]
            pre = taps[4:5, :] + taps[3:4, :] * seen[0]
            for m in range(1, 4):
                seen.append(jnp.where(valid[m], shifted(win, m), 0.0))
                pre = pre + taps[3 - m : 4 - m, :] * seen[m]
            return seen, pre

        def conv_back(q, seen, cols, taps, grad_ref, grad_cols):
            win = jnp.concatenate([q, qnext[:, cols]], axis=0)
            qnext[:, cols] = q[0:8, :]
            grad = taps[3:4, :] * q
            for m in range(1, 4):
                up = pltpu.roll(win, L + 8 - m, 0)[:L, :]
                grad = grad + taps[3 - m : 4 - m, :] * jnp.where(valid_up[m], up, 0.0)
            for m in range(4):
                k = 3 - m
                grad_ref[k : k + 1, grad_cols] += jnp.sum(q * seen[m], axis=0, keepdims=True)
            grad_ref[4:5, grad_cols] += jnp.sum(q, axis=0, keepdims=True)
            return grad

        seen_s, pre_s = conv(slice(width, width + L), sp_ref)
        sig_s = lax.logistic(pre_s)
        act = pre_s * sig_s
        b_map = act[:, :STATE]
        c_map = act[:, STATE:]
        scores_t = jnp.where(mask_t, mm3(b_map, c_map, 1, 1), 0.0)
        d_scores = jnp.zeros((L, L), f32)
        d_b = jnp.zeros((L, STATE), f32)
        d_c = jnp.zeros((L, STATE), f32)
        reduced = jnp.zeros((2 * L, L), f32)
        ends = jnp.zeros((8, L), f32)
        norm_dot = jnp.zeros((L, L), f32)
        size = jnp.zeros((L, L), f32)
        for q in range(pairs):
            cols = slice(q * L, (q + 1) * L)
            taps = cp_ref.at[:, cols]
            skip = cp_ref[5:6, cols]
            seen, pre = conv(cols, taps)
            sig = lax.logistic(pre)
            xin = pre * sig
            dtx = pair_cols(dt, q, first)
            xp = xin * dtx
            y = y_ref[rows, cols]
            ho = y + skip * xin
            gate = gate_ref[rows, cols]
            gsig = lax.logistic(gate)
            sl = gate * gsig
            gated = ho * sl
            gs = gs_ref[rows, cols]
            pg_ref[6:7, cols] += jnp.sum(gs * gated * gate_rms, axis=0, keepdims=True)
            gg = gate_rms * cp_ref[6:7, cols] * gs - gated * pull
            gy = gg * sl
            low_gate = (gg * ho * (gsig * (1.0 + gate * (1.0 - gsig)))).astype(bf16)
            low_ref[rows, cols] = low_gate
            pg_ref[5:6, cols] += jnp.sum(gy * xin, axis=0, keepdims=True)

            yh, yl = split(gy)
            bdh, bdl = block_diag(yh, first), block_diag(yl, first)
            xh, xl = split(xp)
            d_mix = mm(
                jnp.concatenate([xh, xl], axis=1), jnp.concatenate([bdh, bdh], axis=1), 1, 1
            ) + mm(xh, bdl, 1, 1)
            mix = []
            for k in range(2):
                h = 2 * q + k
                spread = jnp.minimum(cum_t[h : h + 1, :] - cum[:, h : h + 1], 0.0)
                factor = jnp.exp(spread)
                d_scores = d_scores + d_mix[:, k * L : (k + 1) * L] * factor
                mix.append(factor * scores_t)
            mh, ml = split(jnp.concatenate(mix, axis=1))
            both = mm(mh, jnp.concatenate([bdh, bdl], axis=1))
            dxp = both[:, :L] + both[:, L:] + mm(ml, bdh)
            wendx = pair_cols(wend, q, first)
            a_in = adj[:, cols]
            dxp = dxp + mm3(b_map, a_in) * wendx
            xw = xp * wendx
            gyw = gy * pair_cols(ecum, q, first)
            s_in = st_ref[s, :, cols]
            d_b = d_b + mm3(xw, a_in, 1, 1)
            d_c = d_c + mm3(gyw, s_in, 1, 1)
            adj[:, cols] = mm3(c_map, gyw, 0, 0) + a_in * pair_cols(cdec, q, first[0:1, :])
            heads = jnp.where(lane == 2 * q + half, 1.0, 0.0).astype(bf16)
            zh, zl = split(jnp.concatenate([gy * y - dxp * xp, dxp * xin], axis=0))
            reduced = reduced + mm(zh, heads) + mm(zl, heads)
            end = jnp.broadcast_to(
                jnp.sum(a_in * send[:, cols], axis=0, keepdims=True), (8, L)
            )
            eh, el = split(end)
            ends = ends + mm(eh, heads) + mm(el, heads)
            send[:, cols] = s_in

            dxin = dxp * dtx + skip * gy
            qv = dxin * (sig * (1.0 + pre * (1.0 - sig)))
            grad = conv_back(qv, seen, cols, taps, pg_ref, cols)
            low_inner = grad.astype(bf16)
            low_ref[rows, width + q * L : width + (q + 1) * L] = low_inner
            wide_gate, wide_inner = low_gate.astype(f32), low_inner.astype(f32)
            norm_dot = norm_dot + wide_gate * gate + wide_inner * seen[0]
            size = size + wide_gate * wide_gate + wide_inner * wide_inner

        d_scores = jnp.where(mask_t, d_scores, 0.0)
        d_b = d_b + mm3(d_scores, c_map)
        d_c = d_c + mm3(d_scores, b_map, 0, 0)
        d_act = jnp.concatenate([d_b, d_c], axis=1)
        q_s = d_act * (sig_s * (1.0 + pre_s * (1.0 - sig_s)))
        shared_cols = slice(width, width + L)
        gsh_ref[rows, :] = conv_back(q_s, seen_s, shared_cols, sp_ref, sg_ref, slice(0, L))

        tail = jnp.where(tcol >= start_end, ends[0:1, :], 0.0)
        keep = jnp.where(mask_t, 1.0, 0.0).astype(bf16)
        d_decay = mm_exact_left(keep, reduced[:L, :]) + tail
        d_dt = reduced[L:, :] + d_decay * hp_ref[1:2, :]
        d_raw = d_dt * lax.logistic(raw)
        hg_ref[0:1, :] += jnp.sum(d_raw, axis=0, keepdims=True)
        hg_ref[1:2, :] += jnp.sum(d_decay * decay, axis=0, keepdims=True)
        low_step = d_raw.astype(bf16)
        low_ref[rows, 2 * width :] = low_step
        wide_step = low_step.astype(f32)
        norm_dot = norm_dot + wide_step * step
        size = size + wide_step * wide_step
        nd_ref[s] = to_row(jnp.sum(norm_dot, axis=1, keepdims=True))
        size_ref[s] = to_row(jnp.sum(size, axis=1, keepdims=True))
        return carry

    lax.fori_loop(0, NSUB, chunk, 0)


def unpack_kernel(me_ref, x_ref, gate_inner_ref, step_ref):
    width = gate_inner_ref.shape[2]
    gate_inner_ref[:, 0, :] = x_ref[0, 0, :, :width]
    gate_inner_ref[:, 1, :] = x_ref[0, 0, :, width : 2 * width]
    step_ref[...] = x_ref[0, 0, :, 2 * width : 2 * width + step_ref.shape[1]]


def place_kernel(me_ref, x_ref, out_ref):
    out_ref[...] = x_ref[0, 0]


def place(x, kernel, shapes):
    _, n, piece, cols = x.shape

    def spec(shape):
        zeros = (0,) * (len(shape) - 1)
        return pl.BlockSpec((piece,) + shape[1:], lambda p, k, me: (p * n + (me[0] ^ k),) + zeros)

    return pl.pallas_call(
        kernel,
        grid_spec=pltpu.PrefetchScalarGridSpec(
            num_scalar_prefetch=1,
            grid=(2, n),
            in_specs=[pl.BlockSpec((1, 1, piece, cols), lambda p, k, me: (p, k, 0, 0))],
            out_specs=[spec(shape) for shape in shapes],
        ),
        out_shape=[jax.ShapeDtypeStruct(shape, f32) for shape in shapes],
        name="place",
    )(lax.axis_index("rows").astype(jnp.int32)[None], x)


def rows_spec(cols, order):
    return pl.BlockSpec((LB, cols), lambda i: (order(i), 0))


def line_spec(order):
    return pl.BlockSpec((NSUB, 1, L), lambda i: (order(i), 0, 0))


def whole_spec(shape):
    return pl.BlockSpec(shape, lambda i: (0,) * len(shape), pipeline_mode=pl.Buffered(1))


def smem_spec():
    return pl.BlockSpec(memory_space=pltpu.SMEM)


VMEM_LIMIT = 60 * 1024 * 1024


def run_fwd(lengths, hidden, gain, wgi, wss, cp, sp, hp):
    tokens, full = hidden.shape
    width = wgi.shape[1] // 2
    lines = tokens // L

    def same(i):
        return i

    return pl.pallas_call(
        fwd_kernel,
        grid=(tokens // LB,),
        in_specs=[
            smem_spec(),
            rows_spec(full, same),
            whole_spec(gain.shape),
            whole_spec(wgi.shape),
            whole_spec(wss.shape),
            whole_spec(cp.shape),
            whole_spec(sp.shape),
            whole_spec(hp.shape),
        ],
        out_specs=[
            rows_spec(full, same),
            line_spec(same),
            rows_spec(width, same),
            rows_spec(width + 2 * L, same),
            rows_spec(width, same),
            rows_spec(width, same),
            pl.BlockSpec((NSUB, STATE, width), lambda i: (i, 0, 0)),
            line_spec(same),
        ],
        out_shape=[
            jax.ShapeDtypeStruct((tokens, full), bf16),
            jax.ShapeDtypeStruct((lines, 1, L), f32),
            jax.ShapeDtypeStruct((tokens, width), f32),
            jax.ShapeDtypeStruct((tokens, width + 2 * L), f32),
            jax.ShapeDtypeStruct((tokens, width), f32),
            jax.ShapeDtypeStruct((tokens, width), f32),
            jax.ShapeDtypeStruct((lines, STATE, width), f32),
            jax.ShapeDtypeStruct((lines, 1, L), f32),
        ],
        scratch_shapes=[
            pltpu.VMEM((LB + 8, width + L), f32),
            pltpu.VMEM((STATE, width), f32),
        ],
        compiler_params=pltpu.CompilerParams(
            dimension_semantics=("arbitrary",), vmem_limit_bytes=VMEM_LIMIT
        ),
        name="mixer_fwd",
    )(lengths, hidden, gain, wgi, wss, cp, sp, hp)


def run_mid(lengths, cot, w_out, gated, cp):
    tokens, full = cot.shape
    width = gated.shape[1]
    lines = tokens // L

    def same(i):
        return i

    return pl.pallas_call(
        mid_kernel,
        grid=(tokens // LB,),
        in_specs=[
            smem_spec(),
            rows_spec(full, same),
            whole_spec(w_out.shape),
            rows_spec(width, same),
            whole_spec(cp.shape),
        ],
        out_specs=[rows_spec(width, same), line_spec(same)],
        out_shape=[
            jax.ShapeDtypeStruct((tokens, width), f32),
            jax.ShapeDtypeStruct((lines, 1, L), f32),
        ],
        compiler_params=pltpu.CompilerParams(
            dimension_semantics=("arbitrary",), vmem_limit_bytes=VMEM_LIMIT
        ),
        name="mixer_mid",
    )(lengths, cot, w_out, gated, cp)


def run_bwd(inner_total, lengths, gate, rest, gs, y, st, gsum, gdot, cp, sp, hp):
    tokens, width = gate.shape
    lines = tokens // L
    blocks = tokens // LB

    def back(i):
        return blocks - 1 - i

    def halo(i):
        return (jnp.maximum(back(i) * (LB // 8) - 1, 0), 0)

    return pl.pallas_call(
        functools.partial(bwd_kernel, float(inner_total)),
        grid=(blocks,),
        in_specs=[
            smem_spec(),
            rows_spec(width, back),
            rows_spec(width + 2 * L, back),
            pl.BlockSpec((8, width + 2 * L), halo),
            rows_spec(width, back),
            rows_spec(width, back),
            pl.BlockSpec((NSUB, STATE, width), lambda i: (back(i), 0, 0)),
            line_spec(back),
            line_spec(back),
            whole_spec(cp.shape),
            whole_spec(sp.shape),
            whole_spec(hp.shape),
        ],
        out_specs=[
            rows_spec(2 * width + L, back),
            rows_spec(L, back),
            line_spec(back),
            line_spec(back),
            pl.BlockSpec((8, width), lambda i: (0, 0)),
            pl.BlockSpec((8, L), lambda i: (0, 0)),
            pl.BlockSpec((8, L), lambda i: (0, 0)),
        ],
        out_shape=[
            jax.ShapeDtypeStruct((tokens, 2 * width + L), bf16),
            jax.ShapeDtypeStruct((tokens, L), f32),
            jax.ShapeDtypeStruct((lines, 1, L), f32),
            jax.ShapeDtypeStruct((lines, 1, L), f32),
            jax.ShapeDtypeStruct((8, width), f32),
            jax.ShapeDtypeStruct((8, L), f32),
            jax.ShapeDtypeStruct((8, L), f32),
        ],
        scratch_shapes=[
            pltpu.VMEM((LB + 8, width + L), f32),
            pltpu.VMEM((8, width + L), f32),
            pltpu.VMEM((STATE, width), f32),
            pltpu.VMEM((STATE, width), f32),
        ],
        compiler_params=pltpu.CompilerParams(
            dimension_semantics=("arbitrary",), vmem_limit_bytes=VMEM_LIMIT
        ),
        name="mixer_bwd",
    )(lengths, gate, rest, rest, gs, y, st, gsum, gdot, cp, sp, hp)


def pack_params(conv_inner, conv_inner_bias, conv_shared, conv_shared_bias, step_bias, log_decay,
                skip_gain, gate_gain):
    width = conv_inner.shape[1]
    heads = step_bias.shape[0]
    skip = jnp.repeat(skip_gain, HEAD)
    cp = jnp.concatenate(
        [conv_inner, conv_inner_bias[None], skip[None], gate_gain[None], jnp.zeros((1, width), f32)],
        axis=0,
    )
    sp = jnp.concatenate([conv_shared, conv_shared_bias[None], jnp.zeros((3, L), f32)], axis=0)
    hp = jnp.zeros((8, L), f32)
    hp = hp.at[0, :heads].set(step_bias).at[1, :heads].set(-jnp.exp(log_decay))
    return cp, sp, hp


def exchange_kernel(axis, x_ref, out_ref, slots, send_sem, recv_sem):
    me = lax.axis_index(axis)
    n = slots.shape[0]
    barrier = pltpu.get_barrier_semaphore()
    for k in range(1, n):
        peer = lax.rem(me + k, n)
        pl.semaphore_signal(barrier, inc=1, device_id={axis: peer})
    pl.semaphore_wait(barrier, n - 1)
    copies = []
    for k in range(1, n):
        peer = lax.rem(me + k, n)
        copy = pltpu.make_async_remote_copy(
            src_ref=x_ref,
            dst_ref=slots.at[k],
            send_sem=send_sem.at[k],
            recv_sem=recv_sem.at[k],
            device_id={axis: peer},
        )
        copy.start()
        copies.append(copy)
    for copy in copies:
        copy.wait()
    slots[0] = x_ref[...]
    total = slots[lax.rem(me, n)]
    for d in range(1, n):
        total = total + slots[lax.rem(me - d + n, n)]
    out_ref[...] = total


def sum_small(x, axis, collective_id):
    n = lax.axis_size(axis)
    return pl.pallas_call(
        functools.partial(exchange_kernel, axis),
        out_shape=jax.ShapeDtypeStruct(x.shape, f32),
        in_specs=[pl.BlockSpec(memory_space=pltpu.VMEM)],
        out_specs=pl.BlockSpec(memory_space=pltpu.VMEM),
        scratch_shapes=[
            pltpu.VMEM((n,) + x.shape, f32),
            pltpu.SemaphoreType.DMA((n,)),
            pltpu.SemaphoreType.DMA((n,)),
        ],
        compiler_params=pltpu.CompilerParams(collective_id=collective_id, has_side_effects=True),
        name="sum_small",
    )(x)


def after(x, *deps):
    deps = [d for d in deps if d is not None]
    return lax.optimization_barrier((x, *deps))[0]


SCALE = 16384.0


def encode(x, bound, kind):
    if bound is not None:
        x = x * (SCALE / bound)
    return x.astype(kind)


def decode(x, bound):
    x = x.astype(f32)
    return x if bound is None else x * (bound / SCALE)


class ScatterLine:

    def __init__(self, send, own, bound, kind):
        self.n = lax.axis_size("heads")
        self.chips = self.n // 2
        self.z = lax.axis_index("heads") >> 1
        self.own, self.kind, self.bound = own, kind, bound
        self.moving, self.out = [None, None], [None, None]
        self.message = encode(send, bound, kind)

    def swap(self):
        pairs = [(i, i ^ 1) for i in range(self.n)]
        self.got = lax.ppermute(self.message, "heads", pairs)

    def block(self, b):
        mine = lax.dynamic_index_in_dim(self.own, b, 0, keepdims=False)
        theirs = lax.dynamic_index_in_dim(self.got, b, 0, keepdims=False)
        return mine + decode(theirs, self.bound)

    def pack(self, r):
        last = self.chips - 1
        for way in range(2):
            b = last - r + self.z if way == 0 else r - last + self.z
            total = self.block(jnp.clip(b, 0, last))
            if r > 0:
                total = total + decode(self.moving[way], self.bound)
            self.out[way] = encode(total, self.bound, self.kind)

    def hold(self, *deps):
        self.moving = [after(m, *deps) for m in self.moving]

    def send(self, r):
        last = self.chips - 1
        out = lax.optimization_barrier(tuple(self.out))
        for way in range(2):
            chips = range(r + 1) if way == 0 else range(last - r, last + 1)
            hop = 2 if way == 0 else -2
            pairs = [(2 * k + c, 2 * k + c + hop) for k in chips for c in range(2)]
            self.moving[way] = lax.ppermute(out[way], "heads", pairs)
        self.moving = list(lax.optimization_barrier(tuple(self.moving)))

    def rest(self, r):
        for k in range(r, self.chips - 1):
            self.pack(k)
            self.send(k)

    def total(self):
        total = self.block(self.z)
        for way in range(2):
            if self.moving[way] is not None:
                total = total + decode(self.moving[way], self.bound)
        return total


class RowSum:

    def __init__(self, x, bound):
        self.n = lax.axis_size("rows")
        self.me = lax.axis_index("rows")
        self.bits = self.n.bit_length() - 1
        self.bound = bound
        piece = x.shape[0] // (2 * self.n)
        cut = x.reshape((2,) + (2,) * self.bits + (piece, x.shape[1]))
        self.cur = [cut[0], cut[1]]
        self.order = [[(k + part) % self.bits for k in range(self.bits)] for part in range(2)]
        self.left = [list(range(self.bits))[::-1] for _ in range(2)]

    def move(self, x, bit):
        return lax.ppermute(x, "rows", [(i, i ^ (1 << bit)) for i in range(self.n)])

    def reduce(self, k):
        for part in range(2):
            bit, left = self.order[part][k], self.left[part]
            mine = (self.me >> bit) & 1
            axis = left.index(bit)
            left.remove(bit)
            cur = self.cur[part]
            send = lax.dynamic_index_in_dim(cur, 1 - mine, axis, keepdims=False)
            keep = lax.dynamic_index_in_dim(cur, mine, axis, keepdims=False)
            got = self.move(encode(send, self.bound, jnp.float16), bit)
            self.cur[part] = keep + decode(got, self.bound)

    def hold(self, *deps):
        self.cur = [after(cur, *deps) for cur in self.cur]

    def spread(self):
        pieces = [{0: encode(cur, self.bound, jnp.float16)} for cur in self.cur]
        for k in reversed(range(self.bits)):
            far = []
            for part in range(2):
                bit = self.order[part][k]
                for rel in list(pieces[part]):
                    pieces[part][rel ^ (1 << bit)] = self.move(pieces[part][rel], bit)
                    far.append((part, rel ^ (1 << bit)))
            held = lax.optimization_barrier(tuple(pieces[part][rel] for part, rel in far))
            for (part, rel), data in zip(far, held):
                pieces[part][rel] = data
        halves = [pieces[part][rel] for part in range(2) for rel in range(self.n)]
        whole = decode(jnp.stack(halves), self.bound)
        return whole.reshape((2, self.n) + whole.shape[1:])


def per_device(
    hidden_in, lengths, norm_gain, in_gate_inner, in_step, in_shared, conv_inner, conv_inner_bias,
    conv_shared, conv_shared_bias, step_bias, log_decay, skip_gain, gate_gain, out_weight, cotangent,
):
    tokens, local = hidden_in.shape
    full = in_gate_inner.shape[0]
    width = in_gate_inner.shape[2]
    heads = step_bias.shape[0]
    chips = full // local // 2
    lines = tokens // L
    inner_total = width * (full // local)
    core = lax.axis_index("heads") & 1
    source = hidden_in.astype(f32)

    hidden_all = lax.all_gather(hidden_in, "heads", axis=1, tiled=True)
    shared_all = lax.all_gather(in_shared, "heads", axis=1, tiled=True)
    gain_all = lax.all_gather(norm_gain, "heads", axis=0, tiled=True)
    cot_all = lax.all_gather(cotangent, "heads", axis=1, tiled=True)
    wgi = in_gate_inner.reshape(full, 2 * width)
    step_pad = jnp.pad(in_step, ((0, 0), (0, L - heads)))
    wss = jnp.concatenate([shared_all.T, step_pad], axis=1)
    w_back = jnp.concatenate([wgi, step_pad], axis=1)

    def halves(w, axis):
        both = []
        for side in (1 - core, core):
            parts = [
                lax.dynamic_slice_in_dim(w, (2 * k + side) * local, local, axis) for k in range(chips)
            ]
            both.append(jnp.stack(parts))
        return both

    back_send, back_own = halves(w_back, 0)
    out_send, out_own = halves(out_weight, 1)
    w_size = jnp.sqrt(jnp.max(jnp.sum(jnp.square(w_back.astype(f32)), axis=1)))
    cp, sp, hp = pack_params(
        conv_inner, conv_inner_bias, conv_shared, conv_shared_bias, step_bias, log_decay,
        skip_gain, gate_gain,
    )

    hidden_all = after(hidden_all, back_send, back_own, out_send, out_own, w_size, cp, sp, hp)
    normed, inv_rows, gate, rest, gated, y, st, gsum_part = run_fwd(
        lengths, hidden_all, gain_all[None], wgi, wss, cp, sp, hp
    )
    inv_rms = inv_rows.reshape(tokens)
    gsum = sum_small(gsum_part.reshape(lines, L), "heads", 1)

    live = (jnp.arange(tokens, dtype=jnp.int32) < jnp.sum(lengths[0])).astype(bf16)
    gate_rms = lax.rsqrt(gsum.reshape(tokens) / inner_total + EPSILON)
    scaled = (gated * gate_rms[:, None] * gate_gain[None, :]).astype(bf16) * live[:, None]

    def project(w, v, axis):
        return lax.dot_general(w, v, (((axis,), (1,)), ((), ())), preferred_element_type=f32)

    mixed = ScatterLine(
        project(out_send, scaled, 1), project(out_own, scaled, 1), None, jnp.float16
    )
    mixed.swap()
    mixed.pack(0)
    cot_late = after(cot_all, *mixed.out)
    mixed.send(0)
    gs, gdot_part = run_mid(lengths, cot_late, out_weight, gated, cp)
    gdot = sum_small(gdot_part.reshape(lines, L), "heads", 2)
    mixed.hold(gdot)
    mixed.pack(1)
    gdot = after(gdot, *mixed.out)
    mixed.send(1)

    low, gsh_part, nd_part, size, pg, sg, hg = run_bwd(
        inner_total, lengths, gate, rest, gs, y, st, gsum.reshape(lines, 1, L),
        gdot.reshape(lines, 1, L), cp, sp, hp,
    )
    bound = jnp.sqrt(size.reshape(lines, L)) * (1.01 * w_size) + 1e-30
    mixed.hold(low)
    mixed.pack(2)
    nd_part = after(nd_part, *mixed.out)
    mixed.send(2)
    small = sum_small(
        jnp.concatenate([nd_part.reshape(lines, L), bound, sg], axis=0), "heads", 3
    )
    norm_dot, sg = small[:lines].reshape(tokens), small[2 * lines :]
    bound = small[lines : 2 * lines].reshape(tokens)
    low = after(low, bound)

    normal = ScatterLine(project(back_send, low, 2), project(back_own, low, 2), bound, jnp.float16)
    normal.swap()
    normal.pack(0)
    low_late = after(low, *normal.out)
    scaled_late = after(scaled, *normal.out)
    mixed.hold(*normal.out)
    normal.send(0)

    grad_proj = lax.dot_general(
        normed, low_late, (((0,), (0,)), ((), ())), preferred_element_type=f32
    )
    top_proj = jnp.max(jnp.abs(grad_proj))
    grad_wout = lax.dot_general(
        scaled_late, cot_all, (((0,), (0,)), ((), ())), preferred_element_type=f32
    )
    top_wout = jnp.max(jnp.abs(grad_wout))
    tops = jnp.stack([top_proj, top_wout])
    tops = jnp.broadcast_to(jnp.repeat(tops * 1.01 + 1e-30, 8)[:, None], (16, L))
    wide = pg.reshape(8 * width // L, L)
    small = sum_small(jnp.concatenate([tops, sg, hg, wide], axis=0), "rows", 4)

    normal.hold(small)
    normal.pack(1)
    small = after(small, *normal.out)
    gsh_part = after(gsh_part, *normal.out)
    mixed.hold(*normal.out)
    normal.send(1)
    top_proj, top_wout, sg, hg = small[0, 0], small[8, 0], small[16:24], small[24:32]
    pg = small[32:].reshape(8, width)
    sum_proj, sum_wout = RowSum(grad_proj, top_proj), RowSum(grad_wout, top_wout)
    for k in range(sum_proj.bits):
        sum_proj.reduce(k)
        sum_wout.reduce(k)
    mixed.rest(3)
    output = (source + mixed.total().T).astype(bf16)

    cut = gsh_part.T.reshape(chips, 2, L // (2 * chips), tokens)
    gsh_own = lax.dynamic_index_in_dim(cut, core, 1, keepdims=False)
    gsh_send = lax.dynamic_index_in_dim(cut, 1 - core, 1, keepdims=False)
    shared = ScatterLine(gsh_send, gsh_own, None, f32)
    shared.swap()
    shared.rest(0)
    low_shared = lax.all_gather(shared.total().astype(bf16), "heads", axis=0, tiled=True)
    shared_raw = rest[:, width : width + L]
    norm_dot = norm_dot + jnp.sum(low_shared.T.astype(f32) * shared_raw, axis=1)
    normed_local = (source * inv_rms[:, None] * norm_gain[None, :]).astype(bf16)
    grad_shared_w = lax.dot_general(
        low_shared, normed_local, (((1,), (0,)), ((), ())), preferred_element_type=f32
    )
    grad_shared_w = lax.psum(grad_shared_w, "rows")

    normal.pack(2)
    sum_proj.hold(*normal.out)
    sum_wout.hold(*normal.out)
    normal.send(2)
    grad_proj, grad_step = place(
        sum_proj.spread(), unpack_kernel, [(full, 2, width), (full, heads)]
    )
    (grad_wout,) = place(sum_wout.spread(), place_kernel, [grad_wout.shape])

    normal.rest(3)
    grad_normed = normal.total() + lax.dot_general(
        in_shared, low_shared, (((0,), (0,)), ((), ())), preferred_element_type=f32
    )
    grad_normed = grad_normed.T
    grad_gain_norm = jnp.sum(grad_normed * source * inv_rms[:, None], axis=0)
    grad_source = (
        inv_rms[:, None] * norm_gain[None, :] * grad_normed
        - source * (inv_rms * inv_rms * norm_dot / full)[:, None]
    )
    grad_input = cotangent.astype(f32) + grad_source
    grad_gain_norm = sum_small(grad_gain_norm.reshape(local // L, L), "rows", 5).reshape(local)
    return (
        output,
        grad_input,
        grad_gain_norm,
        grad_proj,
        grad_step,
        grad_shared_w,
        pg[0:4],
        pg[4],
        sg[0:4],
        sg[4],
        hg[0, :heads],
        hg[1, :heads],
        pg[5].reshape(heads, HEAD).sum(axis=1),
        pg[6],
        grad_wout,
    )


def solution(mesh):
    return jax.shard_map(
        per_device,
        mesh=mesh,
        in_specs=(
            P("rows", "heads"), P("rows", None), P("heads"), P(None, None, "heads"),
            P(None, "heads"), P(None, "heads"), P(None, "heads"), P("heads"), P(), P(),
            P("heads"), P("heads"), P("heads"), P("heads"), P("heads", None), P("rows", "heads"),
        ),
        out_specs=(
            P("rows", "heads"), P("rows", "heads"), P("heads"), P(None, None, "heads"),
            P(None, "heads"), P(None, "heads"), P(None, "heads"), P("heads"), P(), P(),
            P("heads"), P("heads"), P("heads"), P("heads"), P("heads", None),
        ),
        check_vma=False,
    )
```

```python
import functools

import jax
import jax.numpy as jnp
from jax import lax
from jax.experimental import pallas as pl
from jax.experimental.pallas import tpu as pltpu
from jax.sharding import PartitionSpec as P


EPSILON = 1e-05
L = 128
LB = 512
NSUB = LB // L
HEAD = 64
STATE = 64
f32 = jnp.float32
bf16 = jnp.bfloat16


def mm(a, b, ca=1, cb=0):
    return lax.dot_general(a, b, (((ca,), (cb,)), ((), ())), preferred_element_type=f32)


def split(x):
    hi = x.astype(bf16)
    return hi, (x - hi.astype(f32)).astype(bf16)


def mm3(a, b, ca=1, cb=0):
    ah, al = split(a)
    bh, bl = split(b)
    return mm(ah, bh, ca, cb) + mm(ah, bl, ca, cb) + mm(al, bh, ca, cb)


def mm_exact_left(mask, x):
    hi = x.astype(bf16)
    rest = x - hi.astype(f32)
    mid = rest.astype(bf16)
    low = (rest - mid.astype(f32)).astype(bf16)
    return mm(mask, hi) + mm(mask, mid) + mm(mask, low)


def block_diag(x, first):
    zero = jnp.zeros_like(x)
    return jnp.concatenate([jnp.where(first, x, zero), jnp.where(first, zero, x)], axis=0)


def bounds_of(len_ref):
    b0 = len_ref[0, 0]
    b1 = b0 + len_ref[0, 1]
    b2 = b1 + len_ref[0, 2]
    b3 = b2 + len_ref[0, 3]
    return b0, b1, b2, b3


def start_of(bounds, t):
    start = jnp.zeros_like(t)
    for b in bounds:
        start = jnp.where(t >= b, b, start)
    return start


def to_row(col):
    return jnp.transpose(jnp.broadcast_to(col, (L, L)))[0:1, :]


def to_col(row):
    return jnp.transpose(jnp.broadcast_to(row, (L, L)))


def pair_cols(a, q, first):
    return jnp.where(first, a[:, 2 * q : 2 * q + 1], a[:, 2 * q + 1 : 2 * q + 2])


def softplus(v):
    return jnp.maximum(v, 0.0) + jnp.log1p(jnp.exp(-jnp.abs(v)))


def shifted(win, m):
    if m == 0:
        return win[8:, :]
    return pltpu.roll(win, m, 0)[8:, :]


def chunk_columns(hp_ref, step, bounds, base):
    tcol = lax.broadcasted_iota(jnp.int32, (L, L), 0) + base
    trow = lax.broadcasted_iota(jnp.int32, (L, L), 1) + base
    start_col = start_of(bounds, tcol)
    start_end = start_of(bounds, base + (L - 1))
    raw = step + hp_ref[0:1, :]
    dt = softplus(raw)
    decay = hp_ref[1:2, :] * dt
    lower = jnp.where(trow <= tcol, 1.0, 0.0).astype(bf16)
    cum = mm_exact_left(lower, decay)
    cum_end = cum[L - 1 : L, :]
    ecum = jnp.where(start_col < base, jnp.exp(cum), 0.0)
    wend = jnp.where(tcol >= start_end, jnp.exp(cum_end - cum), 0.0)
    carried_end = (start_end < base).astype(f32)
    cdec = jnp.exp(cum_end) * carried_end
    return tcol, trow, start_col, start_end, raw, dt, decay, cum, ecum, wend, cdec


def fwd_kernel(
    first_block,
    len_ref, h_ref, gain_ref, wgi_ref, wss_ref, cp_ref, sp_ref, hp_ref, v_in_ref, state_in_ref,
    normed_ref, inv_ref, gate_ref, rest_ref, gated_ref, y_ref, st_ref, gsum_ref, v_out_ref,
    state_out_ref, vbuf, state,
):
    blk = pl.program_id(0)
    width = gate_ref.shape[1]
    full = h_ref.shape[1]
    pairs = width // L

    @pl.when(blk == 0)
    def _():
        vbuf[0:8, :] = v_in_ref[...]
        state[...] = state_in_ref[...]

    piece = 256

    def norm_rows(s, carry):
        rows = pl.ds(pl.multiple_of(s * L, L), L)
        acc = jnp.zeros((L, piece), f32)
        for k in range(full // piece):
            x = h_ref[rows, k * piece : (k + 1) * piece].astype(f32)
            acc = acc + x * x
        inv = lax.rsqrt(jnp.sum(acc, axis=1, keepdims=True) / full + EPSILON)
        for k in range(full // piece):
            cols = slice(k * piece, (k + 1) * piece)
            x = h_ref[rows, cols].astype(f32)
            normed_ref[rows, cols] = (x * inv * gain_ref[0:1, cols]).astype(bf16)
        inv_ref[s] = to_row(inv)
        return carry

    lax.fori_loop(0, NSUB, norm_rows, 0)
    normed = normed_ref[...]
    gate_ref[...] = mm(normed, wgi_ref[:, :width])
    inner = mm(normed, wgi_ref[:, width:])
    vbuf[8:, :width] = inner
    rest_ref[:, :width] = inner
    tail = mm(normed, wss_ref[...])
    vbuf[8:, width:] = tail[:, :L]
    rest_ref[:, width:] = tail

    bounds = bounds_of(len_ref)
    first = lax.broadcasted_iota(jnp.int32, (L, L), 1) < HEAD

    def chunk(s, carry):
        r0 = pl.multiple_of(s * L, L)
        rows = pl.ds(r0, L)
        base = (blk + first_block) * LB + s * L
        step = rest_ref[rows, width + L :]
        tcol, trow, start_col, _, _, dt, _, cum, ecum, wend, cdec = chunk_columns(
            hp_ref, step, bounds, base
        )
        cum_t = jnp.transpose(cum)
        mask = (trow <= tcol) & (trow >= start_col)
        valid = [tcol - m >= start_col for m in range(4)]

        def conv(cols, taps):
            win = vbuf[pl.ds(r0, L + 8), cols]
            pre = taps[4:5, :] + taps[3:4, :] * win[8:, :]
            for m in range(1, 4):
                pre = pre + taps[3 - m : 4 - m, :] * jnp.where(valid[m], shifted(win, m), 0.0)
            return pre

        pre_s = conv(slice(width, width + L), sp_ref)
        act = pre_s * lax.logistic(pre_s)
        b_map = act[:, :STATE]
        c_map = act[:, STATE:]
        scores = jnp.where(mask, mm3(c_map, b_map, 1, 1), 0.0)
        square = jnp.zeros((L, L), f32)
        for q in range(pairs):
            cols = slice(q * L, (q + 1) * L)
            pre = conv(cols, cp_ref.at[:, cols])
            xin = pre * lax.logistic(pre)
            xp = xin * pair_cols(dt, q, first)
            xh, xl = split(xp)
            bdh, bdl = block_diag(xh, first), block_diag(xl, first)
            mix = []
            for h in (2 * q, 2 * q + 1):
                spread = jnp.minimum(cum[:, h : h + 1] - cum_t[h : h + 1, :], 0.0)
                mix.append(jnp.exp(spread) * scores)
            mh, ml = split(jnp.concatenate(mix, axis=1))
            both = mm(mh, jnp.concatenate([bdh, bdl], axis=1))
            y = both[:, :L] + both[:, L:] + mm(ml, bdh)
            st = state[:, cols]
            st_ref[s, :, cols] = st
            y = y + mm3(c_map, st) * pair_cols(ecum, q, first)
            xw = xp * pair_cols(wend, q, first)
            state[:, cols] = mm3(b_map, xw, 0, 0) + st * pair_cols(cdec, q, first[0:1, :])
            y_ref[rows, cols] = y
            gate = gate_ref[rows, cols]
            gated = (y + cp_ref[5:6, cols] * xin) * (gate * lax.logistic(gate))
            gated_ref[rows, cols] = gated
            square = square + gated * gated
        gsum_ref[s] = to_row(jnp.sum(square, axis=1, keepdims=True))
        return carry

    lax.fori_loop(0, NSUB, chunk, 0)
    vbuf[0:8, :] = vbuf[LB : LB + 8, :]

    @pl.when(blk == pl.num_programs(0) - 1)
    def _():
        v_out_ref[...] = vbuf[0:8, :]
        state_out_ref[...] = state[...]


def mid_kernel(first_block, len_ref, cot_ref, w_ref, gated_ref, cp_ref, gs_ref, gdot_ref):
    blk = pl.program_id(0)
    live = bounds_of(len_ref)[3]
    t = lax.broadcasted_iota(jnp.int32, gs_ref.shape, 0) + (blk + first_block) * LB
    gs = jnp.where(t < live, mm(cot_ref[...], w_ref[...], 1, 1), 0.0)
    gs_ref[...] = gs
    dots = jnp.sum(gs * cp_ref[6:7, :] * gated_ref[...], axis=1, keepdims=True)
    for s in range(NSUB):
        gdot_ref[s] = to_row(dots[s * L : (s + 1) * L, :])


def bwd_kernel(
    inner_total, first_block,
    len_ref, gate_ref, rest_ref, halo_ref, gs_ref, y_ref, st_ref, gsum_ref, gdot_ref,
    cp_ref, sp_ref, hp_ref, v_in_ref, q_in_ref, adj_in_ref, send_in_ref,
    low_ref, gsh_ref, nd_ref, size_ref, pg_ref, sg_ref, hg_ref, q_out_ref, adj_out_ref,
    vbuf, qnext, adj, send,
):
    step_id = pl.program_id(0)
    blk = pl.num_programs(0) - 1 - step_id
    width = gate_ref.shape[1]
    pairs = width // L

    @pl.when(step_id == 0)
    def _():
        qnext[...] = q_in_ref[...]
        adj[...] = adj_in_ref[...]
        send[...] = send_in_ref[...]
        pg_ref[...] = jnp.zeros(pg_ref.shape, f32)
        sg_ref[...] = jnp.zeros(sg_ref.shape, f32)
        hg_ref[...] = jnp.zeros(hg_ref.shape, f32)

    @pl.when(blk == 0)
    def _():
        vbuf[0:8, :] = v_in_ref[...]

    @pl.when(blk > 0)
    def _():
        vbuf[0:8, :] = halo_ref[:, : width + L]

    vbuf[8:, :] = rest_ref[:, : width + L]
    bounds = bounds_of(len_ref)
    first = lax.broadcasted_iota(jnp.int32, (L, L), 1) < HEAD
    lane = lax.broadcasted_iota(jnp.int32, (L, L), 1)
    half = lax.broadcasted_iota(jnp.int32, (L, L), 0) // HEAD

    def chunk(i, carry):
        s = NSUB - 1 - i
        r0 = pl.multiple_of(s * L, L)
        rows = pl.ds(r0, L)
        base = (blk + first_block) * LB + s * L
        step = rest_ref[rows, width + L :]
        tcol, trow, start_col, start_end, raw, dt, decay, cum, ecum, wend, cdec = chunk_columns(
            hp_ref, step, bounds, base
        )
        cum_t = jnp.transpose(cum)
        mask_t = (trow >= tcol) & (start_of(bounds, trow) <= tcol)
        valid = [tcol - m >= start_col for m in range(4)]
        valid_up = [start_of(bounds, tcol + m) <= tcol for m in range(4)]
        gate_rms_row = lax.rsqrt(gsum_ref[s] / inner_total + EPSILON)
        pull_row = gate_rms_row * gate_rms_row * gate_rms_row * gdot_ref[s] / inner_total
        gate_rms = to_col(gate_rms_row)
        pull = to_col(pull_row)

        def conv(cols, taps):
            win = vbuf[pl.ds(r0, L + 8), cols]
            seen = [win[8:, :]]
            pre = taps[4:5, :] + taps[3:4, :] * seen[0]
            for m in range(1, 4):
                seen.append(jnp.where(valid[m], shifted(win, m), 0.0))
                pre = pre + taps[3 - m : 4 - m, :] * seen[m]
            return seen, pre

        def conv_back(q, seen, cols, taps, grad_ref, grad_cols):
            win = jnp.concatenate([q, qnext[:, cols]], axis=0)
            qnext[:, cols] = q[0:8, :]
            grad = taps[3:4, :] * q
            for m in range(1, 4):
                up = pltpu.roll(win, L + 8 - m, 0)[:L, :]
                grad = grad + taps[3 - m : 4 - m, :] * jnp.where(valid_up[m], up, 0.0)
            for m in range(4):
                k = 3 - m
                grad_ref[k : k + 1, grad_cols] += jnp.sum(q * seen[m], axis=0, keepdims=True)
            grad_ref[4:5, grad_cols] += jnp.sum(q, axis=0, keepdims=True)
            return grad

        seen_s, pre_s = conv(slice(width, width + L), sp_ref)
        sig_s = lax.logistic(pre_s)
        act = pre_s * sig_s
        b_map = act[:, :STATE]
        c_map = act[:, STATE:]
        scores_t = jnp.where(mask_t, mm3(b_map, c_map, 1, 1), 0.0)
        d_scores = jnp.zeros((L, L), f32)
        d_b = jnp.zeros((L, STATE), f32)
        d_c = jnp.zeros((L, STATE), f32)
        reduced = jnp.zeros((2 * L, L), f32)
        ends = jnp.zeros((8, L), f32)
        norm_dot = jnp.zeros((L, L), f32)
        size = jnp.zeros((L, L), f32)
        for q in range(pairs):
            cols = slice(q * L, (q + 1) * L)
            taps = cp_ref.at[:, cols]
            skip = cp_ref[5:6, cols]
            seen, pre = conv(cols, taps)
            sig = lax.logistic(pre)
            xin = pre * sig
            dtx = pair_cols(dt, q, first)
            xp = xin * dtx
            y = y_ref[rows, cols]
            ho = y + skip * xin
            gate = gate_ref[rows, cols]
            gsig = lax.logistic(gate)
            sl = gate * gsig
            gated = ho * sl
            gs = gs_ref[rows, cols]
            pg_ref[6:7, cols] += jnp.sum(gs * gated * gate_rms, axis=0, keepdims=True)
            gg = gate_rms * cp_ref[6:7, cols] * gs - gated * pull
            gy = gg * sl
            low_gate = (gg * ho * (gsig * (1.0 + gate * (1.0 - gsig)))).astype(bf16)
            low_ref[rows, cols] = low_gate
            pg_ref[5:6, cols] += jnp.sum(gy * xin, axis=0, keepdims=True)

            yh, yl = split(gy)
            bdh, bdl = block_diag(yh, first), block_diag(yl, first)
            xh, xl = split(xp)
            d_mix = mm(
                jnp.concatenate([xh, xl], axis=1), jnp.concatenate([bdh, bdh], axis=1), 1, 1
            ) + mm(xh, bdl, 1, 1)
            mix = []
            for k in range(2):
                h = 2 * q + k
                spread = jnp.minimum(cum_t[h : h + 1, :] - cum[:, h : h + 1], 0.0)
                factor = jnp.exp(spread)
                d_scores = d_scores + d_mix[:, k * L : (k + 1) * L] * factor
                mix.append(factor * scores_t)
            mh, ml = split(jnp.concatenate(mix, axis=1))
            both = mm(mh, jnp.concatenate([bdh, bdl], axis=1))
            dxp = both[:, :L] + both[:, L:] + mm(ml, bdh)
            wendx = pair_cols(wend, q, first)
            a_in = adj[:, cols]
            dxp = dxp + mm3(b_map, a_in) * wendx
            xw = xp * wendx
            gyw = gy * pair_cols(ecum, q, first)
            s_in = st_ref[s, :, cols]
            d_b = d_b + mm3(xw, a_in, 1, 1)
            d_c = d_c + mm3(gyw, s_in, 1, 1)
            adj[:, cols] = mm3(c_map, gyw, 0, 0) + a_in * pair_cols(cdec, q, first[0:1, :])
            heads = jnp.where(lane == 2 * q + half, 1.0, 0.0).astype(bf16)
            zh, zl = split(jnp.concatenate([gy * y - dxp * xp, dxp * xin], axis=0))
            reduced = reduced + mm(zh, heads) + mm(zl, heads)
            end = jnp.broadcast_to(
                jnp.sum(a_in * send[:, cols], axis=0, keepdims=True), (8, L)
            )
            eh, el = split(end)
            ends = ends + mm(eh, heads) + mm(el, heads)
            send[:, cols] = s_in

            dxin = dxp * dtx + skip * gy
            qv = dxin * (sig * (1.0 + pre * (1.0 - sig)))
            grad = conv_back(qv, seen, cols, taps, pg_ref, cols)
            low_inner = grad.astype(bf16)
            low_ref[rows, width + q * L : width + (q + 1) * L] = low_inner
            wide_gate, wide_inner = low_gate.astype(f32), low_inner.astype(f32)
            norm_dot = norm_dot + wide_gate * gate + wide_inner * seen[0]
            size = size + wide_gate * wide_gate + wide_inner * wide_inner

        d_scores = jnp.where(mask_t, d_scores, 0.0)
        d_b = d_b + mm3(d_scores, c_map)
        d_c = d_c + mm3(d_scores, b_map, 0, 0)
        d_act = jnp.concatenate([d_b, d_c], axis=1)
        q_s = d_act * (sig_s * (1.0 + pre_s * (1.0 - sig_s)))
        shared_cols = slice(width, width + L)
        gsh_ref[rows, :] = conv_back(q_s, seen_s, shared_cols, sp_ref, sg_ref, slice(0, L))

        tail = jnp.where(tcol >= start_end, ends[0:1, :], 0.0)
        keep = jnp.where(mask_t, 1.0, 0.0).astype(bf16)
        d_decay = mm_exact_left(keep, reduced[:L, :]) + tail
        d_dt = reduced[L:, :] + d_decay * hp_ref[1:2, :]
        d_raw = d_dt * lax.logistic(raw)
        hg_ref[0:1, :] += jnp.sum(d_raw, axis=0, keepdims=True)
        hg_ref[1:2, :] += jnp.sum(d_decay * decay, axis=0, keepdims=True)
        low_step = d_raw.astype(bf16)
        low_ref[rows, 2 * width :] = low_step
        wide_step = low_step.astype(f32)
        norm_dot = norm_dot + wide_step * step
        size = size + wide_step * wide_step
        nd_ref[s] = to_row(jnp.sum(norm_dot, axis=1, keepdims=True))
        size_ref[s] = to_row(jnp.sum(size, axis=1, keepdims=True))
        return carry

    lax.fori_loop(0, NSUB, chunk, 0)

    @pl.when(blk == 0)
    def _():
        q_out_ref[...] = qnext[...]
        adj_out_ref[...] = adj[...]


def unpack_kernel(me_ref, x_ref, gate_inner_ref, step_ref):
    width = gate_inner_ref.shape[2]
    gate_inner_ref[:, 0, :] = x_ref[0, 0, :, :width]
    gate_inner_ref[:, 1, :] = x_ref[0, 0, :, width : 2 * width]
    step_ref[...] = x_ref[0, 0, :, 2 * width : 2 * width + step_ref.shape[1]]


def place_kernel(me_ref, x_ref, out_ref):
    out_ref[...] = x_ref[0, 0]


def place(x, kernel, shapes):
    _, n, piece, cols = x.shape

    def spec(shape):
        zeros = (0,) * (len(shape) - 1)
        return pl.BlockSpec((piece,) + shape[1:], lambda p, k, me: (p * n + (me[0] ^ k),) + zeros)

    return pl.pallas_call(
        kernel,
        grid_spec=pltpu.PrefetchScalarGridSpec(
            num_scalar_prefetch=1,
            grid=(2, n),
            in_specs=[pl.BlockSpec((1, 1, piece, cols), lambda p, k, me: (p, k, 0, 0))],
            out_specs=[spec(shape) for shape in shapes],
        ),
        out_shape=[jax.ShapeDtypeStruct(shape, f32) for shape in shapes],
        name="place",
    )(lax.axis_index("rows").astype(jnp.int32)[None], x)


def rows_spec(cols, order):
    return pl.BlockSpec((LB, cols), lambda i: (order(i), 0))


def line_spec(order):
    return pl.BlockSpec((NSUB, 1, L), lambda i: (order(i), 0, 0))


def whole_spec(shape):
    return pl.BlockSpec(shape, lambda i: (0,) * len(shape), pipeline_mode=pl.Buffered(1))


def smem_spec():
    return pl.BlockSpec(memory_space=pltpu.SMEM)


VMEM_LIMIT = 60 * 1024 * 1024


def run_fwd(first_block, lengths, hidden, gain, wgi, wss, cp, sp, hp, v_in, state_in):
    tokens, full = hidden.shape
    width = wgi.shape[1] // 2
    lines = tokens // L

    def same(i):
        return i

    return pl.pallas_call(
        functools.partial(fwd_kernel, first_block),
        grid=(tokens // LB,),
        in_specs=[
            smem_spec(),
            rows_spec(full, same),
            whole_spec(gain.shape),
            whole_spec(wgi.shape),
            whole_spec(wss.shape),
            whole_spec(cp.shape),
            whole_spec(sp.shape),
            whole_spec(hp.shape),
            whole_spec(v_in.shape),
            whole_spec(state_in.shape),
        ],
        out_specs=[
            rows_spec(full, same),
            line_spec(same),
            rows_spec(width, same),
            rows_spec(width + 2 * L, same),
            rows_spec(width, same),
            rows_spec(width, same),
            pl.BlockSpec((NSUB, STATE, width), lambda i: (i, 0, 0)),
            line_spec(same),
            pl.BlockSpec(v_in.shape, lambda i: (0, 0)),
            pl.BlockSpec(state_in.shape, lambda i: (0, 0)),
        ],
        out_shape=[
            jax.ShapeDtypeStruct((tokens, full), bf16),
            jax.ShapeDtypeStruct((lines, 1, L), f32),
            jax.ShapeDtypeStruct((tokens, width), f32),
            jax.ShapeDtypeStruct((tokens, width + 2 * L), f32),
            jax.ShapeDtypeStruct((tokens, width), f32),
            jax.ShapeDtypeStruct((tokens, width), f32),
            jax.ShapeDtypeStruct((lines, STATE, width), f32),
            jax.ShapeDtypeStruct((lines, 1, L), f32),
            jax.ShapeDtypeStruct(v_in.shape, f32),
            jax.ShapeDtypeStruct(state_in.shape, f32),
        ],
        scratch_shapes=[
            pltpu.VMEM((LB + 8, width + L), f32),
            pltpu.VMEM((STATE, width), f32),
        ],
        compiler_params=pltpu.CompilerParams(
            dimension_semantics=("arbitrary",), vmem_limit_bytes=VMEM_LIMIT
        ),
        name="mixer_fwd",
    )(lengths, hidden, gain, wgi, wss, cp, sp, hp, v_in, state_in)


def run_mid(first_block, lengths, cot, w_out, gated, cp):
    tokens, full = cot.shape
    width = gated.shape[1]
    lines = tokens // L

    def same(i):
        return i

    return pl.pallas_call(
        functools.partial(mid_kernel, first_block),
        grid=(tokens // LB,),
        in_specs=[
            smem_spec(),
            rows_spec(full, same),
            whole_spec(w_out.shape),
            rows_spec(width, same),
            whole_spec(cp.shape),
        ],
        out_specs=[rows_spec(width, same), line_spec(same)],
        out_shape=[
            jax.ShapeDtypeStruct((tokens, width), f32),
            jax.ShapeDtypeStruct((lines, 1, L), f32),
        ],
        compiler_params=pltpu.CompilerParams(
            dimension_semantics=("arbitrary",), vmem_limit_bytes=VMEM_LIMIT
        ),
        name="mixer_mid",
    )(lengths, cot, w_out, gated, cp)


def run_bwd(
    inner_total, first_block, lengths, gate, rest, gs, y, st, gsum, gdot, cp, sp, hp, v_in, q_in,
    adj_in, send_in,
):
    tokens, width = gate.shape
    lines = tokens // L
    blocks = tokens // LB

    def back(i):
        return blocks - 1 - i

    def halo(i):
        return (jnp.maximum(back(i) * (LB // 8) - 1, 0), 0)

    return pl.pallas_call(
        functools.partial(bwd_kernel, float(inner_total), first_block),
        grid=(blocks,),
        in_specs=[
            smem_spec(),
            rows_spec(width, back),
            rows_spec(width + 2 * L, back),
            pl.BlockSpec((8, width + 2 * L), halo),
            rows_spec(width, back),
            rows_spec(width, back),
            pl.BlockSpec((NSUB, STATE, width), lambda i: (back(i), 0, 0)),
            line_spec(back),
            line_spec(back),
            whole_spec(cp.shape),
            whole_spec(sp.shape),
            whole_spec(hp.shape),
            whole_spec(v_in.shape),
            whole_spec(q_in.shape),
            whole_spec(adj_in.shape),
            whole_spec(send_in.shape),
        ],
        out_specs=[
            rows_spec(2 * width + L, back),
            rows_spec(L, back),
            line_spec(back),
            line_spec(back),
            pl.BlockSpec((8, width), lambda i: (0, 0)),
            pl.BlockSpec((8, L), lambda i: (0, 0)),
            pl.BlockSpec((8, L), lambda i: (0, 0)),
            pl.BlockSpec(q_in.shape, lambda i: (0, 0)),
            pl.BlockSpec(adj_in.shape, lambda i: (0, 0)),
        ],
        out_shape=[
            jax.ShapeDtypeStruct((tokens, 2 * width + L), bf16),
            jax.ShapeDtypeStruct((tokens, L), f32),
            jax.ShapeDtypeStruct((lines, 1, L), f32),
            jax.ShapeDtypeStruct((lines, 1, L), f32),
            jax.ShapeDtypeStruct((8, width), f32),
            jax.ShapeDtypeStruct((8, L), f32),
            jax.ShapeDtypeStruct((8, L), f32),
            jax.ShapeDtypeStruct(q_in.shape, f32),
            jax.ShapeDtypeStruct(adj_in.shape, f32),
        ],
        scratch_shapes=[
            pltpu.VMEM((LB + 8, width + L), f32),
            pltpu.VMEM((8, width + L), f32),
            pltpu.VMEM((STATE, width), f32),
            pltpu.VMEM((STATE, width), f32),
        ],
        compiler_params=pltpu.CompilerParams(
            dimension_semantics=("arbitrary",), vmem_limit_bytes=VMEM_LIMIT
        ),
        name="mixer_bwd",
    )(lengths, gate, rest, rest, gs, y, st, gsum, gdot, cp, sp, hp, v_in, q_in, adj_in, send_in)


def pack_params(conv_inner, conv_inner_bias, conv_shared, conv_shared_bias, step_bias, log_decay,
                skip_gain, gate_gain):
    width = conv_inner.shape[1]
    heads = step_bias.shape[0]
    skip = jnp.repeat(skip_gain, HEAD)
    cp = jnp.concatenate(
        [conv_inner, conv_inner_bias[None], skip[None], gate_gain[None], jnp.zeros((1, width), f32)],
        axis=0,
    )
    sp = jnp.concatenate([conv_shared, conv_shared_bias[None], jnp.zeros((3, L), f32)], axis=0)
    hp = jnp.zeros((8, L), f32)
    hp = hp.at[0, :heads].set(step_bias).at[1, :heads].set(-jnp.exp(log_decay))
    return cp, sp, hp


def exchange_kernel(axis, x_ref, out_ref, slots, send_sem, recv_sem):
    me = lax.axis_index(axis)
    n = slots.shape[0]
    barrier = pltpu.get_barrier_semaphore()
    for k in range(1, n):
        peer = lax.rem(me + k, n)
        pl.semaphore_signal(barrier, inc=1, device_id={axis: peer})
    pl.semaphore_wait(barrier, n - 1)
    copies = []
    for k in range(1, n):
        peer = lax.rem(me + k, n)
        copy = pltpu.make_async_remote_copy(
            src_ref=x_ref,
            dst_ref=slots.at[k],
            send_sem=send_sem.at[k],
            recv_sem=recv_sem.at[k],
            device_id={axis: peer},
        )
        copy.start()
        copies.append(copy)
    for copy in copies:
        copy.wait()
    slots[0] = x_ref[...]
    total = slots[lax.rem(me, n)]
    for d in range(1, n):
        total = total + slots[lax.rem(me - d + n, n)]
    out_ref[...] = total


def sum_small(x, axis, collective_id):
    n = lax.axis_size(axis)
    return pl.pallas_call(
        functools.partial(exchange_kernel, axis),
        out_shape=jax.ShapeDtypeStruct(x.shape, f32),
        in_specs=[pl.BlockSpec(memory_space=pltpu.VMEM)],
        out_specs=pl.BlockSpec(memory_space=pltpu.VMEM),
        scratch_shapes=[
            pltpu.VMEM((n,) + x.shape, f32),
            pltpu.SemaphoreType.DMA((n,)),
            pltpu.SemaphoreType.DMA((n,)),
        ],
        compiler_params=pltpu.CompilerParams(collective_id=collective_id, has_side_effects=True),
        name="sum_small",
    )(x)


def after(x, *deps):
    deps = [d for d in deps if d is not None]
    return lax.optimization_barrier((x, *deps))[0]


SCALE = 16384.0


def encode(x, bound, kind):
    if bound is not None:
        x = x * (SCALE / bound)
    return x.astype(kind)


def decode(x, bound):
    x = x.astype(f32)
    return x if bound is None else x * (bound / SCALE)


class ScatterLine:

    def __init__(self, send, own, bound, kind):
        self.n = lax.axis_size("heads")
        self.chips = self.n // 2
        self.z = lax.axis_index("heads") >> 1
        self.own, self.kind, self.bound = own, kind, bound
        self.moving, self.out = [None, None], [None, None]
        self.message = encode(send, bound, kind)

    def swap(self):
        pairs = [(i, i ^ 1) for i in range(self.n)]
        self.got = lax.ppermute(self.message, "heads", pairs)

    def block(self, b):
        mine = lax.dynamic_index_in_dim(self.own, b, 0, keepdims=False)
        theirs = lax.dynamic_index_in_dim(self.got, b, 0, keepdims=False)
        return mine + decode(theirs, self.bound)

    def pack(self, r):
        last = self.chips - 1
        for way in range(2):
            b = last - r + self.z if way == 0 else r - last + self.z
            total = self.block(jnp.clip(b, 0, last))
            if r > 0:
                total = total + decode(self.moving[way], self.bound)
            self.out[way] = encode(total, self.bound, self.kind)

    def hold(self, *deps):
        self.moving = [after(m, *deps) for m in self.moving]

    def send(self, r):
        last = self.chips - 1
        out = lax.optimization_barrier(tuple(self.out))
        for way in range(2):
            chips = range(r + 1) if way == 0 else range(last - r, last + 1)
            hop = 2 if way == 0 else -2
            pairs = [(2 * k + c, 2 * k + c + hop) for k in chips for c in range(2)]
            self.moving[way] = lax.ppermute(out[way], "heads", pairs)
        self.moving = list(lax.optimization_barrier(tuple(self.moving)))

    def rest(self, r):
        for k in range(r, self.chips - 1):
            self.pack(k)
            self.send(k)

    def total(self):
        total = self.block(self.z)
        for way in range(2):
            if self.moving[way] is not None:
                total = total + decode(self.moving[way], self.bound)
        return total


class RowSum:

    def __init__(self, x, bound):
        self.n = lax.axis_size("rows")
        self.me = lax.axis_index("rows")
        self.bits = self.n.bit_length() - 1
        self.bound = bound
        piece = x.shape[0] // (2 * self.n)
        cut = x.reshape((2,) + (2,) * self.bits + (piece, x.shape[1]))
        self.cur = [cut[0], cut[1]]
        self.order = [[(k + part) % self.bits for k in range(self.bits)] for part in range(2)]
        self.left = [list(range(self.bits))[::-1] for _ in range(2)]

    def move(self, x, bit):
        return lax.ppermute(x, "rows", [(i, i ^ (1 << bit)) for i in range(self.n)])

    def reduce(self, k):
        for part in range(2):
            bit, left = self.order[part][k], self.left[part]
            mine = (self.me >> bit) & 1
            axis = left.index(bit)
            left.remove(bit)
            cur = self.cur[part]
            send = lax.dynamic_index_in_dim(cur, 1 - mine, axis, keepdims=False)
            keep = lax.dynamic_index_in_dim(cur, mine, axis, keepdims=False)
            got = self.move(encode(send, self.bound, jnp.float16), bit)
            self.cur[part] = keep + decode(got, self.bound)

    def hold(self, *deps):
        self.cur = [after(cur, *deps) for cur in self.cur]

    def spread(self):
        pieces = [{0: encode(cur, self.bound, jnp.float16)} for cur in self.cur]
        for k in reversed(range(self.bits)):
            far = []
            for part in range(2):
                bit = self.order[part][k]
                for rel in list(pieces[part]):
                    pieces[part][rel ^ (1 << bit)] = self.move(pieces[part][rel], bit)
                    far.append((part, rel ^ (1 << bit)))
            held = lax.optimization_barrier(tuple(pieces[part][rel] for part, rel in far))
            for (part, rel), data in zip(far, held):
                pieces[part][rel] = data
        halves = [pieces[part][rel] for part in range(2) for rel in range(self.n)]
        whole = decode(jnp.stack(halves), self.bound)
        return whole.reshape((2, self.n) + whole.shape[1:])


def per_device(
    hidden_in, lengths, norm_gain, in_gate_inner, in_step, in_shared, conv_inner, conv_inner_bias,
    conv_shared, conv_shared_bias, step_bias, log_decay, skip_gain, gate_gain, out_weight, cotangent,
):
    tokens, local = hidden_in.shape
    full = in_gate_inner.shape[0]
    width = in_gate_inner.shape[2]
    heads = step_bias.shape[0]
    chips = full // local // 2
    lines = tokens // L
    inner_total = width * (full // local)
    core = lax.axis_index("heads") & 1
    source = hidden_in.astype(f32)

    part = tokens // 2
    part_lines = lines // 2
    part_blocks = part // LB

    def gather(x):
        return lax.all_gather(x, "heads", axis=1, tiled=True)

    hidden_all = [gather(hidden_in[:part]), gather(hidden_in[part:])]
    shared_all = lax.all_gather(in_shared, "heads", axis=1, tiled=True)
    gain_all = lax.all_gather(norm_gain, "heads", axis=0, tiled=True)
    cot_1 = gather(cotangent[part:])
    cot_all = [gather(cotangent[:part]), cot_1]
    wgi = in_gate_inner.reshape(full, 2 * width)
    step_pad = jnp.pad(in_step, ((0, 0), (0, L - heads)))
    wss = jnp.concatenate([shared_all.T, step_pad], axis=1)
    w_back = jnp.concatenate([wgi, step_pad], axis=1)

    def halves(w, axis):
        both = []
        for side in (1 - core, core):
            parts = [
                lax.dynamic_slice_in_dim(w, (2 * k + side) * local, local, axis) for k in range(chips)
            ]
            both.append(jnp.stack(parts))
        return both

    back_send, back_own = halves(w_back, 0)
    out_send, out_own = halves(out_weight, 1)
    w_size = jnp.sqrt(jnp.max(jnp.sum(jnp.square(w_back.astype(f32)), axis=1)))
    cp, sp, hp = pack_params(
        conv_inner, conv_inner_bias, conv_shared, conv_shared_bias, step_bias, log_decay,
        skip_gain, gate_gain,
    )

    hidden_all[0] = after(
        hidden_all[0], back_send, back_own, out_send, out_own, w_size, cp, sp, hp
    )
    v_rows = jnp.zeros((8, width + L), f32)
    state = jnp.zeros((STATE, width), f32)
    v_starts, fwd = [], []
    for i in range(2):
        v_starts.append(v_rows)
        *kept, v_rows, state = run_fwd(
            i * part_blocks, lengths, hidden_all[i], gain_all[None], wgi, wss, cp, sp, hp, v_rows, state
        )
        fwd.append(kept)
    normed, inv_rows, gate, rest, gated, y, st, gsum_part = zip(*fwd)
    inv_rms = jnp.concatenate([rows.reshape(part) for rows in inv_rows])
    gsum = sum_small(jnp.concatenate(gsum_part).reshape(lines, L), "heads", 1)

    live = (jnp.arange(tokens, dtype=jnp.int32) < jnp.sum(lengths[0])).astype(bf16)
    gate_rms = lax.rsqrt(gsum.reshape(tokens) / inner_total + EPSILON)
    scaled = []
    for i in range(2):
        span = slice(i * part, (i + 1) * part)
        value = gated[i] * gate_rms[span, None] * gate_gain[None, :]
        scaled.append(value.astype(bf16) * live[span, None])

    def project(w, v, axis):
        return lax.dot_general(w, v, (((axis,), (1,)), ((), ())), preferred_element_type=f32)

    mixed = [
        ScatterLine(
            project(out_send, scaled[i], 1), project(out_own, scaled[i], 1), None, jnp.float16
        )
        for i in range(2)
    ]
    ready = []
    for line in mixed:
        line.swap()
        line.pack(0)
        ready += line.out

    q_rows = jnp.zeros((8, width + L), f32)
    adj = jnp.zeros((STATE, width), f32)
    sent = jnp.zeros((STATE, width), f32)
    bwd, normal = [None, None], [None, None]
    for i in (1, 0):
        cot_late = after(cot_all[i], *ready)
        if i == 1:
            for line in mixed:
                line.send(0)
        else:
            normal[1].send(0)
        gs, gdot_part = run_mid(i * part_blocks, lengths, cot_late, out_weight, gated[i], cp)
        gdot = sum_small(gdot_part.reshape(part_lines, L), "heads", 3 - i)
        *kept, q_rows, adj = run_bwd(
            inner_total, i * part_blocks, lengths, gate[i], rest[i], gs, y[i], st[i],
            gsum[i * part_lines : (i + 1) * part_lines].reshape(part_lines, 1, L),
            gdot.reshape(part_lines, 1, L), cp, sp, hp, v_starts[i], q_rows, adj, sent,
        )
        sent = st[i][0]
        low, gsh, nd_part, size, pg, sg, hg = kept
        ready = []
        for line in mixed:
            line.hold(low)
            line.pack(2 - i)
            ready += line.out
        if i == 0:
            normal[1].hold(low)
            normal[1].pack(1)
            ready += normal[1].out
        bound = jnp.sqrt(size.reshape(part_lines, L)) * (1.01 * w_size) + 1e-30
        nd_part = after(nd_part.reshape(part_lines, L), *ready)
        for line in mixed:
            line.send(2 - i)
        if i == 0:
            normal[1].send(1)
        small = sum_small(jnp.concatenate([nd_part, bound], axis=0), "heads", 5 - i)
        bound = small[part_lines:].reshape(part)
        low_now = after(low, bound)
        normal[i] = ScatterLine(
            project(back_send, low_now, 2), project(back_own, low_now, 2), bound, jnp.float16
        )
        normal[i].swap()
        normal[i].pack(0)
        ready = list(normal[i].out)
        bwd[i] = (low, gsh, small[:part_lines].reshape(part), pg, sg, hg)
    low, gsh, norm_dot, pg, sg, hg = zip(*bwd)
    pg, sg, hg = pg[0] + pg[1], sg[0] + sg[1], hg[0] + hg[1]
    norm_dot = jnp.concatenate(norm_dot)

    late = [after(v, *ready) for v in scaled + list(low)]
    normal[0].send(0)
    normal[1].hold(*ready)
    normal[1].pack(2)
    grad_wout = sum(
        lax.dot_general(late[i], cot_all[i], (((0,), (0,)), ((), ())), preferred_element_type=f32)
        for i in range(2)
    )
    top_wout = jnp.max(jnp.abs(grad_wout))
    normal[1].send(2)
    grad_proj = sum(
        lax.dot_general(normed[i], late[2 + i], (((0,), (0,)), ((), ())), preferred_element_type=f32)
        for i in range(2)
    )
    top_proj = jnp.max(jnp.abs(grad_proj))
    sg = sum_small(after(sg, *ready), "heads", 6)
    tops = jnp.stack([top_proj, top_wout])
    tops = jnp.broadcast_to(jnp.repeat(tops * 1.01 + 1e-30, 8)[:, None], (16, L))
    wide = pg.reshape(8 * width // L, L)
    small = sum_small(jnp.concatenate([tops, sg, hg, wide], axis=0), "rows", 7)

    normal[0].hold(small)
    normal[0].pack(1)
    out = normal[0].out
    small = after(small, *out)
    gsh_all = after(jnp.concatenate(gsh), *out)
    for line in mixed:
        line.hold(*out)
    normal[0].send(1)
    top_proj, top_wout, sg, hg = small[0, 0], small[8, 0], small[16:24], small[24:32]
    pg = small[32:].reshape(8, width)
    sum_proj, sum_wout = RowSum(grad_proj, top_proj), RowSum(grad_wout, top_wout)
    for k in range(sum_proj.bits):
        sum_proj.reduce(k)
        sum_wout.reduce(k)
    mixed_out = []
    for line in mixed:
        line.rest(3)
        mixed_out.append(line.total())
    output = (source + jnp.concatenate(mixed_out, axis=1).T).astype(bf16)

    cut = gsh_all.T.reshape(chips, 2, L // (2 * chips), tokens)
    gsh_own = lax.dynamic_index_in_dim(cut, core, 1, keepdims=False)
    gsh_send = lax.dynamic_index_in_dim(cut, 1 - core, 1, keepdims=False)
    shared = ScatterLine(gsh_send, gsh_own, None, f32)
    shared.swap()
    shared.rest(0)
    low_shared = lax.all_gather(shared.total().astype(bf16), "heads", axis=0, tiled=True)
    shared_raw = jnp.concatenate([raw[:, width : width + L] for raw in rest])
    norm_dot = norm_dot + jnp.sum(low_shared.T.astype(f32) * shared_raw, axis=1)
    normed_local = (source * inv_rms[:, None] * norm_gain[None, :]).astype(bf16)
    grad_shared_w = lax.dot_general(
        low_shared, normed_local, (((1,), (0,)), ((), ())), preferred_element_type=f32
    )
    grad_shared_w = lax.psum(grad_shared_w, "rows")

    normal[0].pack(2)
    sum_proj.hold(*normal[0].out)
    sum_wout.hold(*normal[0].out)
    normal[0].send(2)
    grad_proj, grad_step = place(
        sum_proj.spread(), unpack_kernel, [(full, 2, width), (full, heads)]
    )
    (grad_wout,) = place(sum_wout.spread(), place_kernel, [grad_wout.shape])

    totals = []
    for line in normal:
        line.rest(3)
        totals.append(line.total())
    grad_normed = jnp.concatenate(totals, axis=1) + lax.dot_general(
        in_shared, low_shared, (((0,), (0,)), ((), ())), preferred_element_type=f32
    )
    grad_normed = grad_normed.T
    grad_gain_norm = jnp.sum(grad_normed * source * inv_rms[:, None], axis=0)
    grad_source = (
        inv_rms[:, None] * norm_gain[None, :] * grad_normed
        - source * (inv_rms * inv_rms * norm_dot / full)[:, None]
    )
    grad_input = cotangent.astype(f32) + grad_source
    grad_gain_norm = sum_small(grad_gain_norm.reshape(local // L, L), "rows", 8).reshape(local)
    return (
        output,
        grad_input,
        grad_gain_norm,
        grad_proj,
        grad_step,
        grad_shared_w,
        pg[0:4],
        pg[4],
        sg[0:4],
        sg[4],
        hg[0, :heads],
        hg[1, :heads],
        pg[5].reshape(heads, HEAD).sum(axis=1),
        pg[6],
        grad_wout,
    )


def solution(mesh):
    return jax.shard_map(
        per_device,
        mesh=mesh,
        in_specs=(
            P("rows", "heads"), P("rows", None), P("heads"), P(None, None, "heads"),
            P(None, "heads"), P(None, "heads"), P(None, "heads"), P("heads"), P(), P(),
            P("heads"), P("heads"), P("heads"), P("heads"), P("heads", None), P("rows", "heads"),
        ),
        out_specs=(
            P("rows", "heads"), P("rows", "heads"), P("heads"), P(None, None, "heads"),
            P(None, "heads"), P(None, "heads"), P(None, "heads"), P("heads"), P(), P(),
            P("heads"), P("heads"), P("heads"), P("heads"), P("heads", None),
        ),
        check_vma=False,
    )
```

```python
import functools

import jax
import jax.numpy as jnp
from jax import lax
from jax.experimental import pallas as pl
from jax.experimental.pallas import tpu as pltpu
from jax.sharding import PartitionSpec as P


EPSILON = 1e-05
L = 128
LB = 512
NSUB = LB // L
HEAD = 64
STATE = 64
f32 = jnp.float32
bf16 = jnp.bfloat16


def mm(a, b, ca=1, cb=0):
    return lax.dot_general(a, b, (((ca,), (cb,)), ((), ())), preferred_element_type=f32)


def split(x):
    hi = x.astype(bf16)
    return hi, (x - hi.astype(f32)).astype(bf16)


def mm3(a, b, ca=1, cb=0):
    ah, al = split(a)
    bh, bl = split(b)
    return mm(ah, bh, ca, cb) + mm(ah, bl, ca, cb) + mm(al, bh, ca, cb)


def mm_exact_left(mask, x):
    hi = x.astype(bf16)
    rest = x - hi.astype(f32)
    mid = rest.astype(bf16)
    low = (rest - mid.astype(f32)).astype(bf16)
    return mm(mask, hi) + mm(mask, mid) + mm(mask, low)


def block_diag(x, first):
    zero = jnp.zeros_like(x)
    return jnp.concatenate([jnp.where(first, x, zero), jnp.where(first, zero, x)], axis=0)


def bounds_of(len_ref):
    b0 = len_ref[0, 0]
    b1 = b0 + len_ref[0, 1]
    b2 = b1 + len_ref[0, 2]
    b3 = b2 + len_ref[0, 3]
    return b0, b1, b2, b3


def start_of(bounds, t):
    start = jnp.zeros_like(t)
    for b in bounds:
        start = jnp.where(t >= b, b, start)
    return start


def to_row(col):
    return jnp.transpose(jnp.broadcast_to(col, (L, L)))[0:1, :]


def to_col(row):
    return jnp.transpose(jnp.broadcast_to(row, (L, L)))


def pair_cols(a, q, first):
    return jnp.where(first, a[:, 2 * q : 2 * q + 1], a[:, 2 * q + 1 : 2 * q + 2])


def sigmoid(v):
    return 0.5 + 0.5 * jnp.tanh(0.5 * v)


def softplus(v):
    return jnp.maximum(v, 0.0) + jnp.log1p(jnp.exp(-jnp.abs(v)))


def shifted(win, m):
    if m == 0:
        return win[8:, :]
    return pltpu.roll(win, m, 0)[8:, :]


def chunk_columns(hp_ref, step, bounds, base):
    tcol = lax.broadcasted_iota(jnp.int32, (L, L), 0) + base
    trow = lax.broadcasted_iota(jnp.int32, (L, L), 1) + base
    start_col = start_of(bounds, tcol)
    start_end = start_of(bounds, base + (L - 1))
    raw = step + hp_ref[0:1, :]
    dt = softplus(raw)
    decay = hp_ref[1:2, :] * dt
    lower = jnp.where(trow <= tcol, 1.0, 0.0).astype(bf16)
    cum = mm_exact_left(lower, decay)
    cum_end = cum[L - 1 : L, :]
    ecum = jnp.where(start_col < base, jnp.exp(cum), 0.0)
    wend = jnp.where(tcol >= start_end, jnp.exp(cum_end - cum), 0.0)
    carried_end = (start_end < base).astype(f32)
    cdec = jnp.exp(cum_end) * carried_end
    return tcol, trow, start_col, start_end, raw, dt, decay, cum, ecum, wend, cdec


def fwd_kernel(
    len_ref, h_ref, gain_ref, wgi_ref, wss_ref, cp_ref, sp_ref, hp_ref,
    normed_ref, inv_ref, gate_ref, rest_ref, gated_ref, y_ref, st_ref, gsum_ref,
    vbuf, state,
):
    blk = pl.program_id(0)
    width = gate_ref.shape[1]
    full = h_ref.shape[1]
    pairs = width // L

    @pl.when(blk == 0)
    def _():
        vbuf[0:8, :] = jnp.zeros((8, vbuf.shape[1]), f32)
        state[...] = jnp.zeros(state.shape, f32)

    piece = 256

    def norm_rows(s, carry):
        rows = pl.ds(pl.multiple_of(s * L, L), L)
        acc = jnp.zeros((L, piece), f32)
        for k in range(full // piece):
            x = h_ref[rows, k * piece : (k + 1) * piece].astype(f32)
            acc = acc + x * x
        inv = lax.rsqrt(jnp.sum(acc, axis=1, keepdims=True) / full + EPSILON)
        for k in range(full // piece):
            cols = slice(k * piece, (k + 1) * piece)
            x = h_ref[rows, cols].astype(f32)
            normed_ref[rows, cols] = (x * inv * gain_ref[0:1, cols]).astype(bf16)
        inv_ref[s] = to_row(inv)
        return carry

    lax.fori_loop(0, NSUB, norm_rows, 0)
    normed = normed_ref[...]
    gate_ref[...] = mm(normed, wgi_ref[:, :width])
    inner = mm(normed, wgi_ref[:, width:])
    vbuf[8:, :width] = inner
    rest_ref[:, :width] = inner
    tail = mm(normed, wss_ref[...])
    vbuf[8:, width:] = tail[:, :L]
    rest_ref[:, width:] = tail

    bounds = bounds_of(len_ref)
    first = lax.broadcasted_iota(jnp.int32, (L, L), 1) < HEAD

    def chunk(s, carry):
        r0 = pl.multiple_of(s * L, L)
        rows = pl.ds(r0, L)
        base = blk * LB + s * L
        step = rest_ref[rows, width + L :]
        tcol, trow, start_col, _, _, dt, _, cum, ecum, wend, cdec = chunk_columns(
            hp_ref, step, bounds, base
        )
        cum_t = jnp.transpose(cum)
        mask = (trow <= tcol) & (trow >= start_col)
        valid = [tcol - m >= start_col for m in range(4)]

        def conv(cols, taps):
            win = vbuf[pl.ds(r0, L + 8), cols]
            pre = taps[4:5, :] + taps[3:4, :] * win[8:, :]
            for m in range(1, 4):
                pre = pre + taps[3 - m : 4 - m, :] * jnp.where(valid[m], shifted(win, m), 0.0)
            return pre

        pre_s = conv(slice(width, width + L), sp_ref)
        act = pre_s * sigmoid(pre_s)
        b_map = act[:, :STATE]
        c_map = act[:, STATE:]
        scores = jnp.where(mask, mm3(c_map, b_map, 1, 1), 0.0)
        square = jnp.zeros((L, L), f32)
        for q in range(pairs):
            cols = slice(q * L, (q + 1) * L)
            pre = conv(cols, cp_ref.at[:, cols])
            xin = pre * sigmoid(pre)
            xp = xin * pair_cols(dt, q, first)
            xh, xl = split(xp)
            bdh, bdl = block_diag(xh, first), block_diag(xl, first)
            mix = []
            for h in (2 * q, 2 * q + 1):
                spread = jnp.minimum(cum[:, h : h + 1] - cum_t[h : h + 1, :], 0.0)
                mix.append(jnp.exp(spread) * scores)
            mh, ml = split(jnp.concatenate(mix, axis=1))
            both = mm(mh, jnp.concatenate([bdh, bdl], axis=1))
            y = both[:, :L] + both[:, L:] + mm(ml, bdh)
            st = state[:, cols]
            st_ref[s, :, cols] = st
            y = y + mm3(c_map, st) * pair_cols(ecum, q, first)
            xw = xp * pair_cols(wend, q, first)
            state[:, cols] = mm3(b_map, xw, 0, 0) + st * pair_cols(cdec, q, first[0:1, :])
            y_ref[rows, cols] = y
            gate = gate_ref[rows, cols]
            gated = (y + cp_ref[5:6, cols] * xin) * (gate * sigmoid(gate))
            gated_ref[rows, cols] = gated
            square = square + gated * gated
        gsum_ref[s] = to_row(jnp.sum(square, axis=1, keepdims=True))
        return carry

    lax.fori_loop(0, NSUB, chunk, 0)
    vbuf[0:8, :] = vbuf[LB : LB + 8, :]


def mid_kernel(len_ref, cot_ref, w_ref, gated_ref, cp_ref, gs_ref, gdot_ref):
    blk = pl.program_id(0)
    live = bounds_of(len_ref)[3]
    t = lax.broadcasted_iota(jnp.int32, gs_ref.shape, 0) + blk * LB
    gs = jnp.where(t < live, mm(cot_ref[...], w_ref[...], 1, 1), 0.0)
    gs_ref[...] = gs
    dots = jnp.sum(gs * cp_ref[6:7, :] * gated_ref[...], axis=1, keepdims=True)
    for s in range(NSUB):
        gdot_ref[s] = to_row(dots[s * L : (s + 1) * L, :])


def bwd_kernel(
    inner_total,
    len_ref, gate_ref, rest_ref, halo_ref, gs_ref, y_ref, st_ref, gsum_ref, gdot_ref,
    cp_ref, sp_ref, hp_ref,
    low_ref, gsh_ref, nd_ref, size_ref, pg_ref, sg_ref, hg_ref,
    vbuf, qnext, adj, send,
):
    step_id = pl.program_id(0)
    blk = pl.num_programs(0) - 1 - step_id
    width = gate_ref.shape[1]
    pairs = width // L

    @pl.when(step_id == 0)
    def _():
        qnext[...] = jnp.zeros(qnext.shape, f32)
        adj[...] = jnp.zeros(adj.shape, f32)
        send[...] = jnp.zeros(send.shape, f32)
        pg_ref[...] = jnp.zeros(pg_ref.shape, f32)
        sg_ref[...] = jnp.zeros(sg_ref.shape, f32)
        hg_ref[...] = jnp.zeros(hg_ref.shape, f32)

    vbuf[0:8, :] = halo_ref[:, : width + L]
    vbuf[8:, :] = rest_ref[:, : width + L]
    bounds = bounds_of(len_ref)
    first = lax.broadcasted_iota(jnp.int32, (L, L), 1) < HEAD
    lane = lax.broadcasted_iota(jnp.int32, (L, L), 1)
    half = lax.broadcasted_iota(jnp.int32, (L, L), 0) // HEAD

    def chunk(i, carry):
        s = NSUB - 1 - i
        r0 = pl.multiple_of(s * L, L)
        rows = pl.ds(r0, L)
        base = blk * LB + s * L
        step = rest_ref[rows, width + L :]
        tcol, trow, start_col, start_end, raw, dt, decay, cum, ecum, wend, cdec = chunk_columns(
            hp_ref, step, bounds, base
        )
        cum_t = jnp.transpose(cum)
        mask_t = (trow >= tcol) & (start_of(bounds, trow) <= tcol)
        valid = [tcol - m >= start_col for m in range(4)]
        valid_up = [start_of(bounds, tcol + m) <= tcol for m in range(4)]
        gate_rms_row = lax.rsqrt(gsum_ref[s] / inner_total + EPSILON)
        pull_row = gate_rms_row * gate_rms_row * gate_rms_row * gdot_ref[s] / inner_total
        gate_rms = to_col(gate_rms_row)
        pull = to_col(pull_row)

        def conv(cols, taps):
            win = vbuf[pl.ds(r0, L + 8), cols]
            seen = [win[8:, :]]
            pre = taps[4:5, :] + taps[3:4, :] * seen[0]
            for m in range(1, 4):
                seen.append(jnp.where(valid[m], shifted(win, m), 0.0))
                pre = pre + taps[3 - m : 4 - m, :] * seen[m]
            return seen, pre

        def conv_back(q, seen, cols, taps, grad_ref, grad_cols):
            win = jnp.concatenate([q, qnext[:, cols]], axis=0)
            qnext[:, cols] = q[0:8, :]
            grad = taps[3:4, :] * q
            for m in range(1, 4):
                up = pltpu.roll(win, L + 8 - m, 0)[:L, :]
                grad = grad + taps[3 - m : 4 - m, :] * jnp.where(valid_up[m], up, 0.0)
            for m in range(4):
                k = 3 - m
                grad_ref[k : k + 1, grad_cols] += jnp.sum(q * seen[m], axis=0, keepdims=True)
            grad_ref[4:5, grad_cols] += jnp.sum(q, axis=0, keepdims=True)
            return grad

        seen_s, pre_s = conv(slice(width, width + L), sp_ref)
        sig_s = sigmoid(pre_s)
        act = pre_s * sig_s
        b_map = act[:, :STATE]
        c_map = act[:, STATE:]
        scores_t = jnp.where(mask_t, mm3(b_map, c_map, 1, 1), 0.0)
        d_scores = jnp.zeros((L, L), f32)
        d_b = jnp.zeros((L, STATE), f32)
        d_c = jnp.zeros((L, STATE), f32)
        reduced = jnp.zeros((2 * L, L), f32)
        ends = jnp.zeros((8, L), f32)
        norm_dot = jnp.zeros((L, L), f32)
        size = jnp.zeros((L, L), f32)
        for q in range(pairs):
            cols = slice(q * L, (q + 1) * L)
            taps = cp_ref.at[:, cols]
            skip = cp_ref[5:6, cols]
            seen, pre = conv(cols, taps)
            sig = sigmoid(pre)
            xin = pre * sig
            dtx = pair_cols(dt, q, first)
            xp = xin * dtx
            y = y_ref[rows, cols]
            ho = y + skip * xin
            gate = gate_ref[rows, cols]
            gsig = sigmoid(gate)
            sl = gate * gsig
            gated = ho * sl
            gs = gs_ref[rows, cols]
            pg_ref[6:7, cols] += jnp.sum(gs * gated * gate_rms, axis=0, keepdims=True)
            gg = gate_rms * cp_ref[6:7, cols] * gs - gated * pull
            gy = gg * sl
            low_gate = (gg * ho * (gsig * (1.0 + gate * (1.0 - gsig)))).astype(bf16)
            low_ref[rows, cols] = low_gate
            pg_ref[5:6, cols] += jnp.sum(gy * xin, axis=0, keepdims=True)

            yh, yl = split(gy)
            bdh, bdl = block_diag(yh, first), block_diag(yl, first)
            xh, xl = split(xp)
            d_mix = mm(
                jnp.concatenate([xh, xl], axis=1), jnp.concatenate([bdh, bdh], axis=1), 1, 1
            ) + mm(xh, bdl, 1, 1)
            mix = []
            for k in range(2):
                h = 2 * q + k
                spread = jnp.minimum(cum_t[h : h + 1, :] - cum[:, h : h + 1], 0.0)
                factor = jnp.exp(spread)
                d_scores = d_scores + d_mix[:, k * L : (k + 1) * L] * factor
                mix.append(factor * scores_t)
            mh, ml = split(jnp.concatenate(mix, axis=1))
            both = mm(mh, jnp.concatenate([bdh, bdl], axis=1))
            dxp = both[:, :L] + both[:, L:] + mm(ml, bdh)
            wendx = pair_cols(wend, q, first)
            a_in = adj[:, cols]
            dxp = dxp + mm3(b_map, a_in) * wendx
            xw = xp * wendx
            gyw = gy * pair_cols(ecum, q, first)
            s_in = st_ref[s, :, cols]
            d_b = d_b + mm3(xw, a_in, 1, 1)
            d_c = d_c + mm3(gyw, s_in, 1, 1)
            adj[:, cols] = mm3(c_map, gyw, 0, 0) + a_in * pair_cols(cdec, q, first[0:1, :])
            heads = jnp.where(lane == 2 * q + half, 1.0, 0.0).astype(bf16)
            zh, zl = split(jnp.concatenate([gy * y - dxp * xp, dxp * xin], axis=0))
            reduced = reduced + mm(zh, heads) + mm(zl, heads)
            end = jnp.broadcast_to(
                jnp.sum(a_in * send[:, cols], axis=0, keepdims=True), (8, L)
            )
            eh, el = split(end)
            ends = ends + mm(eh, heads) + mm(el, heads)
            send[:, cols] = s_in

            dxin = dxp * dtx + skip * gy
            qv = dxin * (sig * (1.0 + pre * (1.0 - sig)))
            grad = conv_back(qv, seen, cols, taps, pg_ref, cols)
            low_inner = grad.astype(bf16)
            low_ref[rows, width + q * L : width + (q + 1) * L] = low_inner
            wide_gate, wide_inner = low_gate.astype(f32), low_inner.astype(f32)
            norm_dot = norm_dot + wide_gate * gate + wide_inner * seen[0]
            size = size + wide_gate * wide_gate + wide_inner * wide_inner

        d_scores = jnp.where(mask_t, d_scores, 0.0)
        d_b = d_b + mm3(d_scores, c_map)
        d_c = d_c + mm3(d_scores, b_map, 0, 0)
        d_act = jnp.concatenate([d_b, d_c], axis=1)
        q_s = d_act * (sig_s * (1.0 + pre_s * (1.0 - sig_s)))
        shared_cols = slice(width, width + L)
        gsh_ref[rows, :] = conv_back(q_s, seen_s, shared_cols, sp_ref, sg_ref, slice(0, L))

        tail = jnp.where(tcol >= start_end, ends[0:1, :], 0.0)
        keep = jnp.where(mask_t, 1.0, 0.0).astype(bf16)
        d_decay = mm_exact_left(keep, reduced[:L, :]) + tail
        d_dt = reduced[L:, :] + d_decay * hp_ref[1:2, :]
        d_raw = d_dt * sigmoid(raw)
        hg_ref[0:1, :] += jnp.sum(d_raw, axis=0, keepdims=True)
        hg_ref[1:2, :] += jnp.sum(d_decay * decay, axis=0, keepdims=True)
        low_step = d_raw.astype(bf16)
        low_ref[rows, 2 * width :] = low_step
        wide_step = low_step.astype(f32)
        norm_dot = norm_dot + wide_step * step
        size = size + wide_step * wide_step
        nd_ref[s] = to_row(jnp.sum(norm_dot, axis=1, keepdims=True))
        size_ref[s] = to_row(jnp.sum(size, axis=1, keepdims=True))
        return carry

    lax.fori_loop(0, NSUB, chunk, 0)


def unpack_kernel(me_ref, x_ref, gate_inner_ref, step_ref):
    width = gate_inner_ref.shape[2]
    gate_inner_ref[:, 0, :] = x_ref[0, 0, :, :width]
    gate_inner_ref[:, 1, :] = x_ref[0, 0, :, width : 2 * width]
    step_ref[...] = x_ref[0, 0, :, 2 * width : 2 * width + step_ref.shape[1]]


def place_kernel(me_ref, x_ref, out_ref):
    out_ref[...] = x_ref[0, 0]


def place(x, kernel, shapes):
    _, n, piece, cols = x.shape

    def spec(shape):
        zeros = (0,) * (len(shape) - 1)
        return pl.BlockSpec((piece,) + shape[1:], lambda p, k, me: (p * n + (me[0] ^ k),) + zeros)

    return pl.pallas_call(
        kernel,
        grid_spec=pltpu.PrefetchScalarGridSpec(
            num_scalar_prefetch=1,
            grid=(2, n),
            in_specs=[pl.BlockSpec((1, 1, piece, cols), lambda p, k, me: (p, k, 0, 0))],
            out_specs=[spec(shape) for shape in shapes],
        ),
        out_shape=[jax.ShapeDtypeStruct(shape, f32) for shape in shapes],
        name="place",
    )(lax.axis_index("rows").astype(jnp.int32)[None], x)


def rows_spec(cols, order):
    return pl.BlockSpec((LB, cols), lambda i: (order(i), 0))


def line_spec(order):
    return pl.BlockSpec((NSUB, 1, L), lambda i: (order(i), 0, 0))


def whole_spec(shape):
    return pl.BlockSpec(shape, lambda i: (0,) * len(shape), pipeline_mode=pl.Buffered(1))


def smem_spec():
    return pl.BlockSpec(memory_space=pltpu.SMEM)


VMEM_LIMIT = 60 * 1024 * 1024


def run_fwd(lengths, hidden, gain, wgi, wss, cp, sp, hp):
    tokens, full = hidden.shape
    width = wgi.shape[1] // 2
    lines = tokens // L

    def same(i):
        return i

    return pl.pallas_call(
        fwd_kernel,
        grid=(tokens // LB,),
        in_specs=[
            smem_spec(),
            rows_spec(full, same),
            whole_spec(gain.shape),
            whole_spec(wgi.shape),
            whole_spec(wss.shape),
            whole_spec(cp.shape),
            whole_spec(sp.shape),
            whole_spec(hp.shape),
        ],
        out_specs=[
            rows_spec(full, same),
            line_spec(same),
            rows_spec(width, same),
            rows_spec(width + 2 * L, same),
            rows_spec(width, same),
            rows_spec(width, same),
            pl.BlockSpec((NSUB, STATE, width), lambda i: (i, 0, 0)),
            line_spec(same),
        ],
        out_shape=[
            jax.ShapeDtypeStruct((tokens, full), bf16),
            jax.ShapeDtypeStruct((lines, 1, L), f32),
            jax.ShapeDtypeStruct((tokens, width), f32),
            jax.ShapeDtypeStruct((tokens, width + 2 * L), f32),
            jax.ShapeDtypeStruct((tokens, width), f32),
            jax.ShapeDtypeStruct((tokens, width), f32),
            jax.ShapeDtypeStruct((lines, STATE, width), f32),
            jax.ShapeDtypeStruct((lines, 1, L), f32),
        ],
        scratch_shapes=[
            pltpu.VMEM((LB + 8, width + L), f32),
            pltpu.VMEM((STATE, width), f32),
        ],
        compiler_params=pltpu.CompilerParams(
            dimension_semantics=("arbitrary",), vmem_limit_bytes=VMEM_LIMIT
        ),
        name="mixer_fwd",
    )(lengths, hidden, gain, wgi, wss, cp, sp, hp)


def run_mid(lengths, cot, w_out, gated, cp):
    tokens, full = cot.shape
    width = gated.shape[1]
    lines = tokens // L

    def same(i):
        return i

    return pl.pallas_call(
        mid_kernel,
        grid=(tokens // LB,),
        in_specs=[
            smem_spec(),
            rows_spec(full, same),
            whole_spec(w_out.shape),
            rows_spec(width, same),
            whole_spec(cp.shape),
        ],
        out_specs=[rows_spec(width, same), line_spec(same)],
        out_shape=[
            jax.ShapeDtypeStruct((tokens, width), f32),
            jax.ShapeDtypeStruct((lines, 1, L), f32),
        ],
        compiler_params=pltpu.CompilerParams(
            dimension_semantics=("arbitrary",), vmem_limit_bytes=VMEM_LIMIT
        ),
        name="mixer_mid",
    )(lengths, cot, w_out, gated, cp)


def run_bwd(inner_total, lengths, gate, rest, gs, y, st, gsum, gdot, cp, sp, hp):
    tokens, width = gate.shape
    lines = tokens // L
    blocks = tokens // LB

    def back(i):
        return blocks - 1 - i

    def halo(i):
        return (jnp.maximum(back(i) * (LB // 8) - 1, 0), 0)

    return pl.pallas_call(
        functools.partial(bwd_kernel, float(inner_total)),
        grid=(blocks,),
        in_specs=[
            smem_spec(),
            rows_spec(width, back),
            rows_spec(width + 2 * L, back),
            pl.BlockSpec((8, width + 2 * L), halo),
            rows_spec(width, back),
            rows_spec(width, back),
            pl.BlockSpec((NSUB, STATE, width), lambda i: (back(i), 0, 0)),
            line_spec(back),
            line_spec(back),
            whole_spec(cp.shape),
            whole_spec(sp.shape),
            whole_spec(hp.shape),
        ],
        out_specs=[
            rows_spec(2 * width + L, back),
            rows_spec(L, back),
            line_spec(back),
            line_spec(back),
            pl.BlockSpec((8, width), lambda i: (0, 0)),
            pl.BlockSpec((8, L), lambda i: (0, 0)),
            pl.BlockSpec((8, L), lambda i: (0, 0)),
        ],
        out_shape=[
            jax.ShapeDtypeStruct((tokens, 2 * width + L), bf16),
            jax.ShapeDtypeStruct((tokens, L), f32),
            jax.ShapeDtypeStruct((lines, 1, L), f32),
            jax.ShapeDtypeStruct((lines, 1, L), f32),
            jax.ShapeDtypeStruct((8, width), f32),
            jax.ShapeDtypeStruct((8, L), f32),
            jax.ShapeDtypeStruct((8, L), f32),
        ],
        scratch_shapes=[
            pltpu.VMEM((LB + 8, width + L), f32),
            pltpu.VMEM((8, width + L), f32),
            pltpu.VMEM((STATE, width), f32),
            pltpu.VMEM((STATE, width), f32),
        ],
        compiler_params=pltpu.CompilerParams(
            dimension_semantics=("arbitrary",), vmem_limit_bytes=VMEM_LIMIT
        ),
        name="mixer_bwd",
    )(lengths, gate, rest, rest, gs, y, st, gsum, gdot, cp, sp, hp)


def pack_params(conv_inner, conv_inner_bias, conv_shared, conv_shared_bias, step_bias, log_decay,
                skip_gain, gate_gain):
    width = conv_inner.shape[1]
    heads = step_bias.shape[0]
    skip = jnp.repeat(skip_gain, HEAD)
    cp = jnp.concatenate(
        [conv_inner, conv_inner_bias[None], skip[None], gate_gain[None], jnp.zeros((1, width), f32)],
        axis=0,
    )
    sp = jnp.concatenate([conv_shared, conv_shared_bias[None], jnp.zeros((3, L), f32)], axis=0)
    hp = jnp.zeros((8, L), f32)
    hp = hp.at[0, :heads].set(step_bias).at[1, :heads].set(-jnp.exp(log_decay))
    return cp, sp, hp


def exchange_kernel(axis, x_ref, out_ref, slots, send_sem, recv_sem):
    me = lax.axis_index(axis)
    n = slots.shape[0]
    barrier = pltpu.get_barrier_semaphore()
    for k in range(1, n):
        peer = lax.rem(me + k, n)
        pl.semaphore_signal(barrier, inc=1, device_id={axis: peer})
    pl.semaphore_wait(barrier, n - 1)
    copies = []
    for k in range(1, n):
        peer = lax.rem(me + k, n)
        copy = pltpu.make_async_remote_copy(
            src_ref=x_ref,
            dst_ref=slots.at[k],
            send_sem=send_sem.at[k],
            recv_sem=recv_sem.at[k],
            device_id={axis: peer},
        )
        copy.start()
        copies.append(copy)
    for copy in copies:
        copy.wait()
    slots[0] = x_ref[...]
    total = slots[lax.rem(me, n)]
    for d in range(1, n):
        total = total + slots[lax.rem(me - d + n, n)]
    out_ref[...] = total


def sum_small(x, axis, collective_id):
    n = lax.axis_size(axis)
    return pl.pallas_call(
        functools.partial(exchange_kernel, axis),
        out_shape=jax.ShapeDtypeStruct(x.shape, f32),
        in_specs=[pl.BlockSpec(memory_space=pltpu.VMEM)],
        out_specs=pl.BlockSpec(memory_space=pltpu.VMEM),
        scratch_shapes=[
            pltpu.VMEM((n,) + x.shape, f32),
            pltpu.SemaphoreType.DMA((n,)),
            pltpu.SemaphoreType.DMA((n,)),
        ],
        compiler_params=pltpu.CompilerParams(collective_id=collective_id, has_side_effects=True),
        name="sum_small",
    )(x)


def after(x, *deps):
    deps = [d for d in deps if d is not None]
    return lax.optimization_barrier((x, *deps))[0]


SCALE = 16384.0


def encode(x, bound, kind):
    if bound is not None:
        x = x * (SCALE / bound)
    return x.astype(kind)


def decode(x, bound):
    x = x.astype(f32)
    return x if bound is None else x * (bound / SCALE)


class ScatterLine:

    def __init__(self, send, own):
        self.n = lax.axis_size("heads")
        self.chips = self.n // 2
        self.z = lax.axis_index("heads") >> 1
        self.message, self.own, self.kind = send, own, own.dtype
        self.moving, self.out = [None, None], [None, None]

    def swap(self):
        pairs = [(i, i ^ 1) for i in range(self.n)]
        self.got = lax.ppermute(self.message, "heads", pairs)

    def block(self, b):
        mine = lax.dynamic_index_in_dim(self.own, b, 0, keepdims=False)
        theirs = lax.dynamic_index_in_dim(self.got, b, 0, keepdims=False)
        return mine.astype(f32) + theirs.astype(f32)

    def pack(self, r):
        last = self.chips - 1
        for way in range(2):
            b = last - r + self.z if way == 0 else r - last + self.z
            total = self.block(jnp.clip(b, 0, last))
            if r > 0:
                total = total + self.moving[way].astype(f32)
            self.out[way] = total.astype(self.kind)

    def hold(self, *deps):
        self.moving = [after(m, *deps) for m in self.moving]

    def send(self, r):
        last = self.chips - 1
        out = lax.optimization_barrier(tuple(self.out))
        for way in range(2):
            chips = range(r + 1) if way == 0 else range(last - r, last + 1)
            hop = 2 if way == 0 else -2
            pairs = [(2 * k + c, 2 * k + c + hop) for k in chips for c in range(2)]
            self.moving[way] = lax.ppermute(out[way], "heads", pairs)
        self.moving = list(lax.optimization_barrier(tuple(self.moving)))

    def rest(self, r):
        for k in range(r, self.chips - 1):
            self.pack(k)
            self.send(k)

    def total(self):
        total = self.block(self.z)
        for way in range(2):
            if self.moving[way] is not None:
                total = total + self.moving[way].astype(f32)
        return total


class RowSum:

    def __init__(self, x, bound):
        self.n = lax.axis_size("rows")
        self.me = lax.axis_index("rows")
        self.bits = self.n.bit_length() - 1
        self.bound = bound
        piece = x.shape[0] // (2 * self.n)
        cut = x.reshape((2,) + (2,) * self.bits + (piece, x.shape[1]))
        self.cur = [cut[0], cut[1]]
        self.order = [[(k + part) % self.bits for k in range(self.bits)] for part in range(2)]
        self.left = [list(range(self.bits))[::-1] for _ in range(2)]

    def move(self, x, bit):
        return lax.ppermute(x, "rows", [(i, i ^ (1 << bit)) for i in range(self.n)])

    def reduce(self, k):
        for part in range(2):
            bit, left = self.order[part][k], self.left[part]
            mine = (self.me >> bit) & 1
            axis = left.index(bit)
            left.remove(bit)
            cur = self.cur[part]
            send = lax.dynamic_index_in_dim(cur, 1 - mine, axis, keepdims=False)
            keep = lax.dynamic_index_in_dim(cur, mine, axis, keepdims=False)
            got = self.move(encode(send, self.bound, jnp.float16), bit)
            self.cur[part] = keep + decode(got, self.bound)

    def hold(self, *deps):
        self.cur = [after(cur, *deps) for cur in self.cur]

    def spread(self, *deps):
        pieces = [{0: encode(cur, self.bound, jnp.float16)} for cur in self.cur]
        for k in reversed(range(self.bits)):
            far = []
            for part in range(2):
                bit = self.order[part][k]
                for rel in list(pieces[part]):
                    pieces[part][rel ^ (1 << bit)] = self.move(pieces[part][rel], bit)
                    far.append((part, rel ^ (1 << bit)))
            far_data = [pieces[part][rel] for part, rel in far]
            held = lax.optimization_barrier((*far_data, *deps))
            deps = ()
            for (part, rel), data in zip(far, held):
                pieces[part][rel] = data
        halves = [pieces[part][rel] for part in range(2) for rel in range(self.n)]
        whole = decode(jnp.stack(halves), self.bound)
        return whole.reshape((2, self.n) + whole.shape[1:])


def per_device(
    hidden_in, lengths, norm_gain, in_gate_inner, in_step, in_shared, conv_inner, conv_inner_bias,
    conv_shared, conv_shared_bias, step_bias, log_decay, skip_gain, gate_gain, out_weight, cotangent,
):
    tokens, local = hidden_in.shape
    full = in_gate_inner.shape[0]
    width = in_gate_inner.shape[2]
    heads = step_bias.shape[0]
    chips = full // local // 2
    lines = tokens // L
    inner_total = width * (full // local)
    core = lax.axis_index("heads") & 1
    source_t, cot_t = lax.optimization_barrier((hidden_in.T, cotangent.T))

    hidden_all = lax.all_gather(hidden_in, "heads", axis=1, tiled=True)
    shared_all = lax.all_gather(in_shared, "heads", axis=1, tiled=True)
    gain_all = lax.all_gather(norm_gain, "heads", axis=0, tiled=True)
    cot_all = lax.all_gather(cotangent, "heads", axis=1, tiled=True)
    wgi = in_gate_inner.reshape(full, 2 * width)
    step_pad = jnp.pad(in_step, ((0, 0), (0, L - heads)))
    wss = jnp.concatenate([shared_all.T, step_pad], axis=1)
    w_back = jnp.concatenate([wgi, step_pad], axis=1)

    def halves(w, axis):
        both = []
        for side in (1 - core, core):
            parts = [
                lax.dynamic_slice_in_dim(w, (2 * k + side) * local, local, axis) for k in range(chips)
            ]
            both.append(jnp.stack(parts))
        return both

    back_send, back_own = halves(w_back, 0)
    out_send, out_own = halves(out_weight, 1)
    w_size = jnp.sqrt(jnp.max(jnp.sum(jnp.square(w_back.astype(f32)), axis=1)))
    cp, sp, hp = pack_params(
        conv_inner, conv_inner_bias, conv_shared, conv_shared_bias, step_bias, log_decay,
        skip_gain, gate_gain,
    )

    hidden_all = after(hidden_all, back_send, back_own, out_send, out_own, w_size, cp, sp, hp, source_t, cot_t)
    source_t = source_t.astype(f32)
    normed, inv_rows, gate, rest, gated, y, st, gsum_part = run_fwd(
        lengths, hidden_all, gain_all[None], wgi, wss, cp, sp, hp
    )
    inv_rms = inv_rows.reshape(tokens)
    gsum = sum_small(gsum_part.reshape(lines, L), "heads", 1)

    live = (jnp.arange(tokens, dtype=jnp.int32) < jnp.sum(lengths[0])).astype(bf16)
    gate_rms = lax.rsqrt(gsum.reshape(tokens) / inner_total + EPSILON)
    scaled = (gated * gate_rms[:, None] * gate_gain[None, :]).astype(bf16) * live[:, None]

    def project(w, v, axis):
        return lax.dot_general(w, v, (((axis,), (1,)), ((), ())), preferred_element_type=f32)

    half = jnp.float16
    mixed = ScatterLine(
        project(out_send, scaled, 1).astype(half), project(out_own, scaled, 1).astype(half)
    )
    mixed.swap()
    mixed.pack(0)
    cot_late = after(cot_all, *mixed.out)
    mixed.send(0)
    gs, gdot_part = run_mid(lengths, cot_late, out_weight, gated, cp)
    gdot = sum_small(gdot_part.reshape(lines, L), "heads", 2)
    mixed.hold(gdot)
    mixed.pack(1)
    gdot = after(gdot, *mixed.out)
    mixed.send(1)

    low, gsh_part, nd_part, size, pg, sg, hg = run_bwd(
        inner_total, lengths, gate, rest, gs, y, st, gsum.reshape(lines, 1, L),
        gdot.reshape(lines, 1, L), cp, sp, hp,
    )
    bound = jnp.sqrt(size.reshape(lines, L)) * (1.01 * w_size) + 1e-30
    mixed.hold(low)
    mixed.pack(2)
    nd_part = after(nd_part, *mixed.out)
    mixed.send(2)
    small = sum_small(
        jnp.concatenate([nd_part.reshape(lines, L), bound, sg], axis=0), "heads", 3
    )
    norm_dot, sg = small[:lines].reshape(tokens), small[2 * lines :]
    bound = small[lines : 2 * lines].reshape(tokens)
    low = after(low, bound)

    normal = ScatterLine(
        encode(project(back_send, low, 2), bound, half),
        encode(project(back_own, low, 2), bound, half),
    )
    normal.swap()
    normal.pack(0)
    low_late = after(low, *normal.out)
    scaled_late = after(scaled, *normal.out)
    gsh_part = after(gsh_part, *normal.out)
    mixed.hold(*normal.out)
    normal.send(0)

    cut = gsh_part.T.reshape(chips, 2, L // (2 * chips), tokens)
    gsh_own = lax.dynamic_index_in_dim(cut, core, 1, keepdims=False)
    gsh_send = lax.dynamic_index_in_dim(cut, 1 - core, 1, keepdims=False)
    shared = ScatterLine(gsh_send, gsh_own)
    shared.swap()
    grad_wout = lax.dot_general(
        scaled_late, cot_all, (((0,), (0,)), ((), ())), preferred_element_type=f32
    )
    top_wout = jnp.max(jnp.abs(grad_wout))
    shared.pack(0)
    low_late = after(low_late, *shared.out)
    shared.send(0)
    grad_proj = lax.dot_general(
        normed, low_late, (((0,), (0,)), ((), ())), preferred_element_type=f32
    )
    top_proj = jnp.max(jnp.abs(grad_proj))
    shared.hold(top_proj)
    shared.pack(1)
    top_proj = after(top_proj, *shared.out)
    shared.send(1)
    tops = jnp.stack([top_proj, top_wout])
    tops = jnp.broadcast_to(jnp.repeat(tops * 1.01 + 1e-30, 8)[:, None], (16, L))
    wide = pg.reshape(8 * width // L, L)
    small = sum_small(jnp.concatenate([tops, sg, hg, wide], axis=0), "rows", 4)

    normal.hold(small)
    normal.pack(1)
    small = after(small, *normal.out)
    shared.hold(*normal.out)
    mixed.hold(*normal.out)
    normal.send(1)
    top_proj, top_wout, sg, hg = small[0, 0], small[8, 0], small[16:24], small[24:32]
    pg = small[32:].reshape(8, width)
    sum_proj, sum_wout = RowSum(grad_proj, top_proj), RowSum(grad_wout, top_wout)
    for k in range(sum_proj.bits):
        sum_proj.reduce(k)
        sum_wout.reduce(k)
    shared.rest(2)
    low_shared = lax.all_gather(shared.total().astype(bf16), "heads", axis=0, tiled=True)
    mixed.rest(3)
    output_t = (source_t + mixed.total()).astype(bf16)

    normal.pack(2)
    out = normal.out
    normal.send(2)
    grad_proj, grad_step = place(
        sum_proj.spread(*out), unpack_kernel, [(full, 2, width), (full, heads)]
    )
    (grad_wout,) = place(sum_wout.spread(*out), place_kernel, [grad_wout.shape])

    low_shared = after(low_shared, *out)
    shared_raw = rest[:, width : width + L]
    norm_dot = norm_dot + jnp.sum(low_shared.astype(f32) * shared_raw.T, axis=0)
    normed_t = (source_t * inv_rms[None, :] * norm_gain[:, None]).astype(bf16)
    grad_shared_w = lax.dot_general(
        low_shared, normed_t, (((1,), (1,)), ((), ())), preferred_element_type=f32
    )
    grad_shared_w = sum_small(grad_shared_w.reshape(local, L), "rows", 6).reshape(L, local)
    more = lax.dot_general(
        in_shared, low_shared, (((0,), (0,)), ((), ())), preferred_element_type=f32
    )

    normal.rest(3)
    grad_normed = normal.total() * (bound / SCALE)[None, :] + more
    grad_gain_norm = jnp.sum(grad_normed * source_t * inv_rms[None, :], axis=1)
    grad_source = (
        inv_rms[None, :] * norm_gain[:, None] * grad_normed
        - source_t * (inv_rms * inv_rms * norm_dot / full)[None, :]
    )
    grad_input = (cot_t.astype(f32) + grad_source).T
    output = output_t.T
    grad_gain_norm = sum_small(grad_gain_norm.reshape(local // L, L), "rows", 5).reshape(local)
    return (
        output,
        grad_input,
        grad_gain_norm,
        grad_proj,
        grad_step,
        grad_shared_w,
        pg[0:4],
        pg[4],
        sg[0:4],
        sg[4],
        hg[0, :heads],
        hg[1, :heads],
        pg[5].reshape(heads, HEAD).sum(axis=1),
        pg[6],
        grad_wout,
    )


def solution(mesh):
    return jax.shard_map(
        per_device,
        mesh=mesh,
        in_specs=(
            P("rows", "heads"), P("rows", None), P("heads"), P(None, None, "heads"),
            P(None, "heads"), P(None, "heads"), P(None, "heads"), P("heads"), P(), P(),
            P("heads"), P("heads"), P("heads"), P("heads"), P("heads", None), P("rows", "heads"),
        ),
        out_specs=(
            P("rows", "heads"), P("rows", "heads"), P("heads"), P(None, None, "heads"),
            P(None, "heads"), P(None, "heads"), P(None, "heads"), P("heads"), P(), P(),
            P("heads"), P("heads"), P("heads"), P("heads"), P("heads", None),
        ),
        check_vma=False,
    )
```

```python
import functools

import jax
import jax.numpy as jnp
from jax import lax
from jax.experimental import pallas as pl
from jax.experimental.pallas import tpu as pltpu
from jax.sharding import PartitionSpec as P


EPSILON = 1e-05
L = 128
LB = 512
NSUB = LB // L
HEAD = 64
STATE = 64
f32 = jnp.float32
bf16 = jnp.bfloat16


def mm(a, b, ca=1, cb=0):
    return lax.dot_general(a, b, (((ca,), (cb,)), ((), ())), preferred_element_type=f32)


def split(x):
    hi = x.astype(bf16)
    return hi, (x - hi.astype(f32)).astype(bf16)


def mm3(a, b, ca=1, cb=0):
    ah, al = split(a)
    bh, bl = split(b)
    return mm(ah, bh, ca, cb) + mm(ah, bl, ca, cb) + mm(al, bh, ca, cb)


def mm_exact_left(mask, x):
    hi = x.astype(bf16)
    rest = x - hi.astype(f32)
    mid = rest.astype(bf16)
    low = (rest - mid.astype(f32)).astype(bf16)
    return mm(mask, hi) + mm(mask, mid) + mm(mask, low)


def block_diag(x, first):
    zero = jnp.zeros_like(x)
    return jnp.concatenate([jnp.where(first, x, zero), jnp.where(first, zero, x)], axis=0)


def bounds_of(len_ref):
    b0 = len_ref[0, 0]
    b1 = b0 + len_ref[0, 1]
    b2 = b1 + len_ref[0, 2]
    b3 = b2 + len_ref[0, 3]
    return b0, b1, b2, b3


def start_of(bounds, t):
    start = jnp.zeros_like(t)
    for b in bounds:
        start = jnp.where(t >= b, b, start)
    return start


def to_row(col):
    return jnp.transpose(jnp.broadcast_to(col, (L, L)))[0:1, :]


def to_col(row):
    return jnp.transpose(jnp.broadcast_to(row, (L, L)))


def pair_cols(a, q, first):
    return jnp.where(first, a[:, 2 * q : 2 * q + 1], a[:, 2 * q + 1 : 2 * q + 2])


def sigmoid(v):
    return 0.5 + 0.5 * jnp.tanh(0.5 * v)


def softplus(v):
    return jnp.maximum(v, 0.0) + jnp.log1p(jnp.exp(-jnp.abs(v)))


def shifted(win, m):
    if m == 0:
        return win[8:, :]
    return pltpu.roll(win, m, 0)[8:, :]


def chunk_columns(hp_ref, step, bounds, base):
    tcol = lax.broadcasted_iota(jnp.int32, (L, L), 0) + base
    trow = lax.broadcasted_iota(jnp.int32, (L, L), 1) + base
    start_col = start_of(bounds, tcol)
    start_end = start_of(bounds, base + (L - 1))
    raw = step + hp_ref[0:1, :]
    dt = softplus(raw)
    decay = hp_ref[1:2, :] * dt
    lower = jnp.where(trow <= tcol, 1.0, 0.0).astype(bf16)
    cum = mm_exact_left(lower, decay)
    cum_end = cum[L - 1 : L, :]
    ecum = jnp.where(start_col < base, jnp.exp(cum), 0.0)
    wend = jnp.where(tcol >= start_end, jnp.exp(cum_end - cum), 0.0)
    carried_end = (start_end < base).astype(f32)
    cdec = jnp.exp(cum_end) * carried_end
    return tcol, trow, start_col, start_end, raw, dt, decay, cum, ecum, wend, cdec


def fwd_kernel(
    len_ref, h_ref, gain_ref, wgi_ref, wss_ref, cp_ref, sp_ref, hp_ref,
    normed_ref, inv_ref, gate_ref, rest_ref, gated_ref, y_ref, st_ref, gsum_ref,
    vbuf, state,
):
    blk = pl.program_id(0)
    width = gate_ref.shape[1]
    full = h_ref.shape[1]
    pairs = width // L

    @pl.when(blk == 0)
    def _():
        vbuf[0:8, :] = jnp.zeros((8, vbuf.shape[1]), f32)
        state[...] = jnp.zeros(state.shape, f32)

    piece = 256

    def norm_rows(s, carry):
        rows = pl.ds(pl.multiple_of(s * L, L), L)
        acc = jnp.zeros((L, piece), f32)
        for k in range(full // piece):
            x = h_ref[rows, k * piece : (k + 1) * piece].astype(f32)
            acc = acc + x * x
        inv = lax.rsqrt(jnp.sum(acc, axis=1, keepdims=True) / full + EPSILON)
        for k in range(full // piece):
            cols = slice(k * piece, (k + 1) * piece)
            x = h_ref[rows, cols].astype(f32)
            normed_ref[rows, cols] = (x * inv * gain_ref[0:1, cols]).astype(bf16)
        inv_ref[s] = to_row(inv)
        return carry

    lax.fori_loop(0, NSUB, norm_rows, 0)
    normed = normed_ref[...]
    gate_ref[...] = mm(normed, wgi_ref[:, :width])
    inner = mm(normed, wgi_ref[:, width:])
    vbuf[8:, :width] = inner
    rest_ref[:, :width] = inner
    tail = mm(normed, wss_ref[...])
    vbuf[8:, width:] = tail[:, :L]
    rest_ref[:, width:] = tail

    bounds = bounds_of(len_ref)
    first = lax.broadcasted_iota(jnp.int32, (L, L), 1) < HEAD

    def chunk(s, carry):
        r0 = pl.multiple_of(s * L, L)
        rows = pl.ds(r0, L)
        base = blk * LB + s * L
        step = rest_ref[rows, width + L :]
        tcol, trow, start_col, _, _, dt, _, cum, ecum, wend, cdec = chunk_columns(
            hp_ref, step, bounds, base
        )
        cum_t = jnp.transpose(cum)
        mask = (trow <= tcol) & (trow >= start_col)
        valid = [tcol - m >= start_col for m in range(4)]

        def conv(cols, taps):
            win = vbuf[pl.ds(r0, L + 8), cols]
            pre = taps[4:5, :] + taps[3:4, :] * win[8:, :]
            for m in range(1, 4):
                pre = pre + taps[3 - m : 4 - m, :] * jnp.where(valid[m], shifted(win, m), 0.0)
            return pre

        pre_s = conv(slice(width, width + L), sp_ref)
        act = pre_s * sigmoid(pre_s)
        b_map = act[:, :STATE]
        c_map = act[:, STATE:]
        scores = jnp.where(mask, mm3(c_map, b_map, 1, 1), 0.0)
        square = jnp.zeros((L, L), f32)
        for q in range(pairs):
            cols = slice(q * L, (q + 1) * L)
            pre = conv(cols, cp_ref.at[:, cols])
            xin = pre * sigmoid(pre)
            xp = xin * pair_cols(dt, q, first)
            xh, xl = split(xp)
            bdh, bdl = block_diag(xh, first), block_diag(xl, first)
            mix = []
            for h in (2 * q, 2 * q + 1):
                spread = jnp.minimum(cum[:, h : h + 1] - cum_t[h : h + 1, :], 0.0)
                mix.append(jnp.exp(spread) * scores)
            mh, ml = split(jnp.concatenate(mix, axis=1))
            both = mm(mh, jnp.concatenate([bdh, bdl], axis=1))
            y = both[:, :L] + both[:, L:] + mm(ml, bdh)
            st = state[:, cols]
            st_ref[s, :, cols] = st
            y = y + mm3(c_map, st) * pair_cols(ecum, q, first)
            xw = xp * pair_cols(wend, q, first)
            state[:, cols] = mm3(b_map, xw, 0, 0) + st * pair_cols(cdec, q, first[0:1, :])
            y_ref[rows, cols] = y
            gate = gate_ref[rows, cols]
            gated = (y + cp_ref[5:6, cols] * xin) * (gate * sigmoid(gate))
            gated_ref[rows, cols] = gated
            square = square + gated * gated
        gsum_ref[s] = to_row(jnp.sum(square, axis=1, keepdims=True))
        return carry

    lax.fori_loop(0, NSUB, chunk, 0)
    vbuf[0:8, :] = vbuf[LB : LB + 8, :]


def mid_kernel(len_ref, cot_ref, w_ref, gated_ref, cp_ref, gs_ref, gdot_ref):
    blk = pl.program_id(0)
    live = bounds_of(len_ref)[3]
    t = lax.broadcasted_iota(jnp.int32, gs_ref.shape, 0) + blk * LB
    gs = jnp.where(t < live, mm(cot_ref[...], w_ref[...], 1, 1), 0.0)
    gs_ref[...] = gs
    dots = jnp.sum(gs * cp_ref[6:7, :] * gated_ref[...], axis=1, keepdims=True)
    for s in range(NSUB):
        gdot_ref[s] = to_row(dots[s * L : (s + 1) * L, :])


def bwd_kernel(
    inner_total,
    len_ref, gate_ref, rest_ref, halo_ref, gs_ref, y_ref, st_ref, gsum_ref, gdot_ref,
    cp_ref, sp_ref, hp_ref,
    low_ref, gsh_ref, nd_ref, size_ref, pg_ref, sg_ref, hg_ref,
    vbuf, qnext, adj, send,
):
    step_id = pl.program_id(0)
    blk = pl.num_programs(0) - 1 - step_id
    width = gate_ref.shape[1]
    pairs = width // L

    @pl.when(step_id == 0)
    def _():
        qnext[...] = jnp.zeros(qnext.shape, f32)
        adj[...] = jnp.zeros(adj.shape, f32)
        send[...] = jnp.zeros(send.shape, f32)
        pg_ref[...] = jnp.zeros(pg_ref.shape, f32)
        sg_ref[...] = jnp.zeros(sg_ref.shape, f32)
        hg_ref[...] = jnp.zeros(hg_ref.shape, f32)

    vbuf[0:8, :] = halo_ref[:, : width + L]
    vbuf[8:, :] = rest_ref[:, : width + L]
    bounds = bounds_of(len_ref)
    first = lax.broadcasted_iota(jnp.int32, (L, L), 1) < HEAD
    lane = lax.broadcasted_iota(jnp.int32, (L, L), 1)
    half = lax.broadcasted_iota(jnp.int32, (L, L), 0) // HEAD

    def chunk(i, carry):
        s = NSUB - 1 - i
        r0 = pl.multiple_of(s * L, L)
        rows = pl.ds(r0, L)
        base = blk * LB + s * L
        step = rest_ref[rows, width + L :]
        tcol, trow, start_col, start_end, raw, dt, decay, cum, ecum, wend, cdec = chunk_columns(
            hp_ref, step, bounds, base
        )
        cum_t = jnp.transpose(cum)
        mask_t = (trow >= tcol) & (start_of(bounds, trow) <= tcol)
        valid = [tcol - m >= start_col for m in range(4)]
        valid_up = [start_of(bounds, tcol + m) <= tcol for m in range(4)]
        gate_rms_row = lax.rsqrt(gsum_ref[s] / inner_total + EPSILON)
        pull_row = gate_rms_row * gate_rms_row * gate_rms_row * gdot_ref[s] / inner_total
        gate_rms = to_col(gate_rms_row)
        pull = to_col(pull_row)

        def conv(cols, taps):
            win = vbuf[pl.ds(r0, L + 8), cols]
            seen = [win[8:, :]]
            pre = taps[4:5, :] + taps[3:4, :] * seen[0]
            for m in range(1, 4):
                seen.append(jnp.where(valid[m], shifted(win, m), 0.0))
                pre = pre + taps[3 - m : 4 - m, :] * seen[m]
            return seen, pre

        def conv_back(q, seen, cols, taps, grad_ref, grad_cols):
            win = jnp.concatenate([q, qnext[:, cols]], axis=0)
            qnext[:, cols] = q[0:8, :]
            grad = taps[3:4, :] * q
            for m in range(1, 4):
                up = pltpu.roll(win, L + 8 - m, 0)[:L, :]
                grad = grad + taps[3 - m : 4 - m, :] * jnp.where(valid_up[m], up, 0.0)
            for m in range(4):
                k = 3 - m
                grad_ref[k : k + 1, grad_cols] += jnp.sum(q * seen[m], axis=0, keepdims=True)
            grad_ref[4:5, grad_cols] += jnp.sum(q, axis=0, keepdims=True)
            return grad

        seen_s, pre_s = conv(slice(width, width + L), sp_ref)
        sig_s = sigmoid(pre_s)
        act = pre_s * sig_s
        b_map = act[:, :STATE]
        c_map = act[:, STATE:]
        scores_t = jnp.where(mask_t, mm3(b_map, c_map, 1, 1), 0.0)
        d_scores = jnp.zeros((L, L), f32)
        d_b = jnp.zeros((L, STATE), f32)
        d_c = jnp.zeros((L, STATE), f32)
        reduced = jnp.zeros((2 * L, L), f32)
        ends = jnp.zeros((8, L), f32)
        norm_dot = jnp.zeros((L, L), f32)
        size = jnp.zeros((L, L), f32)
        for q in range(pairs):
            cols = slice(q * L, (q + 1) * L)
            taps = cp_ref.at[:, cols]
            skip = cp_ref[5:6, cols]
            seen, pre = conv(cols, taps)
            sig = sigmoid(pre)
            xin = pre * sig
            dtx = pair_cols(dt, q, first)
            xp = xin * dtx
            y = y_ref[rows, cols]
            ho = y + skip * xin
            gate = gate_ref[rows, cols]
            gsig = sigmoid(gate)
            sl = gate * gsig
            gated = ho * sl
            gs = gs_ref[rows, cols]
            pg_ref[6:7, cols] += jnp.sum(gs * gated * gate_rms, axis=0, keepdims=True)
            gg = gate_rms * cp_ref[6:7, cols] * gs - gated * pull
            gy = gg * sl
            low_gate = (gg * ho * (gsig * (1.0 + gate * (1.0 - gsig)))).astype(bf16)
            low_ref[rows, cols] = low_gate
            pg_ref[5:6, cols] += jnp.sum(gy * xin, axis=0, keepdims=True)

            yh, yl = split(gy)
            bdh, bdl = block_diag(yh, first), block_diag(yl, first)
            xh, xl = split(xp)
            d_mix = mm(
                jnp.concatenate([xh, xl], axis=1), jnp.concatenate([bdh, bdh], axis=1), 1, 1
            ) + mm(xh, bdl, 1, 1)
            mix = []
            for k in range(2):
                h = 2 * q + k
                spread = jnp.minimum(cum_t[h : h + 1, :] - cum[:, h : h + 1], 0.0)
                factor = jnp.exp(spread)
                d_scores = d_scores + d_mix[:, k * L : (k + 1) * L] * factor
                mix.append(factor * scores_t)
            mh, ml = split(jnp.concatenate(mix, axis=1))
            both = mm(mh, jnp.concatenate([bdh, bdl], axis=1))
            dxp = both[:, :L] + both[:, L:] + mm(ml, bdh)
            wendx = pair_cols(wend, q, first)
            a_in = adj[:, cols]
            dxp = dxp + mm3(b_map, a_in) * wendx
            xw = xp * wendx
            gyw = gy * pair_cols(ecum, q, first)
            s_in = st_ref[s, :, cols]
            d_b = d_b + mm3(xw, a_in, 1, 1)
            d_c = d_c + mm3(gyw, s_in, 1, 1)
            adj[:, cols] = mm3(c_map, gyw, 0, 0) + a_in * pair_cols(cdec, q, first[0:1, :])
            heads = jnp.where(lane == 2 * q + half, 1.0, 0.0).astype(bf16)
            zh, zl = split(jnp.concatenate([gy * y - dxp * xp, dxp * xin], axis=0))
            reduced = reduced + mm(zh, heads) + mm(zl, heads)
            end = jnp.broadcast_to(
                jnp.sum(a_in * send[:, cols], axis=0, keepdims=True), (8, L)
            )
            eh, el = split(end)
            ends = ends + mm(eh, heads) + mm(el, heads)
            send[:, cols] = s_in

            dxin = dxp * dtx + skip * gy
            qv = dxin * (sig * (1.0 + pre * (1.0 - sig)))
            grad = conv_back(qv, seen, cols, taps, pg_ref, cols)
            low_inner = grad.astype(bf16)
            low_ref[rows, width + q * L : width + (q + 1) * L] = low_inner
            wide_gate, wide_inner = low_gate.astype(f32), low_inner.astype(f32)
            norm_dot = norm_dot + wide_gate * gate + wide_inner * seen[0]
            size = size + wide_gate * wide_gate + wide_inner * wide_inner

        d_scores = jnp.where(mask_t, d_scores, 0.0)
        d_b = d_b + mm3(d_scores, c_map)
        d_c = d_c + mm3(d_scores, b_map, 0, 0)
        d_act = jnp.concatenate([d_b, d_c], axis=1)
        q_s = d_act * (sig_s * (1.0 + pre_s * (1.0 - sig_s)))
        shared_cols = slice(width, width + L)
        gsh_ref[rows, :] = conv_back(q_s, seen_s, shared_cols, sp_ref, sg_ref, slice(0, L))

        tail = jnp.where(tcol >= start_end, ends[0:1, :], 0.0)
        keep = jnp.where(mask_t, 1.0, 0.0).astype(bf16)
        d_decay = mm_exact_left(keep, reduced[:L, :]) + tail
        d_dt = reduced[L:, :] + d_decay * hp_ref[1:2, :]
        d_raw = d_dt * sigmoid(raw)
        hg_ref[0:1, :] += jnp.sum(d_raw, axis=0, keepdims=True)
        hg_ref[1:2, :] += jnp.sum(d_decay * decay, axis=0, keepdims=True)
        low_step = d_raw.astype(bf16)
        low_ref[rows, 2 * width :] = low_step
        wide_step = low_step.astype(f32)
        norm_dot = norm_dot + wide_step * step
        size = size + wide_step * wide_step
        nd_ref[s] = to_row(jnp.sum(norm_dot, axis=1, keepdims=True))
        size_ref[s] = to_row(jnp.sum(size, axis=1, keepdims=True))
        return carry

    lax.fori_loop(0, NSUB, chunk, 0)


def unpack_kernel(me_ref, x_ref, gate_inner_ref, step_ref):
    width = gate_inner_ref.shape[2]
    gate_inner_ref[:, 0, :] = x_ref[0, 0, :, :width]
    gate_inner_ref[:, 1, :] = x_ref[0, 0, :, width : 2 * width]
    step_ref[...] = x_ref[0, 0, :, 2 * width : 2 * width + step_ref.shape[1]]


def place_kernel(me_ref, x_ref, out_ref):
    out_ref[...] = x_ref[0, 0]


def place(x, kernel, shapes):
    _, n, piece, cols = x.shape

    def spec(shape):
        zeros = (0,) * (len(shape) - 1)
        return pl.BlockSpec((piece,) + shape[1:], lambda p, k, me: (p * n + (me[0] ^ k),) + zeros)

    return pl.pallas_call(
        kernel,
        grid_spec=pltpu.PrefetchScalarGridSpec(
            num_scalar_prefetch=1,
            grid=(2, n),
            in_specs=[pl.BlockSpec((1, 1, piece, cols), lambda p, k, me: (p, k, 0, 0))],
            out_specs=[spec(shape) for shape in shapes],
        ),
        out_shape=[jax.ShapeDtypeStruct(shape, f32) for shape in shapes],
        name="place",
    )(lax.axis_index("rows").astype(jnp.int32)[None], x)


def rows_spec(cols, order):
    return pl.BlockSpec((LB, cols), lambda i: (order(i), 0))


def line_spec(order):
    return pl.BlockSpec((NSUB, 1, L), lambda i: (order(i), 0, 0))


def whole_spec(shape):
    return pl.BlockSpec(shape, lambda i: (0,) * len(shape), pipeline_mode=pl.Buffered(1))


def smem_spec():
    return pl.BlockSpec(memory_space=pltpu.SMEM)


VMEM_LIMIT = 60 * 1024 * 1024


def run_fwd(lengths, hidden, gain, wgi, wss, cp, sp, hp):
    tokens, full = hidden.shape
    width = wgi.shape[1] // 2
    lines = tokens // L

    def same(i):
        return i

    return pl.pallas_call(
        fwd_kernel,
        grid=(tokens // LB,),
        in_specs=[
            smem_spec(),
            rows_spec(full, same),
            whole_spec(gain.shape),
            whole_spec(wgi.shape),
            whole_spec(wss.shape),
            whole_spec(cp.shape),
            whole_spec(sp.shape),
            whole_spec(hp.shape),
        ],
        out_specs=[
            rows_spec(full, same),
            line_spec(same),
            rows_spec(width, same),
            rows_spec(width + 2 * L, same),
            rows_spec(width, same),
            rows_spec(width, same),
            pl.BlockSpec((NSUB, STATE, width), lambda i: (i, 0, 0)),
            line_spec(same),
        ],
        out_shape=[
            jax.ShapeDtypeStruct((tokens, full), bf16),
            jax.ShapeDtypeStruct((lines, 1, L), f32),
            jax.ShapeDtypeStruct((tokens, width), f32),
            jax.ShapeDtypeStruct((tokens, width + 2 * L), f32),
            jax.ShapeDtypeStruct((tokens, width), f32),
            jax.ShapeDtypeStruct((tokens, width), f32),
            jax.ShapeDtypeStruct((lines, STATE, width), f32),
            jax.ShapeDtypeStruct((lines, 1, L), f32),
        ],
        scratch_shapes=[
            pltpu.VMEM((LB + 8, width + L), f32),
            pltpu.VMEM((STATE, width), f32),
        ],
        compiler_params=pltpu.CompilerParams(
            dimension_semantics=("arbitrary",), vmem_limit_bytes=VMEM_LIMIT
        ),
        name="mixer_fwd",
    )(lengths, hidden, gain, wgi, wss, cp, sp, hp)


def run_mid(lengths, cot, w_out, gated, cp):
    tokens, full = cot.shape
    width = gated.shape[1]
    lines = tokens // L

    def same(i):
        return i

    return pl.pallas_call(
        mid_kernel,
        grid=(tokens // LB,),
        in_specs=[
            smem_spec(),
            rows_spec(full, same),
            whole_spec(w_out.shape),
            rows_spec(width, same),
            whole_spec(cp.shape),
        ],
        out_specs=[rows_spec(width, same), line_spec(same)],
        out_shape=[
            jax.ShapeDtypeStruct((tokens, width), f32),
            jax.ShapeDtypeStruct((lines, 1, L), f32),
        ],
        compiler_params=pltpu.CompilerParams(
            dimension_semantics=("arbitrary",), vmem_limit_bytes=VMEM_LIMIT
        ),
        name="mixer_mid",
    )(lengths, cot, w_out, gated, cp)


def run_bwd(inner_total, lengths, gate, rest, gs, y, st, gsum, gdot, cp, sp, hp):
    tokens, width = gate.shape
    lines = tokens // L
    blocks = tokens // LB

    def back(i):
        return blocks - 1 - i

    def halo(i):
        return (jnp.maximum(back(i) * (LB // 8) - 1, 0), 0)

    return pl.pallas_call(
        functools.partial(bwd_kernel, float(inner_total)),
        grid=(blocks,),
        in_specs=[
            smem_spec(),
            rows_spec(width, back),
            rows_spec(width + 2 * L, back),
            pl.BlockSpec((8, width + 2 * L), halo),
            rows_spec(width, back),
            rows_spec(width, back),
            pl.BlockSpec((NSUB, STATE, width), lambda i: (back(i), 0, 0)),
            line_spec(back),
            line_spec(back),
            whole_spec(cp.shape),
            whole_spec(sp.shape),
            whole_spec(hp.shape),
        ],
        out_specs=[
            rows_spec(2 * width + L, back),
            rows_spec(L, back),
            line_spec(back),
            line_spec(back),
            pl.BlockSpec((8, width), lambda i: (0, 0)),
            pl.BlockSpec((8, L), lambda i: (0, 0)),
            pl.BlockSpec((8, L), lambda i: (0, 0)),
        ],
        out_shape=[
            jax.ShapeDtypeStruct((tokens, 2 * width + L), bf16),
            jax.ShapeDtypeStruct((tokens, L), f32),
            jax.ShapeDtypeStruct((lines, 1, L), f32),
            jax.ShapeDtypeStruct((lines, 1, L), f32),
            jax.ShapeDtypeStruct((8, width), f32),
            jax.ShapeDtypeStruct((8, L), f32),
            jax.ShapeDtypeStruct((8, L), f32),
        ],
        scratch_shapes=[
            pltpu.VMEM((LB + 8, width + L), f32),
            pltpu.VMEM((8, width + L), f32),
            pltpu.VMEM((STATE, width), f32),
            pltpu.VMEM((STATE, width), f32),
        ],
        compiler_params=pltpu.CompilerParams(
            dimension_semantics=("arbitrary",), vmem_limit_bytes=VMEM_LIMIT
        ),
        name="mixer_bwd",
    )(lengths, gate, rest, rest, gs, y, st, gsum, gdot, cp, sp, hp)


def pack_params(conv_inner, conv_inner_bias, conv_shared, conv_shared_bias, step_bias, log_decay,
                skip_gain, gate_gain):
    width = conv_inner.shape[1]
    heads = step_bias.shape[0]
    skip = jnp.repeat(skip_gain, HEAD)
    cp = jnp.concatenate(
        [conv_inner, conv_inner_bias[None], skip[None], gate_gain[None], jnp.zeros((1, width), f32)],
        axis=0,
    )
    sp = jnp.concatenate([conv_shared, conv_shared_bias[None], jnp.zeros((3, L), f32)], axis=0)
    hp = jnp.zeros((8, L), f32)
    hp = hp.at[0, :heads].set(step_bias).at[1, :heads].set(-jnp.exp(log_decay))
    return cp, sp, hp


def exchange_kernel(axis, x_ref, out_ref, slots, send_sem, recv_sem):
    me = lax.axis_index(axis)
    n = slots.shape[0]
    barrier = pltpu.get_barrier_semaphore()
    for k in range(1, n):
        peer = lax.rem(me + k, n)
        pl.semaphore_signal(barrier, inc=1, device_id={axis: peer})
    pl.semaphore_wait(barrier, n - 1)
    copies = []
    for k in range(1, n):
        peer = lax.rem(me + k, n)
        copy = pltpu.make_async_remote_copy(
            src_ref=x_ref,
            dst_ref=slots.at[k],
            send_sem=send_sem.at[k],
            recv_sem=recv_sem.at[k],
            device_id={axis: peer},
        )
        copy.start()
        copies.append(copy)
    for copy in copies:
        copy.wait()
    slots[0] = x_ref[...]
    total = slots[lax.rem(me, n)]
    for d in range(1, n):
        total = total + slots[lax.rem(me - d + n, n)]
    out_ref[...] = total


def sum_small(x, axis, collective_id):
    n = lax.axis_size(axis)
    return pl.pallas_call(
        functools.partial(exchange_kernel, axis),
        out_shape=jax.ShapeDtypeStruct(x.shape, f32),
        in_specs=[pl.BlockSpec(memory_space=pltpu.VMEM)],
        out_specs=pl.BlockSpec(memory_space=pltpu.VMEM),
        scratch_shapes=[
            pltpu.VMEM((n,) + x.shape, f32),
            pltpu.SemaphoreType.DMA((n,)),
            pltpu.SemaphoreType.DMA((n,)),
        ],
        compiler_params=pltpu.CompilerParams(collective_id=collective_id, has_side_effects=True),
        name="sum_small",
    )(x)


def after(x, *deps):
    deps = [d for d in deps if d is not None]
    return lax.optimization_barrier((x, *deps))[0]


SCALE = 16384.0


def encode(x, bound, kind):
    if bound is not None:
        x = x * (SCALE / bound)
    return x.astype(kind)


def decode(x, bound):
    x = x.astype(f32)
    return x if bound is None else x * (bound / SCALE)


class ScatterLine:

    def __init__(self, send, own):
        self.n = lax.axis_size("heads")
        self.chips = self.n // 2
        self.z = lax.axis_index("heads") >> 1
        self.message, self.own, self.kind = send, own, own.dtype
        self.moving, self.out = [None, None], [None, None]

    def swap(self):
        pairs = [(i, i ^ 1) for i in range(self.n)]
        self.got = lax.ppermute(self.message, "heads", pairs)

    def block(self, b):
        mine = lax.dynamic_index_in_dim(self.own, b, 0, keepdims=False)
        theirs = lax.dynamic_index_in_dim(self.got, b, 0, keepdims=False)
        return mine.astype(f32) + theirs.astype(f32)

    def pack(self, r):
        last = self.chips - 1
        for way in range(2):
            b = last - r + self.z if way == 0 else r - last + self.z
            total = self.block(jnp.clip(b, 0, last))
            if r > 0:
                total = total + self.moving[way].astype(f32)
            self.out[way] = total.astype(self.kind)

    def hold(self, *deps):
        self.moving = [after(m, *deps) for m in self.moving]

    def send(self, r):
        last = self.chips - 1
        out = lax.optimization_barrier(tuple(self.out))
        for way in range(2):
            chips = range(r + 1) if way == 0 else range(last - r, last + 1)
            hop = 2 if way == 0 else -2
            pairs = [(2 * k + c, 2 * k + c + hop) for k in chips for c in range(2)]
            self.moving[way] = lax.ppermute(out[way], "heads", pairs)
        self.moving = list(lax.optimization_barrier(tuple(self.moving)))

    def rest(self, r):
        for k in range(r, self.chips - 1):
            self.pack(k)
            self.send(k)

    def total(self):
        total = self.block(self.z)
        for way in range(2):
            if self.moving[way] is not None:
                total = total + self.moving[way].astype(f32)
        return total


class RowSum:

    def __init__(self, x, bound):
        self.n = lax.axis_size("rows")
        self.me = lax.axis_index("rows")
        self.bits = self.n.bit_length() - 1
        self.bound = bound
        piece = x.shape[0] // (2 * self.n)
        cut = x.reshape((2,) + (2,) * self.bits + (piece, x.shape[1]))
        self.cur = [cut[0], cut[1]]
        self.order = [[(k + part) % self.bits for k in range(self.bits)] for part in range(2)]
        self.left = [list(range(self.bits))[::-1] for _ in range(2)]

    def move(self, x, bit):
        return lax.ppermute(x, "rows", [(i, i ^ (1 << bit)) for i in range(self.n)])

    def reduce(self, k):
        for part in range(2):
            bit, left = self.order[part][k], self.left[part]
            mine = (self.me >> bit) & 1
            axis = left.index(bit)
            left.remove(bit)
            cur = self.cur[part]
            send = lax.dynamic_index_in_dim(cur, 1 - mine, axis, keepdims=False)
            keep = lax.dynamic_index_in_dim(cur, mine, axis, keepdims=False)
            got = self.move(encode(send, self.bound, jnp.float16), bit)
            self.cur[part] = keep + decode(got, self.bound)

    def hold(self, *deps):
        self.cur = [after(cur, *deps) for cur in self.cur]

    def spread(self, *deps):
        pieces = [{0: encode(cur, self.bound, jnp.float16)} for cur in self.cur]
        for k in reversed(range(self.bits)):
            far = []
            for part in range(2):
                bit = self.order[part][k]
                for rel in list(pieces[part]):
                    pieces[part][rel ^ (1 << bit)] = self.move(pieces[part][rel], bit)
                    far.append((part, rel ^ (1 << bit)))
            far_data = [pieces[part][rel] for part, rel in far]
            held = lax.optimization_barrier((*far_data, *deps))
            deps = ()
            for (part, rel), data in zip(far, held):
                pieces[part][rel] = data
        halves = [pieces[part][rel] for part in range(2) for rel in range(self.n)]
        whole = decode(jnp.stack(halves), self.bound)
        return whole.reshape((2, self.n) + whole.shape[1:])


def per_device(
    hidden_in, lengths, norm_gain, in_gate_inner, in_step, in_shared, conv_inner, conv_inner_bias,
    conv_shared, conv_shared_bias, step_bias, log_decay, skip_gain, gate_gain, out_weight, cotangent,
):
    tokens, local = hidden_in.shape
    full = in_gate_inner.shape[0]
    width = in_gate_inner.shape[2]
    heads = step_bias.shape[0]
    chips = full // local // 2
    lines = tokens // L
    inner_total = width * (full // local)
    core = lax.axis_index("heads") & 1
    source_t, cot_t = lax.optimization_barrier((hidden_in.T, cotangent.T))

    hidden_all = lax.all_gather(hidden_in, "heads", axis=1, tiled=True)
    shared_all = lax.all_gather(in_shared, "heads", axis=1, tiled=True)
    gain_all = lax.all_gather(norm_gain, "heads", axis=0, tiled=True)
    cot_all = lax.all_gather(cotangent, "heads", axis=1, tiled=True)
    wgi = in_gate_inner.reshape(full, 2 * width)
    step_pad = jnp.pad(in_step, ((0, 0), (0, L - heads)))
    wss = jnp.concatenate([shared_all.T, step_pad], axis=1)
    w_back = jnp.concatenate([wgi, step_pad], axis=1)

    def halves(w, axis):
        both = []
        for side in (1 - core, core):
            parts = [
                lax.dynamic_slice_in_dim(w, (2 * k + side) * local, local, axis) for k in range(chips)
            ]
            both.append(jnp.stack(parts))
        return both

    back_send, back_own = halves(w_back, 0)
    out_send, out_own = halves(out_weight, 1)
    w_size = jnp.sqrt(jnp.max(jnp.sum(jnp.square(w_back.astype(f32)), axis=1)))
    cp, sp, hp = pack_params(
        conv_inner, conv_inner_bias, conv_shared, conv_shared_bias, step_bias, log_decay,
        skip_gain, gate_gain,
    )

    hidden_all = after(hidden_all, back_send, back_own, out_send, out_own, w_size, cp, sp, hp, source_t, cot_t)
    source_t = source_t.astype(f32)
    normed, inv_rows, gate, rest, gated, y, st, gsum_part = run_fwd(
        lengths, hidden_all, gain_all[None], wgi, wss, cp, sp, hp
    )
    inv_rms = inv_rows.reshape(tokens)
    gsum = sum_small(gsum_part.reshape(lines, L), "heads", 1)

    live = (jnp.arange(tokens, dtype=jnp.int32) < jnp.sum(lengths[0])).astype(bf16)
    gate_rms = lax.rsqrt(gsum.reshape(tokens) / inner_total + EPSILON)
    scaled = (gated * gate_rms[:, None] * gate_gain[None, :]).astype(bf16) * live[:, None]

    def project(w, v, axis):
        return lax.dot_general(w, v, (((axis,), (1,)), ((), ())), preferred_element_type=f32)

    half = jnp.float16
    mixed = ScatterLine(
        project(out_send, scaled, 1).astype(half), project(out_own, scaled, 1).astype(half)
    )
    mixed.swap()
    mixed.pack(0)
    cot_late = after(cot_all, *mixed.out)
    mixed.send(0)
    gs, gdot_part = run_mid(lengths, cot_late, out_weight, gated, cp)
    gdot = sum_small(gdot_part.reshape(lines, L), "heads", 2)
    mixed.hold(gdot)
    mixed.pack(1)
    gdot = after(gdot, *mixed.out)
    mixed.send(1)

    low, gsh_part, nd_part, size, pg, sg, hg = run_bwd(
        inner_total, lengths, gate, rest, gs, y, st, gsum.reshape(lines, 1, L),
        gdot.reshape(lines, 1, L), cp, sp, hp,
    )
    bound = jnp.sqrt(size.reshape(lines, L)) * (1.01 * w_size) + 1e-30
    mixed.hold(low)
    mixed.pack(2)
    nd_part = after(nd_part, *mixed.out)
    mixed.send(2)
    small = sum_small(
        jnp.concatenate([nd_part.reshape(lines, L), bound, sg], axis=0), "heads", 3
    )
    norm_dot, sg = small[:lines].reshape(tokens), small[2 * lines :]
    bound = small[lines : 2 * lines].reshape(tokens)
    low = after(low, bound)

    normal = ScatterLine(
        encode(project(back_send, low, 2), bound, half),
        encode(project(back_own, low, 2), bound, half),
    )
    normal.swap()
    normal.pack(0)
    low_late = after(low, *normal.out)
    scaled_late = after(scaled, *normal.out)
    gsh_part = after(gsh_part, *normal.out)
    mixed.hold(*normal.out)
    normal.send(0)

    cut = gsh_part.T.reshape(chips, 2, L // (2 * chips), tokens)
    gsh_own = lax.dynamic_index_in_dim(cut, core, 1, keepdims=False)
    gsh_send = lax.dynamic_index_in_dim(cut, 1 - core, 1, keepdims=False)
    shared = ScatterLine(gsh_send, gsh_own)
    shared.swap()
    grad_wout = lax.dot_general(
        scaled_late, cot_all, (((0,), (0,)), ((), ())), preferred_element_type=f32
    )
    top_wout = jnp.max(jnp.abs(grad_wout))
    shared.pack(0)
    low_late = after(low_late, *shared.out)
    shared.send(0)
    grad_proj = lax.dot_general(
        normed, low_late, (((0,), (0,)), ((), ())), preferred_element_type=f32
    )
    top_proj = jnp.max(jnp.abs(grad_proj))
    shared.hold(top_proj)
    shared.pack(1)
    top_proj = after(top_proj, *shared.out)
    shared.send(1)
    shared.hold(top_proj)
    shared.pack(2)
    normal.hold(top_proj, *shared.out)
    shared.send(2)
    normal.pack(1)
    top_proj = after(top_proj, *normal.out)
    tops = jnp.stack([top_proj, top_wout])
    tops = jnp.broadcast_to(jnp.repeat(tops * 1.01 + 1e-30, 8)[:, None], (16, L))
    wide = pg.reshape(8 * width // L, L)
    small = sum_small(jnp.concatenate([tops, sg, hg, wide], axis=0), "rows", 4)

    mixed.hold(*normal.out)
    normal.send(1)
    top_proj, top_wout, sg, hg = small[0, 0], small[8, 0], small[16:24], small[24:32]
    pg = small[32:].reshape(8, width)
    sum_proj, sum_wout = RowSum(grad_proj, top_proj), RowSum(grad_wout, top_wout)
    for k in range(sum_proj.bits):
        sum_proj.reduce(k)
        sum_wout.reduce(k)
    shared.rest(3)
    low_shared = lax.all_gather(shared.total().astype(bf16), "heads", axis=0, tiled=True)
    mixed.rest(3)
    output_t = (source_t + mixed.total()).astype(bf16)

    normal.pack(2)
    out = normal.out
    normal.send(2)
    grad_proj, grad_step = place(
        sum_proj.spread(*out), unpack_kernel, [(full, 2, width), (full, heads)]
    )
    (grad_wout,) = place(sum_wout.spread(*out), place_kernel, [grad_wout.shape])

    low_shared = after(low_shared, *out)
    shared_raw = rest[:, width : width + L]
    norm_dot = norm_dot + jnp.sum(low_shared.astype(f32) * shared_raw.T, axis=0)
    normed_t = (source_t * inv_rms[None, :] * norm_gain[:, None]).astype(bf16)
    grad_shared_w = lax.dot_general(
        low_shared, normed_t, (((1,), (1,)), ((), ())), preferred_element_type=f32
    )
    grad_shared_w = sum_small(grad_shared_w.reshape(local, L), "rows", 6).reshape(L, local)
    more = lax.dot_general(
        in_shared, low_shared, (((0,), (0,)), ((), ())), preferred_element_type=f32
    )

    normal.rest(3)
    grad_normed = normal.total() * (bound / SCALE)[None, :] + more
    grad_gain_norm = jnp.sum(grad_normed * source_t * inv_rms[None, :], axis=1)
    grad_source = (
        inv_rms[None, :] * norm_gain[:, None] * grad_normed
        - source_t * (inv_rms * inv_rms * norm_dot / full)[None, :]
    )
    grad_input = (cot_t.astype(f32) + grad_source).T
    output = output_t.T
    grad_gain_norm = sum_small(grad_gain_norm.reshape(local // L, L), "rows", 5).reshape(local)
    return (
        output,
        grad_input,
        grad_gain_norm,
        grad_proj,
        grad_step,
        grad_shared_w,
        pg[0:4],
        pg[4],
        sg[0:4],
        sg[4],
        hg[0, :heads],
        hg[1, :heads],
        pg[5].reshape(heads, HEAD).sum(axis=1),
        pg[6],
        grad_wout,
    )


def solution(mesh):
    return jax.shard_map(
        per_device,
        mesh=mesh,
        in_specs=(
            P("rows", "heads"), P("rows", None), P("heads"), P(None, None, "heads"),
            P(None, "heads"), P(None, "heads"), P(None, "heads"), P("heads"), P(), P(),
            P("heads"), P("heads"), P("heads"), P("heads"), P("heads", None), P("rows", "heads"),
        ),
        out_specs=(
            P("rows", "heads"), P("rows", "heads"), P("heads"), P(None, None, "heads"),
            P(None, "heads"), P(None, "heads"), P(None, "heads"), P("heads"), P(), P(),
            P("heads"), P("heads"), P("heads"), P("heads"), P("heads", None),
        ),
        check_vma=False,
    )
```

```python
import functools

import jax
import jax.numpy as jnp
from jax import lax
from jax.experimental import pallas as pl
from jax.experimental.pallas import tpu as pltpu
from jax.sharding import PartitionSpec as P


EPSILON = 1e-05
L = 128
LB = 512
NSUB = LB // L
HEAD = 64
STATE = 64
f32 = jnp.float32
bf16 = jnp.bfloat16


def mm(a, b, ca=1, cb=0):
    return lax.dot_general(a, b, (((ca,), (cb,)), ((), ())), preferred_element_type=f32)


def split(x):
    hi = x.astype(bf16)
    return hi, (x - hi.astype(f32)).astype(bf16)


def mm3(a, b, ca=1, cb=0):
    ah, al = split(a)
    bh, bl = split(b)
    return mm(ah, bh, ca, cb) + mm(ah, bl, ca, cb) + mm(al, bh, ca, cb)


def mm_exact_left(mask, x):
    hi = x.astype(bf16)
    rest = x - hi.astype(f32)
    mid = rest.astype(bf16)
    low = (rest - mid.astype(f32)).astype(bf16)
    return mm(mask, hi) + mm(mask, mid) + mm(mask, low)


def block_diag(x, first):
    zero = jnp.zeros_like(x)
    return jnp.concatenate([jnp.where(first, x, zero), jnp.where(first, zero, x)], axis=0)


def bounds_of(len_ref):
    b0 = len_ref[0, 0]
    b1 = b0 + len_ref[0, 1]
    b2 = b1 + len_ref[0, 2]
    b3 = b2 + len_ref[0, 3]
    return b0, b1, b2, b3


def start_of(bounds, t):
    start = jnp.zeros_like(t)
    for b in bounds:
        start = jnp.where(t >= b, b, start)
    return start


def to_row(col):
    return jnp.transpose(jnp.broadcast_to(col, (L, L)))[0:1, :]


def to_col(row):
    return jnp.transpose(jnp.broadcast_to(row, (L, L)))


def pair_cols(a, q, first):
    return jnp.where(first, a[:, 2 * q : 2 * q + 1], a[:, 2 * q + 1 : 2 * q + 2])


def sigmoid(v):
    return 0.5 + 0.5 * jnp.tanh(0.5 * v)


def softplus(v):
    return jnp.maximum(v, 0.0) + jnp.log1p(jnp.exp(-jnp.abs(v)))


def shifted(win, m):
    if m == 0:
        return win[8:, :]
    return pltpu.roll(win, m, 0)[8:, :]


def chunk_columns(hp_ref, step, bounds, base):
    tcol = lax.broadcasted_iota(jnp.int32, (L, L), 0) + base
    trow = lax.broadcasted_iota(jnp.int32, (L, L), 1) + base
    start_col = start_of(bounds, tcol)
    start_end = start_of(bounds, base + (L - 1))
    raw = step + hp_ref[0:1, :]
    dt = softplus(raw)
    decay = hp_ref[1:2, :] * dt
    lower = jnp.where(trow <= tcol, 1.0, 0.0).astype(bf16)
    cum = mm_exact_left(lower, decay)
    cum_end = cum[L - 1 : L, :]
    ecum = jnp.where(start_col < base, jnp.exp(cum), 0.0)
    wend = jnp.where(tcol >= start_end, jnp.exp(cum_end - cum), 0.0)
    carried_end = (start_end < base).astype(f32)
    cdec = jnp.exp(cum_end) * carried_end
    return tcol, trow, start_col, start_end, raw, dt, decay, cum, ecum, wend, cdec


def fwd_kernel(
    len_ref, h_ref, gain_ref, wgi_ref, wss_ref, cp_ref, sp_ref, hp_ref,
    normed_ref, inv_ref, gate_ref, rest_ref, gated_ref, y_ref, st_ref, gsum_ref,
    vbuf, state,
):
    blk = pl.program_id(0)
    width = gate_ref.shape[1]
    full = h_ref.shape[1]
    pairs = width // L

    @pl.when(blk == 0)
    def _():
        vbuf[0:8, :] = jnp.zeros((8, vbuf.shape[1]), f32)
        state[...] = jnp.zeros(state.shape, f32)

    piece = 256

    def norm_rows(s, carry):
        rows = pl.ds(pl.multiple_of(s * L, L), L)
        acc = jnp.zeros((L, piece), f32)
        for k in range(full // piece):
            x = h_ref[rows, k * piece : (k + 1) * piece].astype(f32)
            acc = acc + x * x
        inv = lax.rsqrt(jnp.sum(acc, axis=1, keepdims=True) / full + EPSILON)
        for k in range(full // piece):
            cols = slice(k * piece, (k + 1) * piece)
            x = h_ref[rows, cols].astype(f32)
            normed_ref[rows, cols] = (x * inv * gain_ref[0:1, cols]).astype(bf16)
        inv_ref[s] = to_row(inv)
        return carry

    lax.fori_loop(0, NSUB, norm_rows, 0)
    normed = normed_ref[...]
    gate_ref[...] = mm(normed, wgi_ref[:, :width])
    inner = mm(normed, wgi_ref[:, width:])
    vbuf[8:, :width] = inner
    rest_ref[:, :width] = inner
    tail = mm(normed, wss_ref[...])
    vbuf[8:, width:] = tail[:, :L]
    rest_ref[:, width:] = tail

    bounds = bounds_of(len_ref)
    first = lax.broadcasted_iota(jnp.int32, (L, L), 1) < HEAD

    def chunk(s, carry):
        r0 = pl.multiple_of(s * L, L)
        rows = pl.ds(r0, L)
        base = blk * LB + s * L
        step = rest_ref[rows, width + L :]
        tcol, trow, start_col, _, _, dt, _, cum, ecum, wend, cdec = chunk_columns(
            hp_ref, step, bounds, base
        )
        cum_t = jnp.transpose(cum)
        mask = (trow <= tcol) & (trow >= start_col)
        valid = [tcol - m >= start_col for m in range(4)]

        def conv(cols, taps):
            win = vbuf[pl.ds(r0, L + 8), cols]
            pre = taps[4:5, :] + taps[3:4, :] * win[8:, :]
            for m in range(1, 4):
                pre = pre + taps[3 - m : 4 - m, :] * jnp.where(valid[m], shifted(win, m), 0.0)
            return pre

        pre_s = conv(slice(width, width + L), sp_ref)
        act = pre_s * sigmoid(pre_s)
        b_map = act[:, :STATE]
        c_map = act[:, STATE:]
        scores = jnp.where(mask, mm3(c_map, b_map, 1, 1), 0.0)
        square = jnp.zeros((L, L), f32)
        for q in range(pairs):
            cols = slice(q * L, (q + 1) * L)
            pre = conv(cols, cp_ref.at[:, cols])
            xin = pre * sigmoid(pre)
            xp = xin * pair_cols(dt, q, first)
            xh, xl = split(xp)
            bdh, bdl = block_diag(xh, first), block_diag(xl, first)
            mix = []
            for h in (2 * q, 2 * q + 1):
                spread = jnp.minimum(cum[:, h : h + 1] - cum_t[h : h + 1, :], 0.0)
                mix.append(jnp.exp(spread) * scores)
            mh, ml = split(jnp.concatenate(mix, axis=1))
            both = mm(mh, jnp.concatenate([bdh, bdl], axis=1))
            y = both[:, :L] + both[:, L:] + mm(ml, bdh)
            st = state[:, cols]
            st_ref[s, :, cols] = st
            y = y + mm3(c_map, st) * pair_cols(ecum, q, first)
            xw = xp * pair_cols(wend, q, first)
            state[:, cols] = mm3(b_map, xw, 0, 0) + st * pair_cols(cdec, q, first[0:1, :])
            y_ref[rows, cols] = y
            gate = gate_ref[rows, cols]
            gated = (y + cp_ref[5:6, cols] * xin) * (gate * sigmoid(gate))
            gated_ref[rows, cols] = gated
            square = square + gated * gated
        gsum_ref[s] = to_row(jnp.sum(square, axis=1, keepdims=True))
        return carry

    lax.fori_loop(0, NSUB, chunk, 0)
    vbuf[0:8, :] = vbuf[LB : LB + 8, :]


def mid_kernel(len_ref, cot_ref, w_ref, gated_ref, cp_ref, gs_ref, gdot_ref):
    blk = pl.program_id(0)
    live = bounds_of(len_ref)[3]
    t = lax.broadcasted_iota(jnp.int32, gs_ref.shape, 0) + blk * LB
    gs = jnp.where(t < live, mm(cot_ref[...], w_ref[...], 1, 1), 0.0)
    gs_ref[...] = gs
    dots = jnp.sum(gs * cp_ref[6:7, :] * gated_ref[...], axis=1, keepdims=True)
    for s in range(NSUB):
        gdot_ref[s] = to_row(dots[s * L : (s + 1) * L, :])


def bwd_kernel(
    inner_total,
    len_ref, gate_ref, rest_ref, halo_ref, gs_ref, y_ref, st_ref, gsum_ref, gdot_ref,
    cp_ref, sp_ref, hp_ref,
    low_ref, gsh_ref, nd_ref, size_ref, pg_ref, sg_ref, hg_ref,
    vbuf, qnext, adj, send,
):
    step_id = pl.program_id(0)
    blk = pl.num_programs(0) - 1 - step_id
    width = gate_ref.shape[1]
    pairs = width // L

    @pl.when(step_id == 0)
    def _():
        qnext[...] = jnp.zeros(qnext.shape, f32)
        adj[...] = jnp.zeros(adj.shape, f32)
        send[...] = jnp.zeros(send.shape, f32)
        pg_ref[...] = jnp.zeros(pg_ref.shape, f32)
        sg_ref[...] = jnp.zeros(sg_ref.shape, f32)
        hg_ref[...] = jnp.zeros(hg_ref.shape, f32)

    vbuf[0:8, :] = halo_ref[:, : width + L]
    vbuf[8:, :] = rest_ref[:, : width + L]
    bounds = bounds_of(len_ref)
    first = lax.broadcasted_iota(jnp.int32, (L, L), 1) < HEAD
    lane = lax.broadcasted_iota(jnp.int32, (L, L), 1)
    half = lax.broadcasted_iota(jnp.int32, (L, L), 0) // HEAD

    def chunk(i, carry):
        s = NSUB - 1 - i
        r0 = pl.multiple_of(s * L, L)
        rows = pl.ds(r0, L)
        base = blk * LB + s * L
        step = rest_ref[rows, width + L :]
        tcol, trow, start_col, start_end, raw, dt, decay, cum, ecum, wend, cdec = chunk_columns(
            hp_ref, step, bounds, base
        )
        cum_t = jnp.transpose(cum)
        mask_t = (trow >= tcol) & (start_of(bounds, trow) <= tcol)
        valid = [tcol - m >= start_col for m in range(4)]
        valid_up = [start_of(bounds, tcol + m) <= tcol for m in range(4)]
        gate_rms_row = lax.rsqrt(gsum_ref[s] / inner_total + EPSILON)
        pull_row = gate_rms_row * gate_rms_row * gate_rms_row * gdot_ref[s] / inner_total
        gate_rms = to_col(gate_rms_row)
        pull = to_col(pull_row)

        def conv(cols, taps):
            win = vbuf[pl.ds(r0, L + 8), cols]
            seen = [win[8:, :]]
            pre = taps[4:5, :] + taps[3:4, :] * seen[0]
            for m in range(1, 4):
                seen.append(jnp.where(valid[m], shifted(win, m), 0.0))
                pre = pre + taps[3 - m : 4 - m, :] * seen[m]
            return seen, pre

        def conv_back(q, seen, cols, taps, grad_ref, grad_cols):
            win = jnp.concatenate([q, qnext[:, cols]], axis=0)
            qnext[:, cols] = q[0:8, :]
            grad = taps[3:4, :] * q
            for m in range(1, 4):
                up = pltpu.roll(win, L + 8 - m, 0)[:L, :]
                grad = grad + taps[3 - m : 4 - m, :] * jnp.where(valid_up[m], up, 0.0)
            for m in range(4):
                k = 3 - m
                grad_ref[k : k + 1, grad_cols] += jnp.sum(q * seen[m], axis=0, keepdims=True)
            grad_ref[4:5, grad_cols] += jnp.sum(q, axis=0, keepdims=True)
            return grad

        seen_s, pre_s = conv(slice(width, width + L), sp_ref)
        sig_s = sigmoid(pre_s)
        act = pre_s * sig_s
        b_map = act[:, :STATE]
        c_map = act[:, STATE:]
        scores_t = jnp.where(mask_t, mm3(b_map, c_map, 1, 1), 0.0)
        d_scores = jnp.zeros((L, L), f32)
        d_b = jnp.zeros((L, STATE), f32)
        d_c = jnp.zeros((L, STATE), f32)
        reduced = jnp.zeros((2 * L, L), f32)
        ends = jnp.zeros((8, L), f32)
        norm_dot = jnp.zeros((L, L), f32)
        size = jnp.zeros((L, L), f32)
        for q in range(pairs):
            cols = slice(q * L, (q + 1) * L)
            taps = cp_ref.at[:, cols]
            skip = cp_ref[5:6, cols]
            seen, pre = conv(cols, taps)
            sig = sigmoid(pre)
            xin = pre * sig
            dtx = pair_cols(dt, q, first)
            xp = xin * dtx
            y = y_ref[rows, cols]
            ho = y + skip * xin
            gate = gate_ref[rows, cols]
            gsig = sigmoid(gate)
            sl = gate * gsig
            gated = ho * sl
            gs = gs_ref[rows, cols]
            pg_ref[6:7, cols] += jnp.sum(gs * gated * gate_rms, axis=0, keepdims=True)
            gg = gate_rms * cp_ref[6:7, cols] * gs - gated * pull
            gy = gg * sl
            low_gate = (gg * ho * (gsig * (1.0 + gate * (1.0 - gsig)))).astype(bf16)
            low_ref[rows, cols] = low_gate
            pg_ref[5:6, cols] += jnp.sum(gy * xin, axis=0, keepdims=True)

            yh, yl = split(gy)
            bdh, bdl = block_diag(yh, first), block_diag(yl, first)
            xh, xl = split(xp)
            d_mix = mm(
                jnp.concatenate([xh, xl], axis=1), jnp.concatenate([bdh, bdh], axis=1), 1, 1
            ) + mm(xh, bdl, 1, 1)
            mix = []
            for k in range(2):
                h = 2 * q + k
                spread = jnp.minimum(cum_t[h : h + 1, :] - cum[:, h : h + 1], 0.0)
                factor = jnp.exp(spread)
                d_scores = d_scores + d_mix[:, k * L : (k + 1) * L] * factor
                mix.append(factor * scores_t)
            mh, ml = split(jnp.concatenate(mix, axis=1))
            both = mm(mh, jnp.concatenate([bdh, bdl], axis=1))
            dxp = both[:, :L] + both[:, L:] + mm(ml, bdh)
            wendx = pair_cols(wend, q, first)
            a_in = adj[:, cols]
            dxp = dxp + mm3(b_map, a_in) * wendx
            xw = xp * wendx
            gyw = gy * pair_cols(ecum, q, first)
            s_in = st_ref[s, :, cols]
            d_b = d_b + mm3(xw, a_in, 1, 1)
            d_c = d_c + mm3(gyw, s_in, 1, 1)
            adj[:, cols] = mm3(c_map, gyw, 0, 0) + a_in * pair_cols(cdec, q, first[0:1, :])
            heads = jnp.where(lane == 2 * q + half, 1.0, 0.0).astype(bf16)
            zh, zl = split(jnp.concatenate([gy * y - dxp * xp, dxp * xin], axis=0))
            reduced = reduced + mm(zh, heads) + mm(zl, heads)
            end = jnp.broadcast_to(
                jnp.sum(a_in * send[:, cols], axis=0, keepdims=True), (8, L)
            )
            eh, el = split(end)
            ends = ends + mm(eh, heads) + mm(el, heads)
            send[:, cols] = s_in

            dxin = dxp * dtx + skip * gy
            qv = dxin * (sig * (1.0 + pre * (1.0 - sig)))
            grad = conv_back(qv, seen, cols, taps, pg_ref, cols)
            low_inner = grad.astype(bf16)
            low_ref[rows, width + q * L : width + (q + 1) * L] = low_inner
            wide_gate, wide_inner = low_gate.astype(f32), low_inner.astype(f32)
            norm_dot = norm_dot + wide_gate * gate + wide_inner * seen[0]
            size = size + wide_gate * wide_gate + wide_inner * wide_inner

        d_scores = jnp.where(mask_t, d_scores, 0.0)
        d_b = d_b + mm3(d_scores, c_map)
        d_c = d_c + mm3(d_scores, b_map, 0, 0)
        d_act = jnp.concatenate([d_b, d_c], axis=1)
        q_s = d_act * (sig_s * (1.0 + pre_s * (1.0 - sig_s)))
        shared_cols = slice(width, width + L)
        gsh_ref[rows, :] = conv_back(q_s, seen_s, shared_cols, sp_ref, sg_ref, slice(0, L))

        tail = jnp.where(tcol >= start_end, ends[0:1, :], 0.0)
        keep = jnp.where(mask_t, 1.0, 0.0).astype(bf16)
        d_decay = mm_exact_left(keep, reduced[:L, :]) + tail
        d_dt = reduced[L:, :] + d_decay * hp_ref[1:2, :]
        d_raw = d_dt * sigmoid(raw)
        hg_ref[0:1, :] += jnp.sum(d_raw, axis=0, keepdims=True)
        hg_ref[1:2, :] += jnp.sum(d_decay * decay, axis=0, keepdims=True)
        low_step = d_raw.astype(bf16)
        low_ref[rows, 2 * width :] = low_step
        wide_step = low_step.astype(f32)
        norm_dot = norm_dot + wide_step * step
        size = size + wide_step * wide_step
        nd_ref[s] = to_row(jnp.sum(norm_dot, axis=1, keepdims=True))
        size_ref[s] = to_row(jnp.sum(size, axis=1, keepdims=True))
        return carry

    lax.fori_loop(0, NSUB, chunk, 0)


def unpack_kernel(me_ref, x_ref, gate_inner_ref, step_ref):
    width = gate_inner_ref.shape[2]
    gate_inner_ref[:, 0, :] = x_ref[0, 0, :, :width]
    gate_inner_ref[:, 1, :] = x_ref[0, 0, :, width : 2 * width]
    step_ref[...] = x_ref[0, 0, :, 2 * width : 2 * width + step_ref.shape[1]]


def place_kernel(me_ref, x_ref, out_ref):
    out_ref[...] = x_ref[0, 0]


def place(x, kernel, shapes):
    _, n, piece, cols = x.shape

    def spec(shape):
        zeros = (0,) * (len(shape) - 1)
        return pl.BlockSpec((piece,) + shape[1:], lambda p, k, me: (p * n + (me[0] ^ k),) + zeros)

    return pl.pallas_call(
        kernel,
        grid_spec=pltpu.PrefetchScalarGridSpec(
            num_scalar_prefetch=1,
            grid=(2, n),
            in_specs=[pl.BlockSpec((1, 1, piece, cols), lambda p, k, me: (p, k, 0, 0))],
            out_specs=[spec(shape) for shape in shapes],
        ),
        out_shape=[jax.ShapeDtypeStruct(shape, f32) for shape in shapes],
        name="place",
    )(lax.axis_index("rows").astype(jnp.int32)[None], x)


def rows_spec(cols, order):
    return pl.BlockSpec((LB, cols), lambda i: (order(i), 0))


def line_spec(order):
    return pl.BlockSpec((NSUB, 1, L), lambda i: (order(i), 0, 0))


def whole_spec(shape):
    return pl.BlockSpec(shape, lambda i: (0,) * len(shape), pipeline_mode=pl.Buffered(1))


def smem_spec():
    return pl.BlockSpec(memory_space=pltpu.SMEM)


VMEM_LIMIT = 60 * 1024 * 1024


def run_fwd(lengths, hidden, gain, wgi, wss, cp, sp, hp):
    tokens, full = hidden.shape
    width = wgi.shape[1] // 2
    lines = tokens // L

    def same(i):
        return i

    return pl.pallas_call(
        fwd_kernel,
        grid=(tokens // LB,),
        in_specs=[
            smem_spec(),
            rows_spec(full, same),
            whole_spec(gain.shape),
            whole_spec(wgi.shape),
            whole_spec(wss.shape),
            whole_spec(cp.shape),
            whole_spec(sp.shape),
            whole_spec(hp.shape),
        ],
        out_specs=[
            rows_spec(full, same),
            line_spec(same),
            rows_spec(width, same),
            rows_spec(width + 2 * L, same),
            rows_spec(width, same),
            rows_spec(width, same),
            pl.BlockSpec((NSUB, STATE, width), lambda i: (i, 0, 0)),
            line_spec(same),
        ],
        out_shape=[
            jax.ShapeDtypeStruct((tokens, full), bf16),
            jax.ShapeDtypeStruct((lines, 1, L), f32),
            jax.ShapeDtypeStruct((tokens, width), f32),
            jax.ShapeDtypeStruct((tokens, width + 2 * L), f32),
            jax.ShapeDtypeStruct((tokens, width), f32),
            jax.ShapeDtypeStruct((tokens, width), f32),
            jax.ShapeDtypeStruct((lines, STATE, width), f32),
            jax.ShapeDtypeStruct((lines, 1, L), f32),
        ],
        scratch_shapes=[
            pltpu.VMEM((LB + 8, width + L), f32),
            pltpu.VMEM((STATE, width), f32),
        ],
        compiler_params=pltpu.CompilerParams(
            dimension_semantics=("arbitrary",), vmem_limit_bytes=VMEM_LIMIT
        ),
        name="mixer_fwd",
    )(lengths, hidden, gain, wgi, wss, cp, sp, hp)


def run_mid(lengths, cot, w_out, gated, cp):
    tokens, full = cot.shape
    width = gated.shape[1]
    lines = tokens // L

    def same(i):
        return i

    return pl.pallas_call(
        mid_kernel,
        grid=(tokens // LB,),
        in_specs=[
            smem_spec(),
            rows_spec(full, same),
            whole_spec(w_out.shape),
            rows_spec(width, same),
            whole_spec(cp.shape),
        ],
        out_specs=[rows_spec(width, same), line_spec(same)],
        out_shape=[
            jax.ShapeDtypeStruct((tokens, width), f32),
            jax.ShapeDtypeStruct((lines, 1, L), f32),
        ],
        compiler_params=pltpu.CompilerParams(
            dimension_semantics=("arbitrary",), vmem_limit_bytes=VMEM_LIMIT
        ),
        name="mixer_mid",
    )(lengths, cot, w_out, gated, cp)


def run_bwd(inner_total, lengths, gate, rest, gs, y, st, gsum, gdot, cp, sp, hp):
    tokens, width = gate.shape
    lines = tokens // L
    blocks = tokens // LB

    def back(i):
        return blocks - 1 - i

    def halo(i):
        return (jnp.maximum(back(i) * (LB // 8) - 1, 0), 0)

    return pl.pallas_call(
        functools.partial(bwd_kernel, float(inner_total)),
        grid=(blocks,),
        in_specs=[
            smem_spec(),
            rows_spec(width, back),
            rows_spec(width + 2 * L, back),
            pl.BlockSpec((8, width + 2 * L), halo),
            rows_spec(width, back),
            rows_spec(width, back),
            pl.BlockSpec((NSUB, STATE, width), lambda i: (back(i), 0, 0)),
            line_spec(back),
            line_spec(back),
            whole_spec(cp.shape),
            whole_spec(sp.shape),
            whole_spec(hp.shape),
        ],
        out_specs=[
            rows_spec(2 * width + L, back),
            rows_spec(L, back),
            line_spec(back),
            line_spec(back),
            pl.BlockSpec((8, width), lambda i: (0, 0)),
            pl.BlockSpec((8, L), lambda i: (0, 0)),
            pl.BlockSpec((8, L), lambda i: (0, 0)),
        ],
        out_shape=[
            jax.ShapeDtypeStruct((tokens, 2 * width + L), bf16),
            jax.ShapeDtypeStruct((tokens, L), f32),
            jax.ShapeDtypeStruct((lines, 1, L), f32),
            jax.ShapeDtypeStruct((lines, 1, L), f32),
            jax.ShapeDtypeStruct((8, width), f32),
            jax.ShapeDtypeStruct((8, L), f32),
            jax.ShapeDtypeStruct((8, L), f32),
        ],
        scratch_shapes=[
            pltpu.VMEM((LB + 8, width + L), f32),
            pltpu.VMEM((8, width + L), f32),
            pltpu.VMEM((STATE, width), f32),
            pltpu.VMEM((STATE, width), f32),
        ],
        compiler_params=pltpu.CompilerParams(
            dimension_semantics=("arbitrary",), vmem_limit_bytes=VMEM_LIMIT
        ),
        name="mixer_bwd",
    )(lengths, gate, rest, rest, gs, y, st, gsum, gdot, cp, sp, hp)


def pack_params(conv_inner, conv_inner_bias, conv_shared, conv_shared_bias, step_bias, log_decay,
                skip_gain, gate_gain):
    width = conv_inner.shape[1]
    heads = step_bias.shape[0]
    skip = jnp.repeat(skip_gain, HEAD)
    cp = jnp.concatenate(
        [conv_inner, conv_inner_bias[None], skip[None], gate_gain[None], jnp.zeros((1, width), f32)],
        axis=0,
    )
    sp = jnp.concatenate([conv_shared, conv_shared_bias[None], jnp.zeros((3, L), f32)], axis=0)
    hp = jnp.zeros((8, L), f32)
    hp = hp.at[0, :heads].set(step_bias).at[1, :heads].set(-jnp.exp(log_decay))
    return cp, sp, hp


def exchange_kernel(axis, x_ref, out_ref, slots, send_sem, recv_sem):
    me = lax.axis_index(axis)
    n = slots.shape[0]
    barrier = pltpu.get_barrier_semaphore()
    for k in range(1, n):
        peer = lax.rem(me + k, n)
        pl.semaphore_signal(barrier, inc=1, device_id={axis: peer})
    pl.semaphore_wait(barrier, n - 1)
    copies = []
    for k in range(1, n):
        peer = lax.rem(me + k, n)
        copy = pltpu.make_async_remote_copy(
            src_ref=x_ref,
            dst_ref=slots.at[k],
            send_sem=send_sem.at[k],
            recv_sem=recv_sem.at[k],
            device_id={axis: peer},
        )
        copy.start()
        copies.append(copy)
    for copy in copies:
        copy.wait()
    slots[0] = x_ref[...]
    total = slots[lax.rem(me, n)]
    for d in range(1, n):
        total = total + slots[lax.rem(me - d + n, n)]
    out_ref[...] = total


def sum_small(x, axis, collective_id):
    n = lax.axis_size(axis)
    return pl.pallas_call(
        functools.partial(exchange_kernel, axis),
        out_shape=jax.ShapeDtypeStruct(x.shape, f32),
        in_specs=[pl.BlockSpec(memory_space=pltpu.VMEM)],
        out_specs=pl.BlockSpec(memory_space=pltpu.VMEM),
        scratch_shapes=[
            pltpu.VMEM((n,) + x.shape, f32),
            pltpu.SemaphoreType.DMA((n,)),
            pltpu.SemaphoreType.DMA((n,)),
        ],
        compiler_params=pltpu.CompilerParams(collective_id=collective_id, has_side_effects=True),
        name="sum_small",
    )(x)


def after(x, *deps):
    deps = [d for d in deps if d is not None]
    return lax.optimization_barrier((x, *deps))[0]


SCALE = 16384.0


def encode(x, bound, kind):
    if bound is not None:
        x = x * (SCALE / bound)
    return x.astype(kind)


def decode(x, bound):
    x = x.astype(f32)
    return x if bound is None else x * (bound / SCALE)


class ScatterLine:

    def __init__(self, send, own):
        self.n = lax.axis_size("heads")
        self.chips = self.n // 2
        self.z = lax.axis_index("heads") >> 1
        self.message, self.own, self.kind = send, own, own.dtype
        self.moving, self.out = [None, None], [None, None]

    def swap(self):
        pairs = [(i, i ^ 1) for i in range(self.n)]
        self.got = lax.ppermute(self.message, "heads", pairs)

    def block(self, b):
        mine = lax.dynamic_index_in_dim(self.own, b, 0, keepdims=False)
        theirs = lax.dynamic_index_in_dim(self.got, b, 0, keepdims=False)
        return mine.astype(f32) + theirs.astype(f32)

    def pack(self, r):
        last = self.chips - 1
        for way in range(2):
            b = last - r + self.z if way == 0 else r - last + self.z
            total = self.block(jnp.clip(b, 0, last))
            if r > 0:
                total = total + self.moving[way].astype(f32)
            self.out[way] = total.astype(self.kind)

    def hold(self, *deps):
        self.moving = [after(m, *deps) for m in self.moving]

    def send(self, r):
        last = self.chips - 1
        out = lax.optimization_barrier(tuple(self.out))
        for way in range(2):
            chips = range(r + 1) if way == 0 else range(last - r, last + 1)
            hop = 2 if way == 0 else -2
            pairs = [(2 * k + c, 2 * k + c + hop) for k in chips for c in range(2)]
            self.moving[way] = lax.ppermute(out[way], "heads", pairs)
        self.moving = list(lax.optimization_barrier(tuple(self.moving)))

    def rest(self, r):
        for k in range(r, self.chips - 1):
            self.pack(k)
            self.send(k)

    def total(self):
        total = self.block(self.z)
        for way in range(2):
            if self.moving[way] is not None:
                total = total + self.moving[way].astype(f32)
        return total


class RowSum:

    def __init__(self, x, bound):
        self.n = lax.axis_size("rows")
        self.me = lax.axis_index("rows")
        self.bits = self.n.bit_length() - 1
        self.bound = bound
        piece = x.shape[0] // (2 * self.n)
        cut = x.reshape((2,) + (2,) * self.bits + (piece, x.shape[1]))
        self.cur = [cut[0], cut[1]]
        self.order = [[(k + part) % self.bits for k in range(self.bits)] for part in range(2)]
        self.left = [list(range(self.bits))[::-1] for _ in range(2)]

    def move(self, x, bit):
        return lax.ppermute(x, "rows", [(i, i ^ (1 << bit)) for i in range(self.n)])

    def reduce(self, k):
        for part in range(2):
            bit, left = self.order[part][k], self.left[part]
            mine = (self.me >> bit) & 1
            axis = left.index(bit)
            left.remove(bit)
            cur = self.cur[part]
            send = lax.dynamic_index_in_dim(cur, 1 - mine, axis, keepdims=False)
            keep = lax.dynamic_index_in_dim(cur, mine, axis, keepdims=False)
            got = self.move(encode(send, self.bound, jnp.float16), bit)
            self.cur[part] = keep + decode(got, self.bound)

    def hold(self, *deps):
        self.cur = [after(cur, *deps) for cur in self.cur]

    def spread(self, *deps):
        pieces = [{0: encode(cur, self.bound, jnp.float16)} for cur in self.cur]
        for k in reversed(range(self.bits)):
            far = []
            for part in range(2):
                bit = self.order[part][k]
                for rel in list(pieces[part]):
                    pieces[part][rel ^ (1 << bit)] = self.move(pieces[part][rel], bit)
                    far.append((part, rel ^ (1 << bit)))
            far_data = [pieces[part][rel] for part, rel in far]
            held = lax.optimization_barrier((*far_data, *deps))
            deps = ()
            for (part, rel), data in zip(far, held):
                pieces[part][rel] = data
        halves = [pieces[part][rel] for part in range(2) for rel in range(self.n)]
        whole = decode(jnp.stack(halves), self.bound)
        return whole.reshape((2, self.n) + whole.shape[1:])


def per_device(
    hidden_in, lengths, norm_gain, in_gate_inner, in_step, in_shared, conv_inner, conv_inner_bias,
    conv_shared, conv_shared_bias, step_bias, log_decay, skip_gain, gate_gain, out_weight, cotangent,
):
    tokens, local = hidden_in.shape
    full = in_gate_inner.shape[0]
    width = in_gate_inner.shape[2]
    heads = step_bias.shape[0]
    chips = full // local // 2
    lines = tokens // L
    inner_total = width * (full // local)
    core = lax.axis_index("heads") & 1
    source_t, cot_t = lax.optimization_barrier((hidden_in.T, cotangent.T))

    hidden_all = lax.all_gather(hidden_in, "heads", axis=1, tiled=True)
    shared_all = lax.all_gather(in_shared, "heads", axis=1, tiled=True)
    gain_all = lax.all_gather(norm_gain, "heads", axis=0, tiled=True)
    cot_all = lax.all_gather(cotangent, "heads", axis=1, tiled=True)
    wgi = in_gate_inner.reshape(full, 2 * width)
    step_pad = jnp.pad(in_step, ((0, 0), (0, L - heads)))
    wss = jnp.concatenate([shared_all.T, step_pad], axis=1)
    w_back = jnp.concatenate([wgi, step_pad], axis=1)

    def halves(w, axis):
        both = []
        for side in (1 - core, core):
            parts = [
                lax.dynamic_slice_in_dim(w, (2 * k + side) * local, local, axis) for k in range(chips)
            ]
            both.append(jnp.stack(parts))
        return both

    back_send, back_own = halves(w_back, 0)
    out_send, out_own = halves(out_weight, 1)
    w_size = jnp.sqrt(jnp.max(jnp.sum(jnp.square(w_back.astype(f32)), axis=1)))
    cp, sp, hp = pack_params(
        conv_inner, conv_inner_bias, conv_shared, conv_shared_bias, step_bias, log_decay,
        skip_gain, gate_gain,
    )

    hidden_all = after(hidden_all, back_send, back_own, out_send, out_own, w_size, cp, sp, hp, source_t, cot_t)
    source_t = source_t.astype(f32)
    normed, inv_rows, gate, rest, gated, y, st, gsum_part = run_fwd(
        lengths, hidden_all, gain_all[None], wgi, wss, cp, sp, hp
    )
    inv_rms = inv_rows.reshape(tokens)
    gsum = sum_small(gsum_part.reshape(lines, L), "heads", 1)

    live = (jnp.arange(tokens, dtype=jnp.int32) < jnp.sum(lengths[0])).astype(bf16)
    gate_rms = lax.rsqrt(gsum.reshape(tokens) / inner_total + EPSILON)
    scaled = (gated * gate_rms[:, None] * gate_gain[None, :]).astype(bf16) * live[:, None]

    def project(w, v, axis):
        return lax.dot_general(w, v, (((axis,), (1,)), ((), ())), preferred_element_type=f32)

    half = jnp.float16
    mixed = ScatterLine(
        project(out_send, scaled, 1).astype(half), project(out_own, scaled, 1).astype(half)
    )
    mixed.swap()
    mixed.pack(0)
    cot_late = after(cot_all, *mixed.out)
    mixed.send(0)
    gs, gdot_part = run_mid(lengths, cot_late, out_weight, gated, cp)
    gdot = sum_small(gdot_part.reshape(lines, L), "heads", 2)
    mixed.hold(gdot)
    mixed.pack(1)
    gdot = after(gdot, *mixed.out)
    mixed.send(1)

    low, gsh_part, nd_part, size, pg, sg, hg = run_bwd(
        inner_total, lengths, gate, rest, gs, y, st, gsum.reshape(lines, 1, L),
        gdot.reshape(lines, 1, L), cp, sp, hp,
    )
    bound = jnp.sqrt(size.reshape(lines, L)) * (1.01 * w_size) + 1e-30
    mixed.hold(low)
    mixed.pack(2)
    nd_part = after(nd_part, *mixed.out)
    mixed.send(2)
    small = sum_small(
        jnp.concatenate([nd_part.reshape(lines, L), bound, sg], axis=0), "heads", 3
    )
    norm_dot, sg = small[:lines].reshape(tokens), small[2 * lines :]
    bound = small[lines : 2 * lines].reshape(tokens)
    low = after(low, bound)

    normal = ScatterLine(
        encode(project(back_send, low, 2), bound, half),
        encode(project(back_own, low, 2), bound, half),
    )
    normal.swap()
    normal.pack(0)
    low_late = after(low, *normal.out)
    scaled_late = after(scaled, *normal.out)
    gsh_part = after(gsh_part, *normal.out)
    mixed.hold(*normal.out)
    normal.send(0)

    cut = gsh_part.T.reshape(chips, 2, L // (2 * chips), tokens)
    gsh_own = lax.dynamic_index_in_dim(cut, core, 1, keepdims=False)
    gsh_send = lax.dynamic_index_in_dim(cut, 1 - core, 1, keepdims=False)
    shared = ScatterLine(gsh_send, gsh_own)
    shared.swap()
    grad_wout = lax.dot_general(
        scaled_late, cot_all, (((0,), (0,)), ((), ())), preferred_element_type=f32
    )
    top_wout = jnp.max(jnp.abs(grad_wout))
    shared.pack(0)
    low_late = after(low_late, *shared.out)
    shared.send(0)
    grad_proj = lax.dot_general(
        normed, low_late, (((0,), (0,)), ((), ())), preferred_element_type=f32
    )
    top_proj = jnp.max(jnp.abs(grad_proj))
    normal.hold(top_proj)
    normal.pack(1)
    top_proj = after(top_proj, *normal.out)
    tops = jnp.stack([top_proj, top_wout])
    tops = jnp.broadcast_to(jnp.repeat(tops * 1.01 + 1e-30, 8)[:, None], (16, L))
    wide = pg.reshape(8 * width // L, L)
    small = sum_small(jnp.concatenate([tops, sg, hg, wide], axis=0), "rows", 4)

    mixed.hold(*normal.out)
    shared.hold(small)
    normal.send(1)
    shared.pack(1)
    shared.send(1)
    top_proj, top_wout, sg, hg = small[0, 0], small[8, 0], small[16:24], small[24:32]
    pg = small[32:].reshape(8, width)
    sum_proj, sum_wout = RowSum(grad_proj, top_proj), RowSum(grad_wout, top_wout)
    for k in range(sum_proj.bits):
        sum_proj.reduce(k)
        sum_wout.reduce(k)
    mixed.rest(3)
    output_t = (source_t + mixed.total()).astype(bf16)

    normal.pack(2)
    out = list(normal.out)
    shared.hold(*out)
    shared.pack(2)
    shared.send(2)
    normal.send(2)
    grad_proj, grad_step = place(
        sum_proj.spread(*out), unpack_kernel, [(full, 2, width), (full, heads)]
    )
    (grad_wout,) = place(sum_wout.spread(*out), place_kernel, [grad_wout.shape])

    shared.rest(3)
    low_shared = lax.all_gather(shared.total().astype(bf16), "heads", axis=0, tiled=True)
    shared_raw = rest[:, width : width + L]
    norm_dot = norm_dot + jnp.sum(low_shared.astype(f32) * shared_raw.T, axis=0)
    normed_t = (source_t * inv_rms[None, :] * norm_gain[:, None]).astype(bf16)
    grad_shared_w = lax.dot_general(
        low_shared, normed_t, (((1,), (1,)), ((), ())), preferred_element_type=f32
    )
    grad_shared_w = sum_small(grad_shared_w.reshape(local, L), "rows", 6).reshape(L, local)
    more = lax.dot_general(
        in_shared, low_shared, (((0,), (0,)), ((), ())), preferred_element_type=f32
    )

    normal.rest(3)
    grad_normed = normal.total() * (bound / SCALE)[None, :] + more
    grad_gain_norm = jnp.sum(grad_normed * source_t * inv_rms[None, :], axis=1)
    grad_source = (
        inv_rms[None, :] * norm_gain[:, None] * grad_normed
        - source_t * (inv_rms * inv_rms * norm_dot / full)[None, :]
    )
    grad_input = (cot_t.astype(f32) + grad_source).T
    output = output_t.T
    grad_gain_norm = sum_small(grad_gain_norm.reshape(local // L, L), "rows", 5).reshape(local)
    return (
        output,
        grad_input,
        grad_gain_norm,
        grad_proj,
        grad_step,
        grad_shared_w,
        pg[0:4],
        pg[4],
        sg[0:4],
        sg[4],
        hg[0, :heads],
        hg[1, :heads],
        pg[5].reshape(heads, HEAD).sum(axis=1),
        pg[6],
        grad_wout,
    )


def solution(mesh):
    return jax.shard_map(
        per_device,
        mesh=mesh,
        in_specs=(
            P("rows", "heads"), P("rows", None), P("heads"), P(None, None, "heads"),
            P(None, "heads"), P(None, "heads"), P(None, "heads"), P("heads"), P(), P(),
            P("heads"), P("heads"), P("heads"), P("heads"), P("heads", None), P("rows", "heads"),
        ),
        out_specs=(
            P("rows", "heads"), P("rows", "heads"), P("heads"), P(None, None, "heads"),
            P(None, "heads"), P(None, "heads"), P(None, "heads"), P("heads"), P(), P(),
            P("heads"), P("heads"), P("heads"), P("heads"), P("heads", None),
        ),
        check_vma=False,
    )
```
